32 devices in a mesh: dp: 1 (over z), my: 4 (over y), mx: 8 (over x, core).
Axes of the slice: x: 4, y: 4, z: 1, core: 2. Of those that a mesh axis runs over, the one named last changes fastest.
The devices are a block of a 4x4x8 slice.
Arguments:
- x_in: bfloat16 [4096, 7168], P('dp', 'my')
- gain_attn: bfloat16 [7168], P('my')
- w_q: bfloat16 [7168, 56, 128], P('my', 'mx')
- w_k: bfloat16 [7168, 8, 128], P('my', 'mx')
- w_v: bfloat16 [7168, 8, 128], P('my', 'mx')
- w_o: bfloat16 [56, 128, 7168], P('mx', None, 'my')
- gain_mlp: bfloat16 [7168], P('my')
- w_gate: bfloat16 [7168, 20480], P('my', 'mx')
- w_up: bfloat16 [7168, 20480], P('my', 'mx')
- w_down: bfloat16 [20480, 7168], P('mx', 'my')
Outputs:
- output: bfloat16 [4096, 7168], P('dp', 'my')
All inputs are finite; a program needn't handle non-finite values.
Results may differ from the reference program's by a relative error of at most 0.0138619.
Values are sent between devices in bfloat16 or wider.
A program may use at most 768 MiB of HBM per device.

```python
import jax
import jax.numpy as jnp
from jax import lax

TOKENS = 4096
D = 7168
HEADS = 56
KV_HEADS = 8
HEAD = 128
FF = 20480

ROPE_BASE = 10000.0
NORM_EPS = 1e-6
QBLOCK = min(TOKENS, 128)
GROUPS = HEADS // KV_HEADS
HALF_DIM = HEAD // 2


def weight_normal(key_w, fan_in, shape_w):
    return (jax.random.normal(key_w, shape_w, jnp.float32) * fan_in ** -0.5).astype(jnp.bfloat16)


def setup_inputs(seed: int = 0, part: int = 0) -> dict:
    base_key = jax.random.key(seed)
    part_keys = jax.random.split(jax.random.fold_in(base_key, part), 4)
    shared_keys = jax.random.split(base_key, 9)
    col_frac = jnp.arange(D, dtype=jnp.float32) / D
    slope_val = jax.random.uniform(part_keys[0], (), jnp.float32, 1.5, 2.5)
    col_scale = jnp.exp(slope_val * (col_frac - 0.5) - 0.2)
    phase_start = jax.random.uniform(part_keys[1], (), jnp.float32, 0.0, 6.28)
    phase_t = 3.0 * jnp.arange(TOKENS, dtype=jnp.float32) / TOKENS + phase_start
    drift_dirs = jax.random.normal(part_keys[2], (2, D), jnp.float32)
    drift_val = jnp.cos(phase_t)[:, None] * drift_dirs[0][None, :] + jnp.sin(phase_t)[:, None] * drift_dirs[1][None, :]
    noise_val = jax.random.normal(part_keys[3], (TOKENS, D), jnp.float32)
    x_in = (col_scale[None, :] * (noise_val + 0.8 * drift_val)).astype(jnp.bfloat16)
    gain_attn = (0.5 + jax.random.uniform(shared_keys[0], (D,), jnp.float32)).astype(jnp.bfloat16)
    w_q = weight_normal(shared_keys[1], D, (D, HEADS, HEAD))
    w_k = weight_normal(shared_keys[2], D, (D, KV_HEADS, HEAD))
    w_v = weight_normal(shared_keys[3], D, (D, KV_HEADS, HEAD))
    w_o = weight_normal(shared_keys[4], HEADS * HEAD, (HEADS, HEAD, D))
    gain_mlp = (0.5 + jax.random.uniform(shared_keys[5], (D,), jnp.float32)).astype(jnp.bfloat16)
    w_gate = weight_normal(shared_keys[6], D, (D, FF))
    w_up = weight_normal(shared_keys[7], D, (D, FF))
    w_down = weight_normal(shared_keys[8], FF, (FF, D))
    return {"x_in": x_in, "gain_attn": gain_attn, "w_q": w_q, "w_k": w_k, "w_v": w_v, "w_o": w_o, "gain_mlp": gain_mlp, "w_gate": w_gate, "w_up": w_up, "w_down": w_down}


def rms_norm(values, gain):
    values_f = values.astype(jnp.float32)
    mean_sq = jnp.mean(values_f * values_f, axis=-1, keepdims=True)
    return (values_f * lax.rsqrt(mean_sq + NORM_EPS) * gain.astype(jnp.float32)).astype(jnp.bfloat16)


def apply_rope(values, positions):
    inv_freq = ROPE_BASE ** (-jnp.arange(HALF_DIM, dtype=jnp.float32) / HALF_DIM)
    angles = positions[:, None] * inv_freq[None, :]
    cos_t = jnp.cos(angles)[:, None, :]
    sin_t = jnp.sin(angles)[:, None, :]
    values_f = values.astype(jnp.float32)
    first_half = values_f[..., :HALF_DIM]
    second_half = values_f[..., HALF_DIM:]
    return jnp.concatenate([first_half * cos_t - second_half * sin_t, second_half * cos_t + first_half * sin_t], axis=-1).astype(jnp.bfloat16)


def reference(x_in, gain_attn, w_q, w_k, w_v, w_o, gain_mlp, w_gate, w_up, w_down):
    normed = rms_norm(x_in, gain_attn)
    q_heads = jnp.dot(normed, w_q.reshape(D, HEADS * HEAD), preferred_element_type=jnp.float32).astype(jnp.bfloat16).reshape(TOKENS, HEADS, HEAD)
    k_heads = jnp.dot(normed, w_k.reshape(D, KV_HEADS * HEAD), preferred_element_type=jnp.float32).astype(jnp.bfloat16).reshape(TOKENS, KV_HEADS, HEAD)
    v_heads = jnp.dot(normed, w_v.reshape(D, KV_HEADS * HEAD), preferred_element_type=jnp.float32).astype(jnp.bfloat16).reshape(TOKENS, KV_HEADS, HEAD)
    positions = jnp.arange(TOKENS, dtype=jnp.float32)
    q_rot = apply_rope(q_heads, positions)
    k_float = apply_rope(k_heads, positions).astype(jnp.float32)
    v_float = v_heads.astype(jnp.float32)
    q_blocks = q_rot.reshape(TOKENS // QBLOCK, QBLOCK, KV_HEADS, GROUPS, HEAD)
    key_pos = jnp.arange(TOKENS)

    def attend(blk_args):
        q_blk, blk_idx = blk_args
        scores = jnp.einsum("qkgd,tkd->qkgt", q_blk.astype(jnp.float32), k_float) * HEAD ** -0.5
        query_pos = blk_idx * QBLOCK + jnp.arange(QBLOCK)
        causal = key_pos[None, :] <= query_pos[:, None]
        scores = jnp.where(causal[:, None, None, :], scores, -jnp.inf)
        attn_prob = jax.nn.softmax(scores, axis=-1).astype(jnp.bfloat16)
        blk_out = jnp.einsum("qkgt,tkd->qkgd", attn_prob.astype(jnp.float32), v_float)
        return blk_out.astype(jnp.bfloat16).reshape(QBLOCK, HEADS * HEAD)

    attn_heads = lax.map(attend, (q_blocks, jnp.arange(TOKENS // QBLOCK))).reshape(TOKENS, HEADS * HEAD)
    attn_proj = jnp.dot(attn_heads, w_o.reshape(HEADS * HEAD, D), preferred_element_type=jnp.float32)
    residual = (x_in.astype(jnp.float32) + attn_proj).astype(jnp.bfloat16)
    normed_mlp = rms_norm(residual, gain_mlp)
    gate_val = jnp.dot(normed_mlp, w_gate, preferred_element_type=jnp.float32)
    up_val = jnp.dot(normed_mlp, w_up, preferred_element_type=jnp.float32)
    act_val = (jax.nn.silu(gate_val) * up_val).astype(jnp.bfloat16)
    down_val = jnp.dot(act_val, w_down, preferred_element_type=jnp.float32)
    return (residual.astype(jnp.float32) + down_val).astype(jnp.bfloat16)
```

```python
import functools

import jax
import jax.numpy as jnp
from jax import lax
from jax.experimental import pallas as pl
from jax.experimental.pallas import tpu as pltpu
from jax.sharding import PartitionSpec as P

ROPE_BASE = 10000.0
NORM_EPS = 1e-6
CHUNK = 512
MESH = pl.DeviceIdType.MESH
F32 = jnp.float32
BF16 = jnp.bfloat16


def apply_rope(values, positions):
    half_dim = values.shape[-1] // 2
    inv_freq = ROPE_BASE ** (-jnp.arange(half_dim, dtype=jnp.float32) / half_dim)
    angles = positions[:, None] * inv_freq[None, :]
    cos_t = jnp.cos(angles)[:, None, :]
    sin_t = jnp.sin(angles)[:, None, :]
    values_f = values.astype(jnp.float32)
    first_half = values_f[..., :half_dim]
    second_half = values_f[..., half_dim:]
    return jnp.concatenate([first_half * cos_t - second_half * sin_t, second_half * cos_t + first_half * sin_t], axis=-1).astype(jnp.bfloat16)


def attend_local(q_rot, k_full, v_full, query_pos):
    q_tokens, heads_loc, head_dim = q_rot.shape
    kv_loc = k_full.shape[1]
    q_grp = q_rot.reshape(q_tokens, kv_loc, heads_loc // kv_loc, head_dim)
    scores = jnp.einsum("qkgd,tkd->qkgt", q_grp, k_full, preferred_element_type=jnp.float32) * head_dim ** -0.5
    key_pos = jnp.arange(k_full.shape[0])
    causal = key_pos[None, :] <= query_pos[:, None]
    scores = jnp.where(causal[:, None, None, :], scores, -jnp.inf)
    attn_prob = jax.nn.softmax(scores, axis=-1).astype(jnp.bfloat16)
    attn_out = jnp.einsum("qkgt,tkd->qkgd", attn_prob, v_full, preferred_element_type=jnp.float32)
    return attn_out.astype(jnp.bfloat16).reshape(q_tokens, heads_loc, head_dim)


class Place:
    def __init__(self):
        self.y = lax.axis_index("my")
        mx = lax.axis_index("mx")
        self.x = mx // 2
        self.core = mx % 2
        self.yp = (self.y + 1) % 4
        self.ym = (self.y + 3) % 4
        self.yo = (self.y + 2) % 4
        self.xp = (self.x + 1) % 4
        self.xm = (self.x + 3) % 4
        self.xo = (self.x + 2) % 4
        self.dev_yp = {"my": self.yp}
        self.dev_ym = {"my": self.ym}
        self.dev_xp = {"mx": self.xp * 2 + self.core}
        self.dev_xm = {"mx": self.xm * 2 + self.core}
        self.dev_core = {"mx": self.x * 2 + (1 - self.core)}
        self.partners = (self.dev_yp, self.dev_ym, self.dev_xp, self.dev_xm, self.dev_core)

    def entry(self):
        barrier = pltpu.get_barrier_semaphore()
        for dev in self.partners:
            pl.semaphore_signal(barrier, inc=1, device_id=dev, device_id_type=MESH)
        pl.semaphore_wait(barrier, len(self.partners))

    def give_credit(self, credit):
        for slot, dev in ((1, self.dev_yp), (0, self.dev_ym), (3, self.dev_xp), (2, self.dev_xm), (4, self.dev_core)):
            pl.semaphore_signal(credit.at[slot], inc=1, device_id=dev, device_id_type=MESH)

    def take_credit(self, credit):
        for slot in range(5):
            pl.semaphore_wait(credit.at[slot], 1)


def rcopy(src, dst, send_sem, recv_sem, dev):
    return pltpu.make_async_remote_copy(src_ref=src, dst_ref=dst, send_sem=send_sem, recv_sem=recv_sem, device_id=dev, device_id_type=MESH)


def rows(start, size, align):
    return pl.ds(pl.multiple_of(start, align), size)


def mlp_kernel(n_chunks, m_hbm, h_hbm, wg_hbm, wu_hbm, wd_hbm, y_hbm, WG, WU, WD, M, PP, R1, R2, ACT, DP, DR, XR1, XR2, YB, H,
               w_sem, m_sem, h_sem, y_sem, credit, s1s, s1r, s2s, s2r, acs, acr, fws, fwr, dds, ddr, x1s, x1r, x2s, x2r, xas, xar, xfs, xfr, dys, dyr):
    at = Place()
    tc, width = M.shape
    ff = WG.shape[1]
    qb = tc // 4
    hq = qb // 2
    hb = tc // 2
    xb = hb // 4
    hx = xb // 2
    gu_tiles = 5
    gu_w = ff // gu_tiles
    dn_w = 256 if width % 256 == 0 else 128

    w_copies = [pltpu.make_async_copy(s, d, w_sem.at[i]) for i, (s, d) in enumerate(((wg_hbm, WG), (wu_hbm, WU), (wd_hbm, WD)))]
    for c in w_copies:
        c.start()

    def m_copy(c):
        return pltpu.make_async_copy(m_hbm.at[rows(c * tc, tc, tc)], M, m_sem)

    m_copy(0).start()
    at.entry()

    def gu_part(par, lo, hi):
        @pl.loop(lo, hi)
        def _(n):
            g_cols = rows(n * gu_w, gu_w, 128)
            PP[par, :, g_cols] = jnp.dot(M[...], WG[:, g_cols], preferred_element_type=F32).astype(BF16)
            PP[par, :, rows(ff + n * gu_w, gu_w, 128)] = jnp.dot(M[...], WU[:, g_cols], preferred_element_type=F32).astype(BF16)

    def s1_copies(par):
        o = at.yo * qb
        return (rcopy(PP.at[par, rows(o, hq, hq)], R1.at[0], s1s.at[0], s1r.at[0], at.dev_yp),
                rcopy(PP.at[par, rows(o + hq, hq, hq)], R1.at[1], s1s.at[1], s1r.at[1], at.dev_ym))

    def s2_copies(par):
        return (rcopy(PP.at[par, rows(at.yp * qb, qb, qb)], R2.at[par, 0], s2s.at[par, 0], s2r.at[par, 0], at.dev_yp),
                rcopy(PP.at[par, rows(at.ym * qb, qb, qb)], R2.at[par, 1], s2s.at[par, 1], s2r.at[par, 1], at.dev_ym))

    def act_copies(par):
        own = ACT.at[par, rows(at.y * qb, qb, qb)]
        return (rcopy(own, own, acs.at[0], acr.at[0], at.dev_yp), rcopy(own, own, acs.at[1], acr.at[1], at.dev_ym))

    def fwd_copies(par):
        a = ACT.at[par, rows(at.ym * qb, hq, hq)]
        b = ACT.at[par, rows(at.yp * qb + hq, hq, hq)]
        return (rcopy(a, a, fws.at[par, 0], fwr.at[par, 0], at.dev_yp), rcopy(b, b, fws.at[par, 1], fwr.at[par, 1], at.dev_ym))

    def dd_copy():
        return rcopy(DP.at[rows((1 - at.core) * hb, hb, hb)], DR, dds, ddr, at.dev_core)

    own_half = at.core * hb

    def x1_copies():
        o = own_half + at.xo * xb
        return (rcopy(DP.at[rows(o, hx, hx)], XR1.at[0], x1s.at[0], x1r.at[0], at.dev_xp),
                rcopy(DP.at[rows(o + hx, hx, hx)], XR1.at[1], x1s.at[1], x1r.at[1], at.dev_xm))

    def x2_copies():
        return (rcopy(DP.at[rows(own_half + at.xp * xb, xb, xb)], XR2.at[0], x2s.at[0], x2r.at[0], at.dev_xp),
                rcopy(DP.at[rows(own_half + at.xm * xb, xb, xb)], XR2.at[1], x2s.at[1], x2r.at[1], at.dev_xm))

    def yblk(b):
        return YB.at[rows(own_half + b * xb, xb, xb)]

    def xa_copies():
        own = yblk(at.x)
        return (rcopy(own, own, xas.at[0], xar.at[0], at.dev_xp), rcopy(own, own, xas.at[1], xar.at[1], at.dev_xm))

    def xf_copies():
        a = YB.at[rows(own_half + at.xm * xb, hx, hx)]
        b = YB.at[rows(own_half + at.xp * xb + hx, hx, hx)]
        return (rcopy(a, a, xfs.at[0], xfr.at[0], at.dev_xp), rcopy(b, b, xfs.at[1], xfr.at[1], at.dev_xm))

    def dy_copy(i):
        b = (at.x, at.xm, at.xp, at.xo)[i]
        return rcopy(yblk(b), yblk(b), dys.at[i], dyr.at[i], at.dev_core)

    def dy_wait_recv(i):
        b = (at.x, at.xm, at.xp, at.xo)[i]
        other = YB.at[rows((1 - at.core) * hb + b * xb, xb, xb)]
        rcopy(other, other, dys.at[i], dyr.at[i], at.dev_core).wait_recv()

    def h_copy(c):
        return pltpu.make_async_copy(h_hbm.at[rows(c * tc + own_half + at.x * xb, xb, xb)], H, h_sem)

    def y_copy(c):
        return pltpu.make_async_copy(YB, y_hbm.at[rows(c * tc, tc, tc)], y_sem)

    def start(copies):
        for c in copies:
            c.start()

    def wait(copies):
        for c in copies:
            c.wait()

    w_copies[0].wait()
    w_copies[1].wait()
    m_copy(0).wait()
    gu_part(0, 0, gu_tiles)
    w_copies[2].wait()

    @pl.loop(0, n_chunks + 2)
    def _(k):
        par = k % 2
        alt = (k + 1) % 2
        has_s = k < n_chunks
        has_gu = k + 1 < n_chunks
        has_a = jnp.logical_and(k >= 1, k - 1 < n_chunks)
        has_d = k >= 2

        @pl.when(k >= 1)
        def _():
            at.take_credit(credit)

        @pl.when(has_s)
        def _():
            start(s1_copies(par))

        @pl.when(has_gu)
        def _():
            m_copy(k + 1).start()

        @pl.when(has_d)
        def _():
            h_copy(k - 2).start()

        @pl.when(has_a)
        def _():
            wait(s2_copies(alt))
            base = at.y * qb
            step = 16

            @pl.loop(0, qb // step)
            def _(i):
                r = rows(base + i * step, step, step)
                r2 = rows(i * step, step, step)
                g = PP[alt, r, 0:ff].astype(F32) + R2[alt, 0, r2, 0:ff].astype(F32) + R2[alt, 1, r2, 0:ff].astype(F32)
                u = PP[alt, r, ff:2 * ff].astype(F32) + R2[alt, 0, r2, ff:2 * ff].astype(F32) + R2[alt, 1, r2, ff:2 * ff].astype(F32)
                ACT[alt, r, :] = (g * jax.nn.sigmoid(g) * u).astype(BF16)

            start(act_copies(alt))

        @pl.when(has_d)
        def _():
            wait(fwd_copies(par))

            @pl.loop(0, width // dn_w)
            def _(n):
                cols = rows(n * dn_w, dn_w, 128)
                DP[:, cols] = jnp.dot(ACT[par], WD[:, cols], preferred_element_type=F32).astype(BF16)

            dd_copy().start()

        @pl.when(has_s)
        def _():
            wait(s1_copies(par))
            step = 16

            @pl.loop(0, hq // step)
            def _(i):
                ri = rows(i * step, step, step)
                ra = rows(at.yp * qb + i * step, step, step)
                rb = rows(at.ym * qb + hq + i * step, step, step)
                PP[par, ra, :] = (PP[par, ra, :].astype(F32) + R1[0, ri, :].astype(F32)).astype(BF16)
                PP[par, rb, :] = (PP[par, rb, :].astype(F32) + R1[1, ri, :].astype(F32)).astype(BF16)

            start(s2_copies(par))

        @pl.when(has_d)
        def _():
            dd_copy().wait()
            step = 16

            @pl.loop(0, hb // step)
            def _(i):
                ri = rows(i * step, step, step)
                ra = rows(own_half + i * step, step, step)
                DP[ra, :] = (DP[ra, :].astype(F32) + DR[ri, :].astype(F32)).astype(BF16)

            start(x1_copies())

        @pl.when(has_gu)
        def _():
            m_copy(k + 1).wait()
            gu_part(alt, 0, 2)

        @pl.when(has_d)
        def _():
            wait(x1_copies())
            ra = rows(own_half + at.xp * xb, hx, hx)
            rb = rows(own_half + at.xm * xb + hx, hx, hx)
            DP[ra, :] = (DP[ra, :].astype(F32) + XR1[0].astype(F32)).astype(BF16)
            DP[rb, :] = (DP[rb, :].astype(F32) + XR1[1].astype(F32)).astype(BF16)
            start(x2_copies())

        @pl.when(has_gu)
        def _():
            gu_part(alt, 2, 3)

        @pl.when(has_a)
        def _():
            wait(act_copies(alt))
            start(fwd_copies(alt))

        @pl.when(has_d)
        def _():
            wait(x2_copies())
            h_copy(k - 2).wait()
            r = rows(own_half + at.x * xb, xb, xb)
            down = DP[r, :].astype(F32) + XR2[0].astype(F32) + XR2[1].astype(F32)
            YB[r, :] = (H[...].astype(F32) + down).astype(BF16)
            start(xa_copies())
            dy_copy(0).start()

        @pl.when(has_gu)
        def _():
            gu_part(alt, 3, 4)

        @pl.when(has_d)
        def _():
            wait(xa_copies())
            start(xf_copies())
            dy_copy(1).start()
            dy_copy(2).start()

        @pl.when(has_gu)
        def _():
            gu_part(alt, 4, 5)

        @pl.when(has_d)
        def _():
            wait(xf_copies())
            dy_copy(3).start()
            for i in range(4):
                dy_copy(i).wait_send()
                dy_wait_recv(i)
            y_copy(k - 2).start()
            y_copy(k - 2).wait()

        @pl.when(k < n_chunks + 1)
        def _():
            at.give_credit(credit)


def mlp_phase(m_full, h_full, w_gate, w_up, w_down, chunk):
    tokens, width = m_full.shape
    ff = w_gate.shape[1]
    n_chunks = tokens // chunk
    qb, hb = chunk // 4, chunk // 2
    xb = hb // 4
    hbm = pl.BlockSpec(memory_space=pl.ANY)
    sem = pltpu.SemaphoreType.DMA
    vm = lambda *s: pltpu.VMEM(s, BF16)
    return pl.pallas_call(
        functools.partial(mlp_kernel, n_chunks),
        out_shape=jax.ShapeDtypeStruct((tokens, width), BF16),
        in_specs=[hbm] * 5,
        out_specs=hbm,
        scratch_shapes=[
            vm(width, ff), vm(width, ff), vm(ff, width), vm(chunk, width), vm(2, chunk, 2 * ff),
            vm(2, qb // 2, 2 * ff), vm(2, 2, qb, 2 * ff), vm(2, chunk, ff), vm(chunk, width), vm(hb, width),
            vm(2, xb // 2, width), vm(2, xb, width), vm(chunk, width), vm(xb, width),
            sem((3,)), sem, sem, sem, pltpu.SemaphoreType.REGULAR((5,)),
            sem((2,)), sem((2,)), sem((2, 2)), sem((2, 2)), sem((2,)), sem((2,)), sem((2, 2)), sem((2, 2)),
            sem, sem, sem((2,)), sem((2,)), sem((2,)), sem((2,)), sem((2,)), sem((2,)), sem((2,)), sem((2,)), sem((4,)), sem((4,)),
        ],
        compiler_params=pltpu.CompilerParams(collective_id=1, has_side_effects=True, vmem_limit_bytes=67043328),
        name="mlp_phase",
    )(m_full, h_full, w_gate, w_up, w_down)


def solution(mesh, chunk=CHUNK):
    my_size = mesh.shape["my"]

    def width_norm(values, gain, width):
        values_f = values.astype(jnp.float32)
        row_sq = lax.psum(jnp.sum(values_f * values_f, axis=-1, keepdims=True), "my")
        return (values_f * lax.rsqrt(row_sq / width + NORM_EPS) * gain.astype(jnp.float32)).astype(jnp.bfloat16)

    def local_layer(x_in, gain_attn, w_q, w_k, w_v, w_o, gain_mlp, w_gate, w_up, w_down):
        tokens = x_in.shape[0]
        width = x_in.shape[1] * my_size
        q_tokens = tokens // my_size
        row_idx = lax.axis_index("my")
        normed = width_norm(x_in, gain_attn, width)
        q_part = jnp.einsum("td,dhe->the", normed, w_q, preferred_element_type=jnp.float32).astype(jnp.bfloat16)
        k_part = jnp.einsum("td,dhe->the", normed, w_k, preferred_element_type=jnp.float32).astype(jnp.bfloat16)
        v_part = jnp.einsum("td,dhe->the", normed, w_v, preferred_element_type=jnp.float32).astype(jnp.bfloat16)
        q_loc = lax.psum_scatter(q_part, "my", scatter_dimension=0, tiled=True)
        k_loc = lax.psum_scatter(k_part, "my", scatter_dimension=0, tiled=True)
        v_loc = lax.psum_scatter(v_part, "my", scatter_dimension=0, tiled=True)
        query_pos = row_idx * q_tokens + jnp.arange(q_tokens)
        q_rot = apply_rope(q_loc, query_pos.astype(jnp.float32))
        k_rot = apply_rope(k_loc, query_pos.astype(jnp.float32))
        k_full = lax.all_gather(k_rot, "my", axis=0, tiled=True)
        v_full = lax.all_gather(v_loc, "my", axis=0, tiled=True)
        attn_loc = attend_local(q_rot, k_full, v_full, query_pos)
        attn_all = lax.all_gather(attn_loc, "my", axis=0, tiled=True)
        attn_part = jnp.einsum("the,hed->td", attn_all, w_o, preferred_element_type=jnp.float32).astype(jnp.bfloat16)
        attn_sum = lax.psum(attn_part, "mx")
        residual = (x_in.astype(jnp.float32) + attn_sum.astype(jnp.float32)).astype(jnp.bfloat16)
        normed_mlp = width_norm(residual, gain_mlp, width)
        return mlp_phase(normed_mlp, residual, w_gate, w_up, w_down, chunk)

    in_specs = (P("dp", "my"), P("my"), P("my", "mx", None), P("my", "mx", None), P("my", "mx", None), P("mx", None, "my"), P("my"), P("my", "mx"), P("my", "mx"), P("mx", "my"))
    return jax.shard_map(local_layer, mesh=mesh, in_specs=in_specs, out_specs=P("dp", "my"), check_vma=False)
```

```python
import functools

import jax
import jax.numpy as jnp
from jax import lax
from jax.experimental import pallas as pl
from jax.experimental.pallas import tpu as pltpu
from jax.sharding import PartitionSpec as P

ROPE_BASE = 10000.0
NORM_EPS = 1e-6
CHUNK = 512
MESH = pl.DeviceIdType.MESH
F32 = jnp.float32
BF16 = jnp.bfloat16


class Place:
    def __init__(self):
        self.y = lax.axis_index("my")
        mx = lax.axis_index("mx")
        self.x = mx // 2
        self.core = mx % 2
        self.yp = (self.y + 1) % 4
        self.ym = (self.y + 3) % 4
        self.yo = (self.y + 2) % 4
        self.xp = (self.x + 1) % 4
        self.xm = (self.x + 3) % 4
        self.xo = (self.x + 2) % 4
        self.dev_yp = {"my": self.yp}
        self.dev_ym = {"my": self.ym}
        self.dev_xp = {"mx": self.xp * 2 + self.core}
        self.dev_xm = {"mx": self.xm * 2 + self.core}
        self.dev_core = {"mx": self.x * 2 + (1 - self.core)}
        self.partners = (self.dev_yp, self.dev_ym, self.dev_xp, self.dev_xm, self.dev_core)

    def entry(self, extra=()):
        barrier = pltpu.get_barrier_semaphore()
        for dev in self.partners + extra:
            pl.semaphore_signal(barrier, inc=1, device_id=dev, device_id_type=MESH)
        pl.semaphore_wait(barrier, len(self.partners) + len(extra))

    def give_credit(self, credit):
        for slot, dev in ((1, self.dev_yp), (0, self.dev_ym), (3, self.dev_xp), (2, self.dev_xm), (4, self.dev_core)):
            pl.semaphore_signal(credit.at[slot], inc=1, device_id=dev, device_id_type=MESH)

    def take_credit(self, credit):
        for slot in range(5):
            pl.semaphore_wait(credit.at[slot], 1)


def rcopy(src, dst, send_sem, recv_sem, dev):
    return pltpu.make_async_remote_copy(src_ref=src, dst_ref=dst, send_sem=send_sem, recv_sem=recv_sem, device_id=dev, device_id_type=MESH)


def rows(start, size, align):
    return pl.ds(pl.multiple_of(start, align), size)


def mlp_kernel(n_chunks, m_hbm, h_hbm, wg_hbm, wu_hbm, wd_hbm, y_hbm, WG, WU, WD, M, PP, R1, R2, ACT, DP, DR, XR1, XR2, YB, H,
               w_sem, m_sem, h_sem, y_sem, credit, s1s, s1r, s2s, s2r, acs, acr, fws, fwr, dds, ddr, x1s, x1r, x2s, x2r, xas, xar, xfs, xfr, dys, dyr):
    at = Place()
    tc, width = M.shape
    ff = WG.shape[1]
    qb = tc // 4
    hq = qb // 2
    hb = tc // 2
    xb = hb // 4
    hx = xb // 2
    gu_tiles = 5
    gu_w = ff // gu_tiles
    dn_w = 256 if width % 256 == 0 else 128

    w_copies = [pltpu.make_async_copy(s, d, w_sem.at[i]) for i, (s, d) in enumerate(((wg_hbm, WG), (wu_hbm, WU), (wd_hbm, WD)))]
    for c in w_copies:
        c.start()

    def m_copy(c):
        return pltpu.make_async_copy(m_hbm.at[rows(c * tc, tc, tc)], M, m_sem)

    m_copy(0).start()
    at.entry()

    def gu_part(par, lo, hi):
        @pl.loop(lo, hi)
        def _(n):
            g_cols = rows(n * gu_w, gu_w, 128)
            PP[par, :, g_cols] = jnp.dot(M[...], WG[:, g_cols], preferred_element_type=F32).astype(BF16)
            PP[par, :, rows(ff + n * gu_w, gu_w, 128)] = jnp.dot(M[...], WU[:, g_cols], preferred_element_type=F32).astype(BF16)

    def s1_copies(par):
        o = at.yo * qb
        return (rcopy(PP.at[par, rows(o, hq, hq)], R1.at[0], s1s.at[0], s1r.at[0], at.dev_yp),
                rcopy(PP.at[par, rows(o + hq, hq, hq)], R1.at[1], s1s.at[1], s1r.at[1], at.dev_ym))

    def s2_copies(par):
        return (rcopy(PP.at[par, rows(at.yp * qb, qb, qb)], R2.at[par, 0], s2s.at[par, 0], s2r.at[par, 0], at.dev_yp),
                rcopy(PP.at[par, rows(at.ym * qb, qb, qb)], R2.at[par, 1], s2s.at[par, 1], s2r.at[par, 1], at.dev_ym))

    def act_copies(par):
        own = ACT.at[par, rows(at.y * qb, qb, qb)]
        return (rcopy(own, own, acs.at[0], acr.at[0], at.dev_yp), rcopy(own, own, acs.at[1], acr.at[1], at.dev_ym))

    def fwd_copies(par):
        a = ACT.at[par, rows(at.ym * qb, hq, hq)]
        b = ACT.at[par, rows(at.yp * qb + hq, hq, hq)]
        return (rcopy(a, a, fws.at[par, 0], fwr.at[par, 0], at.dev_yp), rcopy(b, b, fws.at[par, 1], fwr.at[par, 1], at.dev_ym))

    def dd_copy():
        return rcopy(DP.at[rows((1 - at.core) * hb, hb, hb)], DR, dds, ddr, at.dev_core)

    own_half = at.core * hb

    def x1_copies():
        o = own_half + at.xo * xb
        return (rcopy(DP.at[rows(o, hx, hx)], XR1.at[0], x1s.at[0], x1r.at[0], at.dev_xp),
                rcopy(DP.at[rows(o + hx, hx, hx)], XR1.at[1], x1s.at[1], x1r.at[1], at.dev_xm))

    def x2_copies():
        return (rcopy(DP.at[rows(own_half + at.xp * xb, xb, xb)], XR2.at[0], x2s.at[0], x2r.at[0], at.dev_xp),
                rcopy(DP.at[rows(own_half + at.xm * xb, xb, xb)], XR2.at[1], x2s.at[1], x2r.at[1], at.dev_xm))

    def yblk(b):
        return YB.at[rows(own_half + b * xb, xb, xb)]

    def xa_copies():
        own = yblk(at.x)
        return (rcopy(own, own, xas.at[0], xar.at[0], at.dev_xp), rcopy(own, own, xas.at[1], xar.at[1], at.dev_xm))

    def xf_copies():
        a = YB.at[rows(own_half + at.xm * xb, hx, hx)]
        b = YB.at[rows(own_half + at.xp * xb + hx, hx, hx)]
        return (rcopy(a, a, xfs.at[0], xfr.at[0], at.dev_xp), rcopy(b, b, xfs.at[1], xfr.at[1], at.dev_xm))

    def dy_copy(i):
        b = (at.x, at.xm, at.xp, at.xo)[i]
        return rcopy(yblk(b), yblk(b), dys.at[i], dyr.at[i], at.dev_core)

    def dy_wait_recv(i):
        b = (at.x, at.xm, at.xp, at.xo)[i]
        other = YB.at[rows((1 - at.core) * hb + b * xb, xb, xb)]
        rcopy(other, other, dys.at[i], dyr.at[i], at.dev_core).wait_recv()

    def h_copy(c):
        return pltpu.make_async_copy(h_hbm.at[rows(c * xb, xb, xb)], H, h_sem)

    def y_copy(c):
        return pltpu.make_async_copy(YB, y_hbm.at[rows(c * tc, tc, tc)], y_sem)

    def start(copies):
        for c in copies:
            c.start()

    def wait(copies):
        for c in copies:
            c.wait()

    w_copies[0].wait()
    w_copies[1].wait()
    m_copy(0).wait()
    gu_part(0, 0, gu_tiles)
    w_copies[2].wait()

    @pl.loop(0, n_chunks + 2)
    def _(k):
        par = k % 2
        alt = (k + 1) % 2
        has_s = k < n_chunks
        has_gu = k + 1 < n_chunks
        has_a = jnp.logical_and(k >= 1, k - 1 < n_chunks)
        has_d = k >= 2

        @pl.when(k >= 1)
        def _():
            at.take_credit(credit)

        @pl.when(has_s)
        def _():
            start(s1_copies(par))

        @pl.when(has_gu)
        def _():
            m_copy(k + 1).start()

        @pl.when(has_d)
        def _():
            h_copy(k - 2).start()

        @pl.when(has_a)
        def _():
            wait(s2_copies(alt))
            base = at.y * qb
            step = 16

            @pl.loop(0, qb // step)
            def _(i):
                r = rows(base + i * step, step, step)
                r2 = rows(i * step, step, step)
                g = PP[alt, r, 0:ff].astype(F32) + R2[alt, 0, r2, 0:ff].astype(F32) + R2[alt, 1, r2, 0:ff].astype(F32)
                u = PP[alt, r, ff:2 * ff].astype(F32) + R2[alt, 0, r2, ff:2 * ff].astype(F32) + R2[alt, 1, r2, ff:2 * ff].astype(F32)
                ACT[alt, r, :] = (g * jax.nn.sigmoid(g) * u).astype(BF16)

            start(act_copies(alt))

        @pl.when(has_d)
        def _():
            wait(fwd_copies(par))

            @pl.loop(0, width // dn_w)
            def _(n):
                cols = rows(n * dn_w, dn_w, 128)
                DP[:, cols] = jnp.dot(ACT[par], WD[:, cols], preferred_element_type=F32).astype(BF16)

            dd_copy().start()

        @pl.when(has_s)
        def _():
            wait(s1_copies(par))
            step = 16

            @pl.loop(0, hq // step)
            def _(i):
                ri = rows(i * step, step, step)
                ra = rows(at.yp * qb + i * step, step, step)
                rb = rows(at.ym * qb + hq + i * step, step, step)
                PP[par, ra, :] = (PP[par, ra, :].astype(F32) + R1[0, ri, :].astype(F32)).astype(BF16)
                PP[par, rb, :] = (PP[par, rb, :].astype(F32) + R1[1, ri, :].astype(F32)).astype(BF16)

            start(s2_copies(par))

        @pl.when(has_d)
        def _():
            dd_copy().wait()
            step = 16

            @pl.loop(0, hb // step)
            def _(i):
                ri = rows(i * step, step, step)
                ra = rows(own_half + i * step, step, step)
                DP[ra, :] = (DP[ra, :].astype(F32) + DR[ri, :].astype(F32)).astype(BF16)

            start(x1_copies())

        @pl.when(has_gu)
        def _():
            m_copy(k + 1).wait()
            gu_part(alt, 0, 2)

        @pl.when(has_d)
        def _():
            wait(x1_copies())
            ra = rows(own_half + at.xp * xb, hx, hx)
            rb = rows(own_half + at.xm * xb + hx, hx, hx)
            DP[ra, :] = (DP[ra, :].astype(F32) + XR1[0].astype(F32)).astype(BF16)
            DP[rb, :] = (DP[rb, :].astype(F32) + XR1[1].astype(F32)).astype(BF16)
            start(x2_copies())

        @pl.when(has_gu)
        def _():
            gu_part(alt, 2, 3)

        @pl.when(has_a)
        def _():
            wait(act_copies(alt))
            start(fwd_copies(alt))

        @pl.when(has_d)
        def _():
            wait(x2_copies())
            h_copy(k - 2).wait()
            r = rows(own_half + at.x * xb, xb, xb)
            down = DP[r, :].astype(F32) + XR2[0].astype(F32) + XR2[1].astype(F32)
            YB[r, :] = (H[...].astype(F32) + down).astype(BF16)
            start(xa_copies())
            dy_copy(0).start()

        @pl.when(has_gu)
        def _():
            gu_part(alt, 3, 4)

        @pl.when(has_d)
        def _():
            wait(xa_copies())
            start(xf_copies())
            dy_copy(1).start()
            dy_copy(2).start()

        @pl.when(has_gu)
        def _():
            gu_part(alt, 4, 5)

        @pl.when(has_d)
        def _():
            wait(xf_copies())
            dy_copy(3).start()
            for i in range(4):
                dy_copy(i).wait_send()
                dy_wait_recv(i)
            y_copy(k - 2).start()
            y_copy(k - 2).wait()

        @pl.when(k < n_chunks + 1)
        def _():
            at.give_credit(credit)


def mlp_phase(m_full, h_own, w_gate, w_up, w_down, chunk):
    tokens, width = m_full.shape
    ff = w_gate.shape[1]
    n_chunks = tokens // chunk
    qb, hb = chunk // 4, chunk // 2
    xb = hb // 4
    hbm = pl.BlockSpec(memory_space=pl.ANY)
    sem = pltpu.SemaphoreType.DMA
    vm = lambda *s: pltpu.VMEM(s, BF16)
    return pl.pallas_call(
        functools.partial(mlp_kernel, n_chunks),
        out_shape=jax.ShapeDtypeStruct((tokens, width), BF16),
        in_specs=[hbm] * 5,
        out_specs=hbm,
        scratch_shapes=[
            vm(width, ff), vm(width, ff), vm(ff, width), vm(chunk, width), vm(2, chunk, 2 * ff),
            vm(2, qb // 2, 2 * ff), vm(2, 2, qb, 2 * ff), vm(2, chunk, ff), vm(chunk, width), vm(hb, width),
            vm(2, xb // 2, width), vm(2, xb, width), vm(chunk, width), vm(xb, width),
            sem((3,)), sem, sem, sem, pltpu.SemaphoreType.REGULAR((5,)),
            sem((2,)), sem((2,)), sem((2, 2)), sem((2, 2)), sem((2,)), sem((2,)), sem((2, 2)), sem((2, 2)),
            sem, sem, sem((2,)), sem((2,)), sem((2,)), sem((2,)), sem((2,)), sem((2,)), sem((2,)), sem((2,)), sem((4,)), sem((4,)),
        ],
        compiler_params=pltpu.CompilerParams(collective_id=1, has_side_effects=True, vmem_limit_bytes=67043328),
        name="mlp_phase",
    )(m_full, h_own, w_gate, w_up, w_down)


def attn_kernel(n_chunks, x_hbm, ga, gm, cos_t, sin_t, wq_hbm, wk_hbm, wv_hbm, wo_hbm, m_hbm, h_hbm,
                WQKV, WO, X, N, QP, R1, R2, QS, KV, O, WP, DR, XR1, XR2, XH, HB, MO, SQ, RC, ST1, ST2,
                w_sem, x_sem, xh_sem, hb_sem, mo_sem, credit,
                t1s, t1r, s1s, s1r, s2s, s2r, kvs, kvr, ocs, ocr, ofs, ofr, dds, ddr, x1s, x1r, x2s, x2r, t2s, t2r, xas, xar, xfs, xfr, dms, dmr):
    at = Place()
    tc, width = N.shape
    full_width = width * 4
    qkv_w = WQKV.shape[1]
    head = 128
    heads = QS.shape[1] // (tc // 4)
    q_w = heads * head
    qb = tc // 4
    hq = qb // 2
    hb = tc // 2
    xb = hb // 4
    hx = xb // 2
    own_half = at.core * hb
    my_rows = own_half + at.x * xb
    peers = ((at.dev_yp, at.yp), (at.dev_ym, at.ym), ({"my": at.yo}, at.yo))
    blk = min(128, tc)
    n_blk = tc // blk
    step = 16

    w_copies = [
        pltpu.make_async_copy(wq_hbm, WQKV.at[:, pl.ds(0, q_w)], w_sem.at[0]),
        pltpu.make_async_copy(wk_hbm, WQKV.at[:, pl.ds(q_w, head)], w_sem.at[1]),
        pltpu.make_async_copy(wv_hbm, WQKV.at[:, pl.ds(q_w + head, head)], w_sem.at[2]),
        pltpu.make_async_copy(wo_hbm, WO, w_sem.at[3]),
    ]

    def x_copy(c):
        return pltpu.make_async_copy(x_hbm.at[rows(c * tc, tc, tc)], X.at[c % 2], x_sem.at[c % 2])

    x_copy(0).start()
    for c in w_copies:
        c.start()
    at.entry(extra=({"my": at.yo},))

    def slot(c):
        return c % 4

    def pair(c):
        return c % 2

    def stats_copies(st, ssem, rsem, c):
        own = st.at[c, at.y]
        return [rcopy(own, own, ssem.at[pair(c), i], rsem.at[c, i], dev) for i, (dev, _) in enumerate(peers)]

    def s1_copies(c):
        s, o = slot(c), at.yo * qb
        return [rcopy(QP.at[s, rows(o, hq, hq)], R1.at[s, 0], s1s.at[pair(c), 0], s1r.at[s, 0], at.dev_yp),
                rcopy(QP.at[s, rows(o + hq, hq, hq)], R1.at[s, 1], s1s.at[pair(c), 1], s1r.at[s, 1], at.dev_ym)]

    def s2_copies(c):
        s = slot(c)
        return [rcopy(QP.at[s, rows(at.yp * qb, qb, qb)], R2.at[s, 0], s2s.at[pair(c), 0], s2r.at[s, 0], at.dev_yp),
                rcopy(QP.at[s, rows(at.ym * qb, qb, qb)], R2.at[s, 1], s2s.at[pair(c), 1], s2r.at[s, 1], at.dev_ym)]

    def kv_copies(c):
        own = KV.at[rows(c * tc + at.y * qb, qb, qb)]
        return [rcopy(own, own, kvs.at[pair(c), i], kvr.at[c, i], dev) for i, (dev, _) in enumerate(peers)]

    def o_copies(c):
        s = slot(c)
        own = O.at[s, rows(at.y * qb, qb, qb)]
        return [rcopy(own, own, ocs.at[pair(c), 0], ocr.at[s, 0], at.dev_yp), rcopy(own, own, ocs.at[pair(c), 1], ocr.at[s, 1], at.dev_ym)]

    def of_copies(c):
        s = slot(c)
        a = O.at[s, rows(at.ym * qb, hq, hq)]
        b = O.at[s, rows(at.yp * qb + hq, hq, hq)]
        return [rcopy(a, a, ofs.at[pair(c), 0], ofr.at[s, 0], at.dev_yp), rcopy(b, b, ofs.at[pair(c), 1], ofr.at[s, 1], at.dev_ym)]

    def dd_copies(c):
        s = slot(c)
        return [rcopy(WP.at[s, rows((1 - at.core) * hb, hb, hb)], DR.at[s], dds.at[pair(c)], ddr.at[s], at.dev_core)]

    def x1_copies(c):
        s, o = slot(c), own_half + at.xo * xb
        return [rcopy(WP.at[s, rows(o, hx, hx)], XR1.at[s, 0], x1s.at[pair(c), 0], x1r.at[s, 0], at.dev_xp),
                rcopy(WP.at[s, rows(o + hx, hx, hx)], XR1.at[s, 1], x1s.at[pair(c), 1], x1r.at[s, 1], at.dev_xm)]

    def x2_copies(c):
        s = slot(c)
        return [rcopy(WP.at[s, rows(own_half + at.xp * xb, xb, xb)], XR2.at[s, 0], x2s.at[pair(c), 0], x2r.at[s, 0], at.dev_xp),
                rcopy(WP.at[s, rows(own_half + at.xm * xb, xb, xb)], XR2.at[s, 1], x2s.at[pair(c), 1], x2r.at[s, 1], at.dev_xm)]

    def m_rows(c, start, size):
        return m_hbm.at[rows(c * tc + start, size, size)]

    def xa_copies(c):
        src, dst = MO.at[slot(c)], m_rows(c, my_rows, xb)
        return [rcopy(src, dst, xas.at[pair(c), 0], xar.at[c, 0], at.dev_xp), rcopy(src, dst, xas.at[pair(c), 1], xar.at[c, 1], at.dev_xm)]

    def xf_copies(c):
        a = m_rows(c, own_half + at.xm * xb, hx)
        b = m_rows(c, own_half + at.xp * xb + hx, hx)
        return [rcopy(a, a, xfs.at[pair(c), 0], xfr.at[c, 0], at.dev_xp), rcopy(b, b, xfs.at[pair(c), 1], xfr.at[c, 1], at.dev_xm)]

    def dm_copy(c, i):
        if i == 0:
            return rcopy(MO.at[slot(c)], m_rows(c, my_rows, xb), dms.at[pair(c), 0], dmr.at[c, 0], at.dev_core)
        b = m_rows(c, own_half + (at.xm, at.xp, at.xo)[i - 1] * xb, xb)
        return rcopy(b, b, dms.at[pair(c), i], dmr.at[c, i], at.dev_core)

    def dm_wait_recv(c, i):
        b = m_rows(c, (1 - at.core) * hb + (at.x, at.xm, at.xp, at.xo)[i] * xb, xb)
        rcopy(b, b, dms.at[pair(c), i], dmr.at[c, i], at.dev_core).wait_recv()

    def xh_copy(c):
        return pltpu.make_async_copy(x_hbm.at[rows(c * tc + my_rows, xb, xb)], XH.at[pair(c)], xh_sem.at[pair(c)])

    def hb_copy(c):
        return pltpu.make_async_copy(HB.at[slot(c)], h_hbm.at[rows(c * xb, xb, xb)], hb_sem.at[pair(c)])

    def mo_copy(c):
        return pltpu.make_async_copy(MO.at[slot(c)], m_rows(c, my_rows, xb), mo_sem.at[pair(c)])

    def start(copies):
        for cp in copies:
            cp.start()

    def wait(copies):
        for cp in copies:
            cp.wait()

    def as_row(col_b):
        r, l = col_b.shape
        eye = lax.broadcasted_iota(jnp.int32, (r, l), 0) == lax.broadcasted_iota(jnp.int32, (r, l), 1)
        return jnp.sum(jnp.where(eye, col_b, 0.0), axis=0, keepdims=True)

    def as_col(row, r):
        l = row.shape[1]
        eye = lax.broadcasted_iota(jnp.int32, (r, l), 0) == lax.broadcasted_iota(jnp.int32, (r, l), 1)
        return jnp.sum(jnp.where(eye, jnp.broadcast_to(row, (r, l)), 0.0), axis=1, keepdims=True)

    def square_sum(v):
        vf = v.astype(F32)
        return jnp.sum(vf * vf, axis=-1, keepdims=True)

    def inv_rms(st, c):
        tot = (st[c, 0] + st[c, 1]) + (st[c, 2] + st[c, 3])
        return lax.rsqrt(tot / full_width + NORM_EPS)

    def stage(k, s, body):
        c = k - s

        @pl.when(jnp.logical_and(c >= 0, c < n_chunks))
        def _():
            body(c)

    def st_sumsq(c):
        x_copy(c).wait()

        @pl.loop(0, tc // step)
        def _(i):
            r = rows(i * step, step, step)
            SQ[r, :] = jnp.broadcast_to(square_sum(X[c % 2, r, :]), (step, 128))

        parts = [as_row(SQ[b * blk:(b + 1) * blk, :]) for b in range(n_blk)]
        parts = parts + [jnp.zeros_like(parts[0])] * (8 - n_blk)
        ST1[c, at.y] = jnp.concatenate(parts, axis=0)
        start(stats_copies(ST1, t1s, t1r, c))

    def st_qkv(c):
        wait(stats_copies(ST1, t1s, t1r, c))
        inv = inv_rms(ST1, c)
        for b in range(n_blk):
            RC[b * blk:(b + 1) * blk, :] = jnp.broadcast_to(as_col(inv[b:b + 1, :], blk), (blk, 128))

        @pl.loop(0, tc // step)
        def _(i):
            r = rows(i * step, step, step)
            N[r, :] = (X[c % 2, r, :].astype(F32) * RC[r, 0:1] * ga[...]).astype(BF16)

        n_t = qkv_w // 384

        @pl.loop(0, n_t)
        def _(n):
            cols = rows(n * 384, 384, 128)
            QP[slot(c), :, cols] = jnp.dot(N[...], WQKV[:, cols], preferred_element_type=F32).astype(BF16)

        start(s1_copies(c))

    def st_add1(c):
        wait(s1_copies(c))
        s = slot(c)

        @pl.loop(0, hq // step)
        def _(i):
            ri = rows(i * step, step, step)
            ra = rows(at.yp * qb + i * step, step, step)
            rb = rows(at.ym * qb + hq + i * step, step, step)
            QP[s, ra, :] = (QP[s, ra, :].astype(F32) + R1[s, 0, ri, :].astype(F32)).astype(BF16)
            QP[s, rb, :] = (QP[s, rb, :].astype(F32) + R1[s, 1, ri, :].astype(F32)).astype(BF16)

        start(s2_copies(c))

    def st_rope(c):
        wait(s2_copies(c))
        s = slot(c)
        own = rows(at.y * qb, qb, qb)
        cos_v = cos_t[rows(c * qb, qb, qb), :]
        sin_v = sin_t[rows(c * qb, qb, qb), :]

        def piece(i):
            cols = slice(i * head, (i + 1) * head)
            v = QP[s, own, cols].astype(F32) + R2[s, 0, :, cols].astype(F32) + R2[s, 1, :, cols].astype(F32)
            return v.astype(BF16)

        def turned(i):
            v = piece(i).astype(F32)
            return (v * cos_v + pltpu.roll(v, head // 2, 1) * sin_v).astype(BF16)

        kv_rows = rows(c * tc + at.y * qb, qb, qb)
        KV[kv_rows, 0:head] = turned(heads)
        KV[kv_rows, head:2 * head] = piece(heads + 1)
        start(kv_copies(c))
        for i in range(heads):
            QS[pair(c), i * qb:(i + 1) * qb, :] = turned(i)

    def st_attend(c):
        wait(kv_copies(c))
        q = QS[pair(c)]
        scale = head ** -0.5 * 1.4426950408889634

        def scores(j):
            keys = KV[rows(j * tc, tc, tc), 0:head]
            return lax.dot_general(q, keys, (((1,), (1,)), ((), ())), preferred_element_type=F32) * scale

        def values(j, p):
            return jnp.dot(p.astype(BF16), KV[rows(j * tc, tc, tc), head:2 * head], preferred_element_type=F32)

        qpos = at.y * qb + lax.broadcasted_iota(jnp.int32, (qb, tc), 0)
        keep = lax.broadcasted_iota(jnp.int32, (qb, tc), 1) <= qpos
        sc = scores(c).reshape(heads, qb, tc)
        sc = jnp.where(keep[None], sc, -jnp.inf).reshape(heads * qb, tc)
        top = jnp.max(sc, axis=-1, keepdims=True)
        p = jnp.exp2(sc - top)

        def more(j, carry):
            top, total, acc = carry
            sc = scores(j)
            new = jnp.maximum(top, jnp.max(sc, axis=-1, keepdims=True))
            fade = jnp.exp2(top - new)
            p = jnp.exp2(sc - new)
            return new, total * fade + jnp.sum(p, axis=-1, keepdims=True), acc * fade + values(j, p)

        top, total, acc = lax.fori_loop(0, c, more, (top, jnp.sum(p, axis=-1, keepdims=True), values(c, p)))
        out = (acc / total).astype(BF16)
        for i in range(heads):
            O[slot(c), rows(at.y * qb, qb, qb), i * head:(i + 1) * head] = out[i * qb:(i + 1) * qb, :]
        start(o_copies(c))

    def st_ofwd(c):
        wait(o_copies(c))
        start(of_copies(c))

    def st_oproj(c):
        wait(of_copies(c))
        dn_w = 256 if width % 256 == 0 else 128

        @pl.loop(0, width // dn_w)
        def _(n):
            cols = rows(n * dn_w, dn_w, 128)
            WP[slot(c), :, cols] = jnp.dot(O[slot(c)], WO[:, cols], preferred_element_type=F32).astype(BF16)

        start(dd_copies(c))

    def st_x1(c):
        wait(dd_copies(c))
        s = slot(c)

        @pl.loop(0, hb // step)
        def _(i):
            ri = rows(i * step, step, step)
            ra = rows(own_half + i * step, step, step)
            WP[s, ra, :] = (WP[s, ra, :].astype(F32) + DR[s, ri, :].astype(F32)).astype(BF16)

        start(x1_copies(c))

    def st_x2(c):
        xh_copy(c).start()
        wait(x1_copies(c))
        s = slot(c)
        ra = rows(own_half + at.xp * xb, hx, hx)
        rb = rows(own_half + at.xm * xb + hx, hx, hx)
        WP[s, ra, :] = (WP[s, ra, :].astype(F32) + XR1[s, 0].astype(F32)).astype(BF16)
        WP[s, rb, :] = (WP[s, rb, :].astype(F32) + XR1[s, 1].astype(F32)).astype(BF16)
        start(x2_copies(c))

    def st_h(c):
        wait(x2_copies(c))
        xh_copy(c).wait()
        s = slot(c)
        total = WP[s, rows(my_rows, xb, xb), :].astype(F32) + XR2[s, 0].astype(F32) + XR2[s, 1].astype(F32)
        h = (XH[pair(c)].astype(F32) + total).astype(BF16)
        HB[s] = h
        row = as_row(jnp.broadcast_to(square_sum(h), (xb, 128)))
        ST2[c, at.y] = jnp.broadcast_to(row, (8, 128))
        start(stats_copies(ST2, t2s, t2r, c))
        hb_copy(c).start()

    def st_m(c):
        wait(stats_copies(ST2, t2s, t2r, c))
        hb_copy(c).wait()
        s = slot(c)
        inv = as_col(inv_rms(ST2, c)[0:1, :], xb)
        MO[s] = (HB[s].astype(F32) * inv * gm[...]).astype(BF16)
        start(xa_copies(c))
        dm_copy(c, 0).start()
        mo_copy(c).start()

    def st_xf(c):
        wait(xa_copies(c))
        dm_copy(c, 0).wait_send()
        mo_copy(c).wait()
        start(xf_copies(c))
        dm_copy(c, 1).start()
        dm_copy(c, 2).start()

    def st_dm(c):
        wait(xf_copies(c))
        dm_copy(c, 1).wait_send()
        dm_copy(c, 2).wait_send()
        dm_copy(c, 3).start()

    def st_end(c):
        dm_copy(c, 3).wait_send()
        for i in range(4):
            dm_wait_recv(c, i)

    bodies = (st_sumsq, st_qkv, st_add1, st_rope, st_attend, st_ofwd, st_oproj, st_x1, st_x2, st_h, st_m, st_xf, st_dm, st_end)
    n_iter = n_chunks + len(bodies) - 1
    for cp in w_copies:
        cp.wait()

    @pl.loop(0, n_iter)
    def _(k):
        @pl.when(k >= 2)
        def _():
            at.take_credit(credit)

        for s, body in enumerate(bodies):
            stage(k, s, body)
            if s == 1:
                @pl.when(k + 1 < n_chunks)
                def _():
                    x_copy(k + 1).start()

        @pl.when(k < n_iter - 2)
        def _():
            at.give_credit(credit)


def attn_phase(x_in, gain_attn, gain_mlp, cos_t, sin_t, w_q, w_k, w_v, w_o, chunk):
    tokens, width = x_in.shape
    q_w = w_q.shape[1]
    heads = q_w // 128
    n_chunks = tokens // chunk
    qb, hb = chunk // 4, chunk // 2
    xb = hb // 4
    hbm = pl.BlockSpec(memory_space=pl.ANY)
    vmem = pl.BlockSpec(memory_space=pltpu.VMEM)
    sem = pltpu.SemaphoreType.DMA
    vm = lambda *s: pltpu.VMEM(s, BF16)
    vf = lambda *s: pltpu.VMEM(s, F32)
    qkv_w = q_w + 256
    return pl.pallas_call(
        functools.partial(attn_kernel, n_chunks),
        out_shape=(jax.ShapeDtypeStruct((tokens, width), BF16), jax.ShapeDtypeStruct((tokens // 8, width), BF16)),
        in_specs=[hbm, vmem, vmem, vmem, vmem, hbm, hbm, hbm, hbm],
        out_specs=(hbm, hbm),
        scratch_shapes=[
            vm(width, qkv_w), vm(q_w, width), vm(2, chunk, width), vm(chunk, width), vm(4, chunk, qkv_w),
            vm(4, 2, qb // 2, qkv_w), vm(4, 2, qb, qkv_w), vm(2, heads * qb, 128), vm(tokens, 256), vm(4, chunk, q_w),
            vm(4, chunk, width), vm(4, hb, width), vm(4, 2, xb // 2, width), vm(4, 2, xb, width), vm(2, xb, width), vm(4, xb, width), vm(4, xb, width),
            vf(chunk, 128), vf(chunk, 128), vf(n_chunks, 4, 8, 128), vf(n_chunks, 4, 8, 128),
            sem((4,)), sem((2,)), sem((2,)), sem((2,)), sem((2,)), pltpu.SemaphoreType.REGULAR((5,)),
            sem((2, 3)), sem((n_chunks, 3)), sem((2, 2)), sem((4, 2)), sem((2, 2)), sem((4, 2)), sem((2, 3)), sem((n_chunks, 3)),
            sem((2, 2)), sem((4, 2)), sem((2, 2)), sem((4, 2)), sem((2,)), sem((4,)), sem((2, 2)), sem((4, 2)), sem((2, 2)), sem((4, 2)),
            sem((2, 3)), sem((n_chunks, 3)), sem((2, 2)), sem((n_chunks, 2)), sem((2, 2)), sem((n_chunks, 2)), sem((2, 4)), sem((n_chunks, 4)),
        ],
        compiler_params=pltpu.CompilerParams(collective_id=2, has_side_effects=True, vmem_limit_bytes=67043328),
        name="attn_phase",
    )(x_in, gain_attn, gain_mlp, cos_t, sin_t, w_q, w_k, w_v, w_o)


def solution(mesh, chunk=CHUNK):
    my_size = mesh.shape["my"]

    def local_layer(x_in, gain_attn, w_q, w_k, w_v, w_o, gain_mlp, w_gate, w_up, w_down):
        tokens, width = x_in.shape
        head = w_q.shape[-1]
        qb = chunk // my_size
        row = jnp.arange(tokens // my_size)
        positions = (row // qb) * chunk + lax.axis_index("my") * qb + row % qb
        half = head // 2
        inv_freq = ROPE_BASE ** (-jnp.arange(half, dtype=F32) / half)
        angles = positions.astype(F32)[:, None] * inv_freq[None, :]
        cos_h, sin_h = jnp.cos(angles), jnp.sin(angles)
        cos_t = jnp.concatenate([cos_h, cos_h], axis=-1)
        sin_t = jnp.concatenate([-sin_h, sin_h], axis=-1)
        m_full, h_own = attn_phase(
            x_in, gain_attn.astype(F32).reshape(1, width), gain_mlp.astype(F32).reshape(1, width), cos_t, sin_t,
            w_q.reshape(width, -1), w_k.reshape(width, -1), w_v.reshape(width, -1), w_o.reshape(-1, width), chunk)
        return mlp_phase(m_full, h_own, w_gate, w_up, w_down, chunk)

    in_specs = (P("dp", "my"), P("my"), P("my", "mx", None), P("my", "mx", None), P("my", "mx", None), P("mx", None, "my"), P("my"), P("my", "mx"), P("my", "mx"), P("mx", "my"))
    return jax.shard_map(local_layer, mesh=mesh, in_specs=in_specs, out_specs=P("dp", "my"), check_vma=False)
```

```python
import functools

import jax
import jax.numpy as jnp
from jax import lax
from jax.experimental import pallas as pl
from jax.experimental.pallas import tpu as pltpu
from jax.sharding import PartitionSpec as P

ROPE_BASE = 10000.0
NORM_EPS = 1e-6
CHUNK = 512
EARLY = 2
MESH = pl.DeviceIdType.MESH
F32 = jnp.float32
BF16 = jnp.bfloat16


class Place:
    def __init__(self):
        self.y = lax.axis_index("my")
        mx = lax.axis_index("mx")
        self.x = mx // 2
        self.core = mx % 2
        self.yp = (self.y + 1) % 4
        self.ym = (self.y + 3) % 4
        self.yo = (self.y + 2) % 4
        self.xp = (self.x + 1) % 4
        self.xm = (self.x + 3) % 4
        self.xo = (self.x + 2) % 4
        self.dev_yp = {"my": self.yp}
        self.dev_ym = {"my": self.ym}
        self.dev_xp = {"mx": self.xp * 2 + self.core}
        self.dev_xm = {"mx": self.xm * 2 + self.core}
        self.dev_core = {"mx": self.x * 2 + (1 - self.core)}
        self.dev_yo = {"my": self.yo}
        self.ys = (self.dev_yp, self.dev_ym)
        self.xs = (self.dev_xp, self.dev_xm)
        self.partners = (self.dev_yp, self.dev_ym, self.dev_xp, self.dev_xm, self.dev_core)

    def entry(self, extra=()):
        barrier = pltpu.get_barrier_semaphore()
        for dev in self.partners + extra:
            pl.semaphore_signal(barrier, inc=1, device_id=dev, device_id_type=MESH)
        pl.semaphore_wait(barrier, len(self.partners) + len(extra))

    def give_credit(self, credit):
        for slot, dev in ((1, self.dev_yp), (0, self.dev_ym), (3, self.dev_xp), (2, self.dev_xm), (4, self.dev_core)):
            pl.semaphore_signal(credit.at[slot], inc=1, device_id=dev, device_id_type=MESH)

    def take_credit(self, credit):
        for slot in range(5):
            pl.semaphore_wait(credit.at[slot], 1)


def rcopy(src, dst, send_sem, recv_sem, dev):
    return pltpu.make_async_remote_copy(src_ref=src, dst_ref=dst, send_sem=send_sem, recv_sem=recv_sem, device_id=dev, device_id_type=MESH)


def as_row(col_b):
    eye = lax.broadcasted_iota(jnp.int32, col_b.shape, 0) == lax.broadcasted_iota(jnp.int32, col_b.shape, 1)
    return jnp.sum(jnp.where(eye, col_b, 0.0), axis=0, keepdims=True)


def as_col(row, r):
    shape = (r, row.shape[1])
    eye = lax.broadcasted_iota(jnp.int32, shape, 0) == lax.broadcasted_iota(jnp.int32, shape, 1)
    return jnp.sum(jnp.where(eye, jnp.broadcast_to(row, shape), 0.0), axis=1, keepdims=True)


def square_sum(v):
    vf = v.astype(F32)
    return jnp.sum(vf * vf, axis=-1, keepdims=True)


def inv_rms(st, c, full_width):
    tot = (st[c, 0] + st[c, 1]) + (st[c, 2] + st[c, 3])
    return lax.rsqrt(tot / full_width + NORM_EPS)


def two(srcs, dsts, send, recv, devs):
    return [rcopy(src, dst, send.at[i], recv.at[i], dev) for i, (src, dst, dev) in enumerate(zip(srcs, dsts, devs))]


def slots(ref):
    return [ref.at[i] for i in range(2)]


def start(copies):
    for c in copies:
        c.start()


def wait(copies):
    for c in copies:
        c.wait()


def rows(start, size, align):
    return pl.ds(pl.multiple_of(start, align), size)


def mlp_kernel(n_chunks, x_hbm, gains, me_hbm, he_hbm, wp_hbm, wg_hbm, wu_hbm, wd_hbm, y_hbm, ml_hbm, hl_hbm,
               WG, WU, WD, M, PP, R1, R2, ACT, DP, DR, XR1, XR2, YB, H, OP, OR, OX1, OX2, XH, HB, MO, ST,
               w_sem, m_sem, h_sem, y_sem, o_sem, ods, odr, oxs, oxr, ots, otr, oms, omr, credit, s1s, s1r, s2s, s2r, acs, acr, fws, fwr, dds, ddr, x1s, x1r, x2s, x2r, xas, xar, xfs, xfr, dys, dyr):
    at = Place()
    tc, width = M.shape
    ff = WG.shape[1]
    qb = tc // 4
    hq = qb // 2
    hb = tc // 2
    xb = hb // 4
    hx = xb // 2
    gu_tiles = 5
    gu_w = ff // gu_tiles
    dn_w = 256 if width % 256 == 0 else 128

    def m_wait():
        pltpu.make_async_copy(me_hbm.at[pl.ds(0, tc)], M, m_sem).wait()

    def m_start(c):
        @pl.when(c < EARLY)
        def _():
            pltpu.make_async_copy(me_hbm.at[rows(c * tc, tc, tc)], M, m_sem).start()

        @pl.when(c >= EARLY)
        def _():
            pltpu.make_async_copy(ml_hbm.at[rows((c - EARLY) * tc, tc, tc)], M, m_sem).start()

    def gu_copies(n):
        cols = rows(n * gu_w, gu_w, 128)
        return [pltpu.make_async_copy(wg_hbm.at[:, cols], WG.at[:, cols], w_sem.at[n]),
                pltpu.make_async_copy(wu_hbm.at[:, cols], WU.at[:, cols], w_sem.at[gu_tiles + n])]

    wd_copy = pltpu.make_async_copy(wd_hbm, WD, w_sem.at[2 * gu_tiles])
    pltpu.make_async_copy(me_hbm.at[pl.ds(0, tc)], M, m_sem).start()
    for n in range(gu_tiles):
        start(gu_copies(n))
    wd_copy.start()
    at.entry(extra=(at.dev_yo,))

    def gu_part(par, lo, hi):
        @pl.loop(lo, hi)
        def _(n):
            g_cols = rows(n * gu_w, gu_w, 128)
            PP[par, :, g_cols] = jnp.dot(M[...], WG[:, g_cols], preferred_element_type=F32).astype(BF16)
            PP[par, :, rows(ff + n * gu_w, gu_w, 128)] = jnp.dot(M[...], WU[:, g_cols], preferred_element_type=F32).astype(BF16)

    def s1_copies(par):
        o = at.yo * qb
        return two([PP.at[par, rows(r, hq, hq)] for r in (o, o + hq)], slots(R1), s1s, s1r, at.ys)

    def s2_copies(par):
        return two([PP.at[par, rows(b * qb, qb, qb)] for b in (at.yp, at.ym)], slots(R2.at[par]), s2s.at[par], s2r.at[par], at.ys)

    def act_copies(par):
        own = [ACT.at[par, rows(at.y * qb, qb, qb)]] * 2
        return two(own, own, acs, acr, at.ys)

    def fwd_copies(par):
        half = [ACT.at[par, rows(r, hq, hq)] for r in (at.ym * qb, at.yp * qb + hq)]
        return two(half, half, fws.at[par], fwr.at[par], at.ys)

    def dd_copy():
        return rcopy(DP.at[rows((1 - at.core) * hb, hb, hb)], DR, dds, ddr, at.dev_core)

    own_half = at.core * hb

    def x1_copies():
        o = own_half + at.xo * xb
        return two([DP.at[rows(r, hx, hx)] for r in (o, o + hx)], slots(XR1), x1s, x1r, at.xs)

    def x2_copies():
        return two([DP.at[rows(own_half + b * xb, xb, xb)] for b in (at.xp, at.xm)], slots(XR2), x2s, x2r, at.xs)

    def yblk(b):
        return YB.at[rows(own_half + b * xb, xb, xb)]

    def xa_copies():
        own = [yblk(at.x)] * 2
        return two(own, own, xas, xar, at.xs)

    def xf_copies():
        half = [YB.at[rows(own_half + r, hx, hx)] for r in (at.xm * xb, at.xp * xb + hx)]
        return two(half, half, xfs, xfr, at.xs)

    def dy_copy(i):
        b = (at.x, at.xm, at.xp, at.xo)[i]
        return rcopy(yblk(b), yblk(b), dys.at[i], dyr.at[i], at.dev_core)

    def dy_wait_recv(i):
        b = (at.x, at.xm, at.xp, at.xo)[i]
        other = YB.at[rows((1 - at.core) * hb + b * xb, xb, xb)]
        rcopy(other, other, dys.at[i], dyr.at[i], at.dev_core).wait_recv()

    def h_wait():
        pltpu.make_async_copy(he_hbm.at[pl.ds(0, xb)], H, h_sem).wait()

    def h_start(c):
        @pl.when(c < EARLY)
        def _():
            pltpu.make_async_copy(he_hbm.at[rows(c * xb, xb, xb)], H, h_sem).start()

        @pl.when(c >= EARLY)
        def _():
            pltpu.make_async_copy(hl_hbm.at[rows((c - EARLY) * xb, xb, xb)], H, h_sem).start()

    def y_copy(c):
        return pltpu.make_async_copy(YB, y_hbm.at[rows(c * tc, tc, tc)], y_sem)

    my_rows = own_half + at.x * xb
    peers = at.ys + (at.dev_yo,)

    def od_copy(c):
        return rcopy(wp_hbm.at[rows((c - EARLY) * tc + (1 - at.core) * hb, hb, hb)], OR, ods, odr, at.dev_core)

    def op_copy(c):
        return pltpu.make_async_copy(wp_hbm.at[rows((c - EARLY) * tc + own_half, hb, hb)], OP, o_sem.at[0])

    def xh_copy(c):
        return pltpu.make_async_copy(x_hbm.at[rows(c * tc + my_rows, xb, xb)], XH, o_sem.at[1])

    def hl_copy(c):
        return pltpu.make_async_copy(HB, hl_hbm.at[rows((c - EARLY) * xb, xb, xb)], o_sem.at[2])

    def ml_rows(c, first, size):
        return ml_hbm.at[rows((c - EARLY) * tc + first, size, size)]

    def mo_copy(c):
        return pltpu.make_async_copy(MO, ml_rows(c, my_rows, xb), o_sem.at[3])

    def o1_copies():
        return two([OP.at[rows(at.xo * xb + r, hx, hx)] for r in (0, hx)], slots(OX1), oxs.at[0], oxr.at[0], at.xs)

    def o2_copies():
        return two([OP.at[rows(b * xb, xb, xb)] for b in (at.xp, at.xm)], slots(OX2), oxs.at[1], oxr.at[1], at.xs)

    def ot_copies(c):
        own = ST.at[c, at.y]
        return [rcopy(own, own, ots.at[i], otr.at[c, i], dev) for i, dev in enumerate(peers)]

    def oa_copies(c):
        return two([MO] * 2, [ml_rows(c, my_rows, xb)] * 2, oxs.at[2], oxr.at[2], at.xs)

    def of_copies(c):
        half = [ml_rows(c, own_half + r, hx) for r in (at.xm * xb, at.xp * xb + hx)]
        return two(half, half, oxs.at[3], oxr.at[3], at.xs)

    def om_copy(c, i):
        b = ml_rows(c, own_half + (at.x, at.xm, at.xp, at.xo)[i] * xb, xb)
        return rcopy(MO if i == 0 else b, b, oms.at[i], omr.at[i], at.dev_core)

    def om_wait_recv(c, i):
        b = ml_rows(c, (1 - at.core) * hb + (at.x, at.xm, at.xp, at.xo)[i] * xb, xb)
        rcopy(b, b, oms.at[i], omr.at[i], at.dev_core).wait_recv()

    def o_begin(c):
        od_copy(c).start()
        op_copy(c).start()
        xh_copy(c).start()

    def o_core(c):
        od_copy(c).wait()
        op_copy(c).wait()

        @pl.loop(0, hb // 16)
        def _(i):
            r = rows(i * 16, 16, 16)
            OP[r, :] = (OP[r, :].astype(F32) + OR[r, :].astype(F32)).astype(BF16)

        start(o1_copies())

    def o_ring(c):
        wait(o1_copies())
        ra = rows(at.xp * xb, hx, hx)
        rb = rows(at.xm * xb + hx, hx, hx)
        OP[ra, :] = (OP[ra, :].astype(F32) + OX1[0].astype(F32)).astype(BF16)
        OP[rb, :] = (OP[rb, :].astype(F32) + OX1[1].astype(F32)).astype(BF16)
        start(o2_copies())

    def o_sum(c):
        wait(o2_copies())
        xh_copy(c).wait()
        total = OP[rows(at.x * xb, xb, xb), :].astype(F32) + OX2[0].astype(F32) + OX2[1].astype(F32)
        h = (XH[...].astype(F32) + total).astype(BF16)
        HB[...] = h
        ST[c, at.y] = jnp.broadcast_to(as_row(jnp.broadcast_to(square_sum(h), (xb, 128))), (8, 128))
        start(ot_copies(c))
        hl_copy(c).start()

    def o_norm(c):
        wait(ot_copies(c))
        hl_copy(c).wait()
        inv = as_col(inv_rms(ST, c, width * 4)[0:1, :], xb)
        MO[...] = (HB[...].astype(F32) * inv * gains[1:2, :]).astype(BF16)
        start(oa_copies(c))
        om_copy(c, 0).start()
        mo_copy(c).start()

    def o_pass(c):
        wait(oa_copies(c))
        mo_copy(c).wait()
        start(of_copies(c))
        om_copy(c, 1).start()
        om_copy(c, 2).start()

    def o_last(c):
        wait(of_copies(c))
        om_copy(c, 3).start()

    def o_end(c):
        for i in range(4):
            om_copy(c, i).wait_send()
            om_wait_recv(c, i)

    m_wait()
    for i, b in enumerate((at.yo, at.yp, at.ym, at.y)):
        br = rows(b * qb, qb, qb)

        @pl.loop(0, gu_tiles)
        def _(n):
            if i == 0:
                wait(gu_copies(n))
            g_cols = rows(n * gu_w, gu_w, 128)
            PP[0, br, g_cols] = jnp.dot(M[br, :], WG[:, g_cols], preferred_element_type=F32).astype(BF16)
            PP[0, br, rows(ff + n * gu_w, gu_w, 128)] = jnp.dot(M[br, :], WU[:, g_cols], preferred_element_type=F32).astype(BF16)

        if i == 0:
            start(s1_copies(0))
    wd_copy.wait()

    @pl.loop(0, n_chunks + 2)
    def _(k):
        par = k % 2
        alt = (k + 1) % 2
        has_s = k < n_chunks
        has_gu = k + 1 < n_chunks
        has_a = jnp.logical_and(k >= 1, k - 1 < n_chunks)
        has_d = k >= 2

        @pl.when(k >= 1)
        def _():
            at.take_credit(credit)

        @pl.when(jnp.logical_and(has_s, k >= 1))
        def _():
            start(s1_copies(par))

        @pl.when(has_d)
        def _():
            h_start(k - 2)

        def o_step(body):
            @pl.when(k + EARLY < n_chunks)
            def _():
                body(k + EARLY)

        def m_step(body):
            @pl.when(jnp.logical_and(k + 1 >= EARLY, has_gu))
            def _():
                body(k + 1)

        o_step(o_begin)
        m_step(o_norm)

        @pl.when(has_a)
        def _():
            wait(s2_copies(alt))
            base = at.y * qb
            step = 16

            @pl.loop(0, qb // step)
            def _(i):
                r = rows(base + i * step, step, step)
                r2 = rows(i * step, step, step)
                g = PP[alt, r, 0:ff].astype(F32) + R2[alt, 0, r2, 0:ff].astype(F32) + R2[alt, 1, r2, 0:ff].astype(F32)
                u = PP[alt, r, ff:2 * ff].astype(F32) + R2[alt, 0, r2, ff:2 * ff].astype(F32) + R2[alt, 1, r2, ff:2 * ff].astype(F32)
                ACT[alt, r, :] = (g * jax.nn.sigmoid(g) * u).astype(BF16)

            start(act_copies(alt))

        m_step(o_pass)

        @pl.when(has_d)
        def _():
            wait(fwd_copies(par))

            @pl.loop(0, width // dn_w)
            def _(n):
                cols = rows(n * dn_w, dn_w, 128)
                DP[:, cols] = jnp.dot(ACT[par], WD[:, cols], preferred_element_type=F32).astype(BF16)

            dd_copy().start()

        o_step(o_core)
        m_step(o_last)

        @pl.when(has_s)
        def _():
            wait(s1_copies(par))
            step = 16

            @pl.loop(0, hq // step)
            def _(i):
                ri = rows(i * step, step, step)
                ra = rows(at.yp * qb + i * step, step, step)
                rb = rows(at.ym * qb + hq + i * step, step, step)
                PP[par, ra, :] = (PP[par, ra, :].astype(F32) + R1[0, ri, :].astype(F32)).astype(BF16)
                PP[par, rb, :] = (PP[par, rb, :].astype(F32) + R1[1, ri, :].astype(F32)).astype(BF16)

            start(s2_copies(par))

        o_step(o_ring)
        m_step(o_end)

        @pl.when(has_gu)
        def _():
            m_start(k + 1)

        @pl.when(has_d)
        def _():
            dd_copy().wait()
            step = 16

            @pl.loop(0, hb // step)
            def _(i):
                ri = rows(i * step, step, step)
                ra = rows(own_half + i * step, step, step)
                DP[ra, :] = (DP[ra, :].astype(F32) + DR[ri, :].astype(F32)).astype(BF16)

            start(x1_copies())

        @pl.when(has_gu)
        def _():
            m_wait()
            gu_part(alt, 0, 2)

        o_step(o_sum)

        @pl.when(has_d)
        def _():
            wait(x1_copies())
            ra = rows(own_half + at.xp * xb, hx, hx)
            rb = rows(own_half + at.xm * xb + hx, hx, hx)
            DP[ra, :] = (DP[ra, :].astype(F32) + XR1[0].astype(F32)).astype(BF16)
            DP[rb, :] = (DP[rb, :].astype(F32) + XR1[1].astype(F32)).astype(BF16)
            start(x2_copies())

        @pl.when(has_gu)
        def _():
            gu_part(alt, 2, 3)

        @pl.when(has_a)
        def _():
            wait(act_copies(alt))
            start(fwd_copies(alt))

        @pl.when(has_d)
        def _():
            wait(x2_copies())
            h_wait()
            r = rows(own_half + at.x * xb, xb, xb)
            down = DP[r, :].astype(F32) + XR2[0].astype(F32) + XR2[1].astype(F32)
            YB[r, :] = (H[...].astype(F32) + down).astype(BF16)
            start(xa_copies())
            dy_copy(0).start()

        @pl.when(has_gu)
        def _():
            gu_part(alt, 3, 4)

        @pl.when(has_d)
        def _():
            wait(xa_copies())
            start(xf_copies())
            dy_copy(1).start()
            dy_copy(2).start()

        @pl.when(has_gu)
        def _():
            gu_part(alt, 4, 5)

        @pl.when(has_d)
        def _():
            wait(xf_copies())
            dy_copy(3).start()
            for i in range(4):
                dy_copy(i).wait_send()
                dy_wait_recv(i)
            y_copy(k - 2).start()
            y_copy(k - 2).wait()

        @pl.when(k < n_chunks + 1)
        def _():
            at.give_credit(credit)


def mlp_phase(x_in, gains, m_early, h_early, o_part, w_gate, w_up, w_down, chunk):
    tokens, width = x_in.shape
    ff = w_gate.shape[1]
    n_chunks = tokens // chunk
    qb, hb = chunk // 4, chunk // 2
    xb = hb // 4
    hbm = pl.BlockSpec(memory_space=pl.ANY)
    sem = pltpu.SemaphoreType.DMA
    S2, P2 = sem((2,)), sem((2, 2))
    vm = lambda *s: pltpu.VMEM(s, BF16)
    return pl.pallas_call(
        functools.partial(mlp_kernel, n_chunks),
        out_shape=tuple(jax.ShapeDtypeStruct((n, width), BF16) for n in (tokens, tokens - EARLY * chunk, tokens // 8 - EARLY * xb)),
        in_specs=[hbm, pl.BlockSpec(memory_space=pltpu.VMEM)] + [hbm] * 6,
        out_specs=(hbm, hbm, hbm),
        scratch_shapes=[
            vm(width, ff), vm(width, ff), vm(ff, width), vm(chunk, width), vm(2, chunk, 2 * ff),
            vm(2, qb // 2, 2 * ff), vm(2, 2, qb, 2 * ff), vm(2, chunk, ff), vm(chunk, width), vm(hb, width),
            vm(2, xb // 2, width), vm(2, xb, width), vm(chunk, width), vm(xb, width),
            vm(hb, width), vm(hb, width), vm(2, xb // 2, width), vm(2, xb, width), vm(xb, width), vm(xb, width), vm(xb, width),
            pltpu.VMEM((n_chunks, 4, 8, 128), F32),
            sem((11,)), sem, sem, sem, sem((4,)), sem, sem, sem((4, 2)), sem((4, 2)), sem((3,)), sem((n_chunks, 3)), sem((4,)), sem((4,)), pltpu.SemaphoreType.REGULAR((5,)),
            S2, S2, P2, P2, S2, S2, P2, P2,
            sem, sem, S2, S2, S2, S2, S2, S2, S2, S2, sem((4,)), sem((4,)),
        ],
        compiler_params=pltpu.CompilerParams(collective_id=1, has_side_effects=True, vmem_limit_bytes=67043328),
        name="mlp_phase",
    )(x_in, gains, m_early, h_early, o_part, w_gate, w_up, w_down)[0]


def attn_kernel(n_chunks, x_hbm, gains, cos_t, sin_t, wq_hbm, wk_hbm, wv_hbm, wo_hbm, m_hbm, h_hbm, wp_hbm,
                WQKV, WO, X, N, QP, R1, R2, QS, KV, O, WP, DR, XR1, XR2, XH, HB, MO, SQ, RC, ST1, ST2,
                w_sem, x_sem, xh_sem, hb_sem, mo_sem, wp_sem, credit,
                t1s, t1r, s1s, s1r, s2s, s2r, kvs, kvr, ocs, ocr, ofs, ofr, dds, ddr, x1s, x1r, x2s, x2r, t2s, t2r, xas, xar, xfs, xfr, dms, dmr):
    at = Place()
    tc, width = N.shape
    full_width = width * 4
    qkv_w = WQKV.shape[1]
    head = 128
    heads = QS.shape[1] // (tc // 4)
    q_w = heads * head
    qb = tc // 4
    hq = qb // 2
    hb = tc // 2
    xb = hb // 4
    hx = xb // 2
    own_half = at.core * hb
    my_rows = own_half + at.x * xb
    peers = at.ys + (at.dev_yo,)
    blk = min(128, tc)
    n_blk = tc // blk
    step = 16

    w_copies = [
        pltpu.make_async_copy(w, WQKV.at[:, pl.ds(i * head, head)], w_sem.at[i])
        for i, w in enumerate([wq_hbm.at[h] for h in range(heads)] + [wk_hbm, wv_hbm])
    ] + [pltpu.make_async_copy(wo_hbm, WO, w_sem.at[heads + 2])]

    def x_copy(c):
        return pltpu.make_async_copy(x_hbm.at[rows(c * tc, tc, tc)], X.at[c % 2], x_sem.at[c % 2])

    x_copy(0).start()
    for c in w_copies:
        c.start()
    at.entry(extra=(at.dev_yo,))

    def slot(c):
        return c % 4

    def pair(c):
        return c % 2

    def stats_copies(st, ssem, rsem, c):
        own = st.at[c, at.y]
        return [rcopy(own, own, ssem.at[pair(c), i], rsem.at[c, i], dev) for i, dev in enumerate(peers)]

    def s1_copies(c):
        s, o = slot(c), at.yo * qb
        return two([QP.at[s, rows(r, hq, hq)] for r in (o, o + hq)], slots(R1.at[s]), s1s.at[pair(c)], s1r.at[s], at.ys)

    def s2_copies(c):
        s = slot(c)
        return two([QP.at[s, rows(b * qb, qb, qb)] for b in (at.yp, at.ym)], slots(R2.at[s]), s2s.at[pair(c)], s2r.at[s], at.ys)

    def kv_copies(c):
        own = KV.at[rows(c * tc + at.y * qb, qb, qb)]
        return [rcopy(own, own, kvs.at[pair(c), i], kvr.at[c, i], dev) for i, dev in enumerate(peers)]

    def o_copies(c):
        own = [O.at[slot(c), rows(at.y * qb, qb, qb)]] * 2
        return two(own, own, ocs.at[pair(c)], ocr.at[slot(c)], at.ys)

    def of_copies(c):
        half = [O.at[slot(c), rows(r, hq, hq)] for r in (at.ym * qb, at.yp * qb + hq)]
        return two(half, half, ofs.at[pair(c)], ofr.at[slot(c)], at.ys)

    def dd_copies(c):
        s = slot(c)
        return [rcopy(WP.at[s, rows((1 - at.core) * hb, hb, hb)], DR.at[s], dds.at[pair(c)], ddr.at[s], at.dev_core)]

    def x1_copies(c):
        s, o = slot(c), own_half + at.xo * xb
        return two([WP.at[s, rows(r, hx, hx)] for r in (o, o + hx)], slots(XR1.at[s]), x1s.at[pair(c)], x1r.at[s], at.xs)

    def x2_copies(c):
        s = slot(c)
        return two([WP.at[s, rows(own_half + b * xb, xb, xb)] for b in (at.xp, at.xm)], slots(XR2.at[s]), x2s.at[pair(c)], x2r.at[s], at.xs)

    def m_rows(c, start, size):
        return m_hbm.at[rows(c * tc + start, size, size)]

    def xa_copies(c):
        return two([MO.at[slot(c)]] * 2, [m_rows(c, my_rows, xb)] * 2, xas.at[pair(c)], xar.at[c], at.xs)

    def xf_copies(c):
        half = [m_rows(c, own_half + r, hx) for r in (at.xm * xb, at.xp * xb + hx)]
        return two(half, half, xfs.at[pair(c)], xfr.at[c], at.xs)

    def dm_copy(c, i):
        if i == 0:
            return rcopy(MO.at[slot(c)], m_rows(c, my_rows, xb), dms.at[pair(c), 0], dmr.at[c, 0], at.dev_core)
        b = m_rows(c, own_half + (at.xm, at.xp, at.xo)[i - 1] * xb, xb)
        return rcopy(b, b, dms.at[pair(c), i], dmr.at[c, i], at.dev_core)

    def dm_wait_recv(c, i):
        b = m_rows(c, (1 - at.core) * hb + (at.x, at.xm, at.xp, at.xo)[i] * xb, xb)
        rcopy(b, b, dms.at[pair(c), i], dmr.at[c, i], at.dev_core).wait_recv()

    def xh_copy(c):
        return pltpu.make_async_copy(x_hbm.at[rows(c * tc + my_rows, xb, xb)], XH.at[pair(c)], xh_sem.at[pair(c)])

    def hb_copy(c):
        return pltpu.make_async_copy(HB.at[slot(c)], h_hbm.at[rows(c * xb, xb, xb)], hb_sem.at[pair(c)])

    def mo_copy(c):
        return pltpu.make_async_copy(MO.at[slot(c)], m_rows(c, my_rows, xb), mo_sem.at[pair(c)])

    def wp_copy(c):
        return pltpu.make_async_copy(WP.at[slot(c)], wp_hbm.at[rows((c - EARLY) * tc, tc, tc)], wp_sem.at[pair(c)])

    def stage(k, s, body):
        c = k - s

        @pl.when(jnp.logical_and(c >= 0, c < (EARLY if s >= 8 else n_chunks)))
        def _():
            body(c)

    def st_sumsq(c):
        x_copy(c).wait()

        @pl.loop(0, tc // step)
        def _(i):
            r = rows(i * step, step, step)
            SQ[r, :] = jnp.broadcast_to(square_sum(X[c % 2, r, :]), (step, 128))

        parts = [as_row(SQ[b * blk:(b + 1) * blk, :]) for b in range(n_blk)]
        parts = parts + [jnp.zeros_like(parts[0])] * (8 - n_blk)
        ST1[c, at.y] = jnp.concatenate(parts, axis=0)
        start(stats_copies(ST1, t1s, t1r, c))

    def st_qkv(c):
        wait(stats_copies(ST1, t1s, t1r, c))

        @pl.when(c == 0)
        def _():
            wait(w_copies[:-1])

        inv = inv_rms(ST1, c, full_width)
        for b in range(n_blk):
            RC[b * blk:(b + 1) * blk, :] = jnp.broadcast_to(as_col(inv[b:b + 1, :], blk), (blk, 128))

        @pl.loop(0, tc // step)
        def _(i):
            r = rows(i * step, step, step)
            N[r, :] = (X[c % 2, r, :].astype(F32) * RC[r, 0:1] * gains[0:1, :]).astype(BF16)

        n_t = qkv_w // 384

        @pl.loop(0, n_t)
        def _(n):
            cols = rows(n * 384, 384, 128)
            QP[slot(c), :, cols] = jnp.dot(N[...], WQKV[:, cols], preferred_element_type=F32).astype(BF16)

        start(s1_copies(c))

    def st_add1(c):
        wait(s1_copies(c))
        s = slot(c)

        @pl.loop(0, hq // step)
        def _(i):
            ri = rows(i * step, step, step)
            ra = rows(at.yp * qb + i * step, step, step)
            rb = rows(at.ym * qb + hq + i * step, step, step)
            QP[s, ra, :] = (QP[s, ra, :].astype(F32) + R1[s, 0, ri, :].astype(F32)).astype(BF16)
            QP[s, rb, :] = (QP[s, rb, :].astype(F32) + R1[s, 1, ri, :].astype(F32)).astype(BF16)

        start(s2_copies(c))

    def st_rope(c):
        wait(s2_copies(c))
        s = slot(c)
        own = rows(at.y * qb, qb, qb)
        cos_v = cos_t[rows(c * qb, qb, qb), :]
        sin_v = sin_t[rows(c * qb, qb, qb), :]

        def piece(i):
            cols = slice(i * head, (i + 1) * head)
            v = QP[s, own, cols].astype(F32) + R2[s, 0, :, cols].astype(F32) + R2[s, 1, :, cols].astype(F32)
            return v.astype(BF16)

        def turned(i):
            v = piece(i).astype(F32)
            return (v * cos_v + pltpu.roll(v, head // 2, 1) * sin_v).astype(BF16)

        kv_rows = rows(c * tc + at.y * qb, qb, qb)
        KV[kv_rows, 0:head] = turned(heads)
        KV[kv_rows, head:2 * head] = piece(heads + 1)
        start(kv_copies(c))
        for i in range(heads):
            QS[pair(c), i * qb:(i + 1) * qb, :] = turned(i)

    def st_attend(c):
        wait(kv_copies(c))
        q = QS[pair(c)]
        scale = head ** -0.5 * 1.4426950408889634

        def scores(j):
            keys = KV[rows(j * tc, tc, tc), 0:head]
            return lax.dot_general(q, keys, (((1,), (1,)), ((), ())), preferred_element_type=F32) * scale

        def values(j, p):
            return jnp.dot(p.astype(BF16), KV[rows(j * tc, tc, tc), head:2 * head], preferred_element_type=F32)

        qpos = at.y * qb + lax.broadcasted_iota(jnp.int32, (qb, tc), 0)
        keep = lax.broadcasted_iota(jnp.int32, (qb, tc), 1) <= qpos
        sc = scores(c).reshape(heads, qb, tc)
        sc = jnp.where(keep[None], sc, -jnp.inf).reshape(heads * qb, tc)
        top = jnp.max(sc, axis=-1, keepdims=True)
        p = jnp.exp2(sc - top)

        def more(j, carry):
            top, total, acc = carry
            sc = scores(j)
            new = jnp.maximum(top, jnp.max(sc, axis=-1, keepdims=True))
            fade = jnp.exp2(top - new)
            p = jnp.exp2(sc - new)
            return new, total * fade + jnp.sum(p, axis=-1, keepdims=True), acc * fade + values(j, p)

        top, total, acc = lax.fori_loop(0, c, more, (top, jnp.sum(p, axis=-1, keepdims=True), values(c, p)))
        out = (acc / total).astype(BF16)
        for i in range(heads):
            O[slot(c), rows(at.y * qb, qb, qb), i * head:(i + 1) * head] = out[i * qb:(i + 1) * qb, :]
        start(o_copies(c))

    def st_ofwd(c):
        wait(o_copies(c))
        start(of_copies(c))

    def st_oproj(c):
        wait(of_copies(c))

        @pl.when(c == 0)
        def _():
            w_copies[-1].wait()

        dn_w = 256 if width % 256 == 0 else 128

        @pl.loop(0, width // dn_w)
        def _(n):
            cols = rows(n * dn_w, dn_w, 128)
            WP[slot(c), :, cols] = jnp.dot(O[slot(c)], WO[:, cols], preferred_element_type=F32).astype(BF16)

        @pl.when(c < EARLY)
        def _():
            start(dd_copies(c))

        @pl.when(c >= EARLY)
        def _():
            wp_copy(c).start()

    def st_x1(c):
        @pl.when(c < EARLY)
        def _():
            st_x1_early(c)

        @pl.when(c >= EARLY)
        def _():
            wp_copy(c).wait()

    def st_x1_early(c):
        wait(dd_copies(c))
        s = slot(c)

        @pl.loop(0, hb // step)
        def _(i):
            ri = rows(i * step, step, step)
            ra = rows(own_half + i * step, step, step)
            WP[s, ra, :] = (WP[s, ra, :].astype(F32) + DR[s, ri, :].astype(F32)).astype(BF16)

        start(x1_copies(c))

    def st_x2(c):
        xh_copy(c).start()
        wait(x1_copies(c))
        s = slot(c)
        ra = rows(own_half + at.xp * xb, hx, hx)
        rb = rows(own_half + at.xm * xb + hx, hx, hx)
        WP[s, ra, :] = (WP[s, ra, :].astype(F32) + XR1[s, 0].astype(F32)).astype(BF16)
        WP[s, rb, :] = (WP[s, rb, :].astype(F32) + XR1[s, 1].astype(F32)).astype(BF16)
        start(x2_copies(c))

    def st_h(c):
        wait(x2_copies(c))
        xh_copy(c).wait()
        s = slot(c)
        total = WP[s, rows(my_rows, xb, xb), :].astype(F32) + XR2[s, 0].astype(F32) + XR2[s, 1].astype(F32)
        h = (XH[pair(c)].astype(F32) + total).astype(BF16)
        HB[s] = h
        row = as_row(jnp.broadcast_to(square_sum(h), (xb, 128)))
        ST2[c, at.y] = jnp.broadcast_to(row, (8, 128))
        start(stats_copies(ST2, t2s, t2r, c))
        hb_copy(c).start()

    def st_m(c):
        wait(stats_copies(ST2, t2s, t2r, c))
        hb_copy(c).wait()
        s = slot(c)
        inv = as_col(inv_rms(ST2, c, full_width)[0:1, :], xb)
        MO[s] = (HB[s].astype(F32) * inv * gains[1:2, :]).astype(BF16)
        start(xa_copies(c))
        dm_copy(c, 0).start()
        mo_copy(c).start()

    def st_xf(c):
        wait(xa_copies(c))
        dm_copy(c, 0).wait_send()
        mo_copy(c).wait()
        start(xf_copies(c))
        dm_copy(c, 1).start()
        dm_copy(c, 2).start()

    def st_dm(c):
        wait(xf_copies(c))
        dm_copy(c, 1).wait_send()
        dm_copy(c, 2).wait_send()
        dm_copy(c, 3).start()

    def st_end(c):
        dm_copy(c, 3).wait_send()
        for i in range(4):
            dm_wait_recv(c, i)

    bodies = (st_sumsq, st_qkv, st_add1, st_rope, st_attend, st_ofwd, st_oproj, st_x1, st_x2, st_h, st_m, st_xf, st_dm, st_end)
    n_iter = max(n_chunks + 7, EARLY + len(bodies) - 1)

    @pl.loop(0, n_iter)
    def _(k):
        @pl.when(k >= 2)
        def _():
            at.take_credit(credit)

        for s, body in enumerate(bodies):
            stage(k, s, body)
            if s == 1:
                @pl.when(k + 1 < n_chunks)
                def _():
                    x_copy(k + 1).start()

        @pl.when(k < n_iter - 2)
        def _():
            at.give_credit(credit)


def attn_phase(x_in, gains, cos_t, sin_t, w_q, w_k, w_v, w_o, chunk):
    tokens, width = x_in.shape
    heads = w_q.shape[0]
    q_w = heads * 128
    n_chunks = tokens // chunk
    qb, hb = chunk // 4, chunk // 2
    xb = hb // 4
    hbm = pl.BlockSpec(memory_space=pl.ANY)
    vmem = pl.BlockSpec(memory_space=pltpu.VMEM)
    sem = pltpu.SemaphoreType.DMA
    S2, P2 = sem((2,)), sem((2, 2))
    vm = lambda *s: pltpu.VMEM(s, BF16)
    vf = lambda *s: pltpu.VMEM(s, F32)
    qkv_w = q_w + 256
    return pl.pallas_call(
        functools.partial(attn_kernel, n_chunks),
        out_shape=tuple(jax.ShapeDtypeStruct((n, width), BF16) for n in (EARLY * chunk, EARLY * xb, tokens - EARLY * chunk)),
        in_specs=[hbm, vmem, vmem, vmem, hbm, hbm, hbm, hbm],
        out_specs=(hbm, hbm, hbm),
        scratch_shapes=[
            vm(width, qkv_w), vm(q_w, width), vm(2, chunk, width), vm(chunk, width), vm(4, chunk, qkv_w),
            vm(4, 2, qb // 2, qkv_w), vm(4, 2, qb, qkv_w), vm(2, heads * qb, 128), vm(tokens, 256), vm(4, chunk, q_w),
            vm(4, chunk, width), vm(4, hb, width), vm(4, 2, xb // 2, width), vm(4, 2, xb, width), vm(2, xb, width), vm(4, xb, width), vm(4, xb, width),
            vf(chunk, 128), vf(chunk, 128), vf(n_chunks, 4, 8, 128), vf(n_chunks, 4, 8, 128),
            sem((heads + 3,)), S2, S2, S2, S2, S2, pltpu.SemaphoreType.REGULAR((5,)),
            sem((2, 3)), sem((n_chunks, 3)), P2, sem((4, 2)), P2, sem((4, 2)), sem((2, 3)), sem((n_chunks, 3)),
            P2, sem((4, 2)), P2, sem((4, 2)), S2, sem((4,)), P2, sem((4, 2)), P2, sem((4, 2)),
            sem((2, 3)), sem((n_chunks, 3)), P2, sem((n_chunks, 2)), P2, sem((n_chunks, 2)), sem((2, 4)), sem((n_chunks, 4)),
        ],
        compiler_params=pltpu.CompilerParams(collective_id=2, has_side_effects=True, vmem_limit_bytes=67043328),
        name="attn_phase",
    )(x_in, gains, cos_t, sin_t, w_q, w_k, w_v, w_o)


def solution(mesh, chunk=CHUNK):
    my_size = mesh.shape["my"]

    def local_layer(x_in, gain_attn, w_q, w_k, w_v, w_o, gain_mlp, w_gate, w_up, w_down):
        tokens, width = x_in.shape
        head = w_q.shape[-1]
        qb = chunk // my_size
        row = jnp.arange(tokens // my_size)
        positions = (row // qb) * chunk + lax.axis_index("my") * qb + row % qb
        half = head // 2
        inv_freq = ROPE_BASE ** (-jnp.arange(half, dtype=F32) / half)
        angles = positions.astype(F32)[:, None] * inv_freq[None, :]
        cos_h, sin_h = jnp.cos(angles), jnp.sin(angles)
        cos_t = jnp.concatenate([cos_h, cos_h], axis=-1)
        sin_t = jnp.concatenate([-sin_h, sin_h], axis=-1)
        gains = jnp.stack([gain_attn, gain_mlp]).astype(F32)
        m_early, h_early, o_part = attn_phase(
            x_in, gains, cos_t, sin_t, w_q.transpose(1, 0, 2), w_k.reshape(width, -1), w_v.reshape(width, -1), w_o.reshape(-1, width), chunk)
        return mlp_phase(x_in, gains, m_early, h_early, o_part, w_gate, w_up, w_down, chunk)

    in_specs = (P("dp", "my"), P("my"), P("my", "mx", None), P("my", "mx", None), P("my", "mx", None), P("mx", None, "my"), P("my"), P("my", "mx"), P("my", "mx"), P("mx", "my"))
    return jax.shard_map(local_layer, mesh=mesh, in_specs=in_specs, out_specs=P("dp", "my"), check_vma=False)
```

```python
import functools

import jax
import jax.numpy as jnp
from jax import lax
from jax.experimental import pallas as pl
from jax.experimental.pallas import tpu as pltpu
from jax.sharding import PartitionSpec as P

ROPE_BASE = 10000.0
NORM_EPS = 1e-6
CHUNK = 512
EARLY = 2
MESH = pl.DeviceIdType.MESH
F32 = jnp.float32
BF16 = jnp.bfloat16


class Place:
    def __init__(self):
        self.y = lax.axis_index("my")
        mx = lax.axis_index("mx")
        self.x = mx // 2
        self.core = mx % 2
        self.yp = (self.y + 1) % 4
        self.ym = (self.y + 3) % 4
        self.yo = (self.y + 2) % 4
        self.xp = (self.x + 1) % 4
        self.xm = (self.x + 3) % 4
        self.xo = (self.x + 2) % 4
        self.dev_yp = {"my": self.yp}
        self.dev_ym = {"my": self.ym}
        self.dev_xp = {"mx": self.xp * 2 + self.core}
        self.dev_xm = {"mx": self.xm * 2 + self.core}
        self.dev_core = {"mx": self.x * 2 + (1 - self.core)}
        self.dev_yo = {"my": self.yo}
        self.ys = (self.dev_yp, self.dev_ym)
        self.xs = (self.dev_xp, self.dev_xm)
        self.partners = (self.dev_yp, self.dev_ym, self.dev_xp, self.dev_xm, self.dev_core)

    def entry(self, extra=()):
        barrier = pltpu.get_barrier_semaphore()
        for dev in self.partners + extra:
            pl.semaphore_signal(barrier, inc=1, device_id=dev, device_id_type=MESH)
        pl.semaphore_wait(barrier, len(self.partners) + len(extra))

    def give_credit(self, credit):
        for slot, dev in ((1, self.dev_yp), (0, self.dev_ym), (3, self.dev_xp), (2, self.dev_xm), (4, self.dev_core)):
            pl.semaphore_signal(credit.at[slot], inc=1, device_id=dev, device_id_type=MESH)

    def take_credit(self, credit):
        for slot in range(5):
            pl.semaphore_wait(credit.at[slot], 1)


def rcopy(src, dst, send_sem, recv_sem, dev):
    return pltpu.make_async_remote_copy(src_ref=src, dst_ref=dst, send_sem=send_sem, recv_sem=recv_sem, device_id=dev, device_id_type=MESH)


def as_row(col_b):
    eye = lax.broadcasted_iota(jnp.int32, col_b.shape, 0) == lax.broadcasted_iota(jnp.int32, col_b.shape, 1)
    return jnp.sum(jnp.where(eye, col_b, 0.0), axis=0, keepdims=True)


def as_col(row, r):
    shape = (r, row.shape[1])
    eye = lax.broadcasted_iota(jnp.int32, shape, 0) == lax.broadcasted_iota(jnp.int32, shape, 1)
    return jnp.sum(jnp.where(eye, jnp.broadcast_to(row, shape), 0.0), axis=1, keepdims=True)


def square_sum(v):
    vf = v.astype(F32)
    return jnp.sum(vf * vf, axis=-1, keepdims=True)


def inv_rms(st, c, full_width):
    tot = (st[c, 0] + st[c, 1]) + (st[c, 2] + st[c, 3])
    return lax.rsqrt(tot / full_width + NORM_EPS)


def two(srcs, dsts, send, recv, devs):
    return [rcopy(src, dst, send.at[i], recv.at[i], dev) for i, (src, dst, dev) in enumerate(zip(srcs, dsts, devs))]


def slots(ref):
    return [ref.at[i] for i in range(2)]


def start(copies):
    for c in copies:
        c.start()


def wait(copies):
    for c in copies:
        c.wait()


def rows(start, size, align):
    return pl.ds(pl.multiple_of(start, align), size)


def mlp_kernel(n_chunks, x_hbm, gains, me_hbm, he_hbm, wp_hbm, wg_hbm, wu_hbm, wd_hbm, y_hbm, ml_hbm, hl_hbm,
               WG, WU, WD, M, PP, R1, R2, ACT, DP, DR, XR1, XR2, YB, H, OP, OR, OX1, OX2, XH, HB, MO, ST,
               w_sem, m_sem, h_sem, y_sem, o_sem, ods, odr, oxs, oxr, ots, otr, oms, omr, credit, s1s, s1r, s2s, s2r, acs, acr, fws, fwr, dds, ddr, x1s, x1r, x2s, x2r, xas, xar, xfs, xfr, dys, dyr):
    at = Place()
    tc, width = M.shape
    ff = WG.shape[1]
    qb = tc // 4
    hq = qb // 2
    hb = tc // 2
    xb = hb // 4
    hx = xb // 2
    gu_tiles = 5
    gu_w = ff // gu_tiles
    dn_w = 256 if width % 256 == 0 else 128

    def m_wait():
        pltpu.make_async_copy(me_hbm.at[pl.ds(0, tc)], M, m_sem).wait()

    def m_start(c):
        @pl.when(c < EARLY)
        def _():
            pltpu.make_async_copy(me_hbm.at[rows(c * tc, tc, tc)], M, m_sem).start()

        @pl.when(c >= EARLY)
        def _():
            pltpu.make_async_copy(ml_hbm.at[rows((c - EARLY) * tc, tc, tc)], M, m_sem).start()

    def gu_copies(n):
        cols = rows(n * gu_w, gu_w, 128)
        return [pltpu.make_async_copy(wg_hbm.at[:, cols], WG.at[:, cols], w_sem.at[n]),
                pltpu.make_async_copy(wu_hbm.at[:, cols], WU.at[:, cols], w_sem.at[gu_tiles + n])]

    wd_copy = pltpu.make_async_copy(wd_hbm, WD, w_sem.at[2 * gu_tiles])
    pltpu.make_async_copy(me_hbm.at[pl.ds(0, tc)], M, m_sem).start()
    for n in range(gu_tiles):
        start(gu_copies(n))
    wd_copy.start()
    at.entry(extra=(at.dev_yo,))

    def gu_part(par, lo, hi):
        @pl.loop(lo, hi)
        def _(n):
            g_cols = rows(n * gu_w, gu_w, 128)
            PP[par, :, g_cols] = jnp.dot(M[...], WG[:, g_cols], preferred_element_type=F32).astype(BF16)
            PP[par, :, rows(ff + n * gu_w, gu_w, 128)] = jnp.dot(M[...], WU[:, g_cols], preferred_element_type=F32).astype(BF16)

    def s1_copies(par):
        o = at.yo * qb
        return two([PP.at[par, rows(r, hq, hq)] for r in (o, o + hq)], slots(R1), s1s, s1r, at.ys)

    def s2_copies(par):
        return two([PP.at[par, rows(b * qb, qb, qb)] for b in (at.yp, at.ym)], slots(R2.at[par]), s2s.at[par], s2r.at[par], at.ys)

    def act_copies(par):
        own = [ACT.at[par, rows(at.y * qb, qb, qb)]] * 2
        return two(own, own, acs, acr, at.ys)

    def fwd_copies(par):
        half = [ACT.at[par, rows(r, hq, hq)] for r in (at.ym * qb, at.yp * qb + hq)]
        return two(half, half, fws.at[par], fwr.at[par], at.ys)

    def dd_copy():
        return rcopy(DP.at[rows((1 - at.core) * hb, hb, hb)], DR, dds, ddr, at.dev_core)

    def last_copy():
        return rcopy(DP.at[rows((1 - at.core) * hb, hb, hb)], OR, ods, odr, at.dev_core)

    def down(par):
        @pl.loop(0, width // dn_w)
        def _(n):
            cols = rows(n * dn_w, dn_w, 128)
            DP[:, cols] = jnp.dot(ACT[par], WD[:, cols], preferred_element_type=F32).astype(BF16)

    own_half = at.core * hb

    def core_add(part):
        @pl.loop(0, hb // 16)
        def _(i):
            ri = rows(i * 16, 16, 16)
            ra = rows(own_half + i * 16, 16, 16)
            DP[ra, :] = (DP[ra, :].astype(F32) + part[ri, :].astype(F32)).astype(BF16)

        start(x1_copies())

    def x1_copies():
        o = own_half + at.xo * xb
        return two([DP.at[rows(r, hx, hx)] for r in (o, o + hx)], slots(XR1), x1s, x1r, at.xs)

    def x2_copies():
        return two([DP.at[rows(own_half + b * xb, xb, xb)] for b in (at.xp, at.xm)], slots(XR2), x2s, x2r, at.xs)

    def yblk(b):
        return YB.at[rows(own_half + b * xb, xb, xb)]

    def xa_copies():
        own = [yblk(at.x)] * 2
        return two(own, own, xas, xar, at.xs)

    def xf_copies():
        half = [YB.at[rows(own_half + r, hx, hx)] for r in (at.xm * xb, at.xp * xb + hx)]
        return two(half, half, xfs, xfr, at.xs)

    def dy_copy(i):
        b = (at.x, at.xm, at.xp, at.xo)[i]
        return rcopy(yblk(b), yblk(b), dys.at[i], dyr.at[i], at.dev_core)

    def dy_wait_recv(i):
        b = (at.x, at.xm, at.xp, at.xo)[i]
        other = YB.at[rows((1 - at.core) * hb + b * xb, xb, xb)]
        rcopy(other, other, dys.at[i], dyr.at[i], at.dev_core).wait_recv()

    def h_wait():
        pltpu.make_async_copy(he_hbm.at[pl.ds(0, xb)], H, h_sem).wait()

    def h_start(c):
        @pl.when(c < EARLY)
        def _():
            pltpu.make_async_copy(he_hbm.at[rows(c * xb, xb, xb)], H, h_sem).start()

        @pl.when(c >= EARLY)
        def _():
            pltpu.make_async_copy(hl_hbm.at[rows((c - EARLY) * xb, xb, xb)], H, h_sem).start()

    def y_copy(c):
        return pltpu.make_async_copy(YB, y_hbm.at[rows(c * tc, tc, tc)], y_sem)

    my_rows = own_half + at.x * xb
    peers = at.ys + (at.dev_yo,)

    def od_copy(c):
        return rcopy(wp_hbm.at[rows((c - EARLY) * tc + (1 - at.core) * hb, hb, hb)], OR, ods, odr, at.dev_core)

    def op_copy(c):
        return pltpu.make_async_copy(wp_hbm.at[rows((c - EARLY) * tc + own_half, hb, hb)], OP, o_sem.at[0])

    def xh_copy(c):
        return pltpu.make_async_copy(x_hbm.at[rows(c * tc + my_rows, xb, xb)], XH, o_sem.at[1])

    def hl_copy(c):
        return pltpu.make_async_copy(HB, hl_hbm.at[rows((c - EARLY) * xb, xb, xb)], o_sem.at[2])

    def ml_rows(c, first, size):
        return ml_hbm.at[rows((c - EARLY) * tc + first, size, size)]

    def mo_copy(c):
        return pltpu.make_async_copy(MO, ml_rows(c, my_rows, xb), o_sem.at[3])

    def o1_copies():
        return two([OP.at[rows(at.xo * xb + r, hx, hx)] for r in (0, hx)], slots(OX1), oxs.at[0], oxr.at[0], at.xs)

    def o2_copies():
        return two([OP.at[rows(b * xb, xb, xb)] for b in (at.xp, at.xm)], slots(OX2), oxs.at[1], oxr.at[1], at.xs)

    def ot_copies(c):
        own = ST.at[c, at.y]
        return [rcopy(own, own, ots.at[i], otr.at[c, i], dev) for i, dev in enumerate(peers)]

    def oa_copies(c):
        return two([MO] * 2, [ml_rows(c, my_rows, xb)] * 2, oxs.at[2], oxr.at[2], at.xs)

    def of_copies(c):
        half = [ml_rows(c, own_half + r, hx) for r in (at.xm * xb, at.xp * xb + hx)]
        return two(half, half, oxs.at[3], oxr.at[3], at.xs)

    def om_copy(c, i):
        b = ml_rows(c, own_half + (at.x, at.xm, at.xp, at.xo)[i] * xb, xb)
        return rcopy(MO if i == 0 else b, b, oms.at[i], omr.at[i], at.dev_core)

    def om_wait_recv(c, i):
        b = ml_rows(c, (1 - at.core) * hb + (at.x, at.xm, at.xp, at.xo)[i] * xb, xb)
        rcopy(b, b, oms.at[i], omr.at[i], at.dev_core).wait_recv()

    def o_begin(c):
        od_copy(c).start()
        op_copy(c).start()
        xh_copy(c).start()

    def o_core(c):
        od_copy(c).wait()
        op_copy(c).wait()

        @pl.loop(0, hb // 16)
        def _(i):
            r = rows(i * 16, 16, 16)
            OP[r, :] = (OP[r, :].astype(F32) + OR[r, :].astype(F32)).astype(BF16)

        start(o1_copies())

    def o_ring(c):
        wait(o1_copies())
        ra = rows(at.xp * xb, hx, hx)
        rb = rows(at.xm * xb + hx, hx, hx)
        OP[ra, :] = (OP[ra, :].astype(F32) + OX1[0].astype(F32)).astype(BF16)
        OP[rb, :] = (OP[rb, :].astype(F32) + OX1[1].astype(F32)).astype(BF16)
        start(o2_copies())

    def o_sum(c):
        wait(o2_copies())
        xh_copy(c).wait()
        total = OP[rows(at.x * xb, xb, xb), :].astype(F32) + OX2[0].astype(F32) + OX2[1].astype(F32)
        h = (XH[...].astype(F32) + total).astype(BF16)
        HB[...] = h
        ST[c, at.y] = jnp.broadcast_to(as_row(jnp.broadcast_to(square_sum(h), (xb, 128))), (8, 128))
        start(ot_copies(c))
        hl_copy(c).start()

    def o_norm(c):
        wait(ot_copies(c))
        hl_copy(c).wait()
        inv = as_col(inv_rms(ST, c, width * 4)[0:1, :], xb)
        MO[...] = (HB[...].astype(F32) * inv * gains[1:2, :]).astype(BF16)
        start(oa_copies(c))
        om_copy(c, 0).start()
        mo_copy(c).start()

    def o_pass(c):
        wait(oa_copies(c))
        mo_copy(c).wait()
        start(of_copies(c))
        om_copy(c, 1).start()
        om_copy(c, 2).start()

    def o_last(c):
        wait(of_copies(c))
        om_copy(c, 3).start()

    def o_end(c):
        for i in range(4):
            om_copy(c, i).wait_send()
            om_wait_recv(c, i)

    m_wait()
    for i, b in enumerate((at.yo, at.yp, at.ym, at.y)):
        br = rows(b * qb, qb, qb)

        @pl.loop(0, gu_tiles)
        def _(n):
            if i == 0:
                wait(gu_copies(n))
            g_cols = rows(n * gu_w, gu_w, 128)
            PP[0, br, g_cols] = jnp.dot(M[br, :], WG[:, g_cols], preferred_element_type=F32).astype(BF16)
            PP[0, br, rows(ff + n * gu_w, gu_w, 128)] = jnp.dot(M[br, :], WU[:, g_cols], preferred_element_type=F32).astype(BF16)

        if i == 0:
            start(s1_copies(0))
    wd_copy.wait()

    @pl.loop(0, n_chunks + 2)
    def _(k):
        par = k % 2
        alt = (k + 1) % 2
        has_s = k < n_chunks
        has_gu = k + 1 < n_chunks
        has_a = jnp.logical_and(k >= 1, k - 1 < n_chunks)
        has_d = k >= 2

        @pl.when(k >= 1)
        def _():
            at.take_credit(credit)

        @pl.when(jnp.logical_and(has_s, k >= 1))
        def _():
            start(s1_copies(par))

        @pl.when(has_d)
        def _():
            h_start(k - 2)

        def o_step(body):
            @pl.when(k + EARLY < n_chunks)
            def _():
                body(k + EARLY)

        def m_step(body):
            @pl.when(jnp.logical_and(k + 1 >= EARLY, has_gu))
            def _():
                body(k + 1)

        o_step(o_begin)
        m_step(o_norm)

        @pl.when(has_a)
        def _():
            wait(s2_copies(alt))
            base = at.y * qb
            step = 16

            @pl.loop(0, qb // step)
            def _(i):
                r = rows(base + i * step, step, step)
                r2 = rows(i * step, step, step)
                g = PP[alt, r, 0:ff].astype(F32) + R2[alt, 0, r2, 0:ff].astype(F32) + R2[alt, 1, r2, 0:ff].astype(F32)
                u = PP[alt, r, ff:2 * ff].astype(F32) + R2[alt, 0, r2, ff:2 * ff].astype(F32) + R2[alt, 1, r2, ff:2 * ff].astype(F32)
                ACT[alt, r, :] = (g * jax.nn.sigmoid(g) * u).astype(BF16)

            start(act_copies(alt))

        m_step(o_pass)

        is_last = k == n_chunks + 1
        has_dd = jnp.logical_and(has_d, k < n_chunks + 1)

        @pl.when(has_dd)
        def _():
            wait(fwd_copies(par))
            down(par)
            dd_copy().start()

        o_step(o_core)
        m_step(o_last)

        @pl.when(has_s)
        def _():
            wait(s1_copies(par))
            step = 16

            @pl.loop(0, hq // step)
            def _(i):
                ri = rows(i * step, step, step)
                ra = rows(at.yp * qb + i * step, step, step)
                rb = rows(at.ym * qb + hq + i * step, step, step)
                PP[par, ra, :] = (PP[par, ra, :].astype(F32) + R1[0, ri, :].astype(F32)).astype(BF16)
                PP[par, rb, :] = (PP[par, rb, :].astype(F32) + R1[1, ri, :].astype(F32)).astype(BF16)

            start(s2_copies(par))

        o_step(o_ring)
        m_step(o_end)

        @pl.when(has_gu)
        def _():
            m_start(k + 1)

        @pl.when(has_dd)
        def _():
            dd_copy().wait()
            core_add(DR)

        @pl.when(is_last)
        def _():
            last_copy().wait()
            core_add(OR)

        @pl.when(has_gu)
        def _():
            m_wait()
            gu_part(alt, 0, 2)

        o_step(o_sum)

        @pl.when(has_d)
        def _():
            wait(x1_copies())
            ra = rows(own_half + at.xp * xb, hx, hx)
            rb = rows(own_half + at.xm * xb + hx, hx, hx)
            DP[ra, :] = (DP[ra, :].astype(F32) + XR1[0].astype(F32)).astype(BF16)
            DP[rb, :] = (DP[rb, :].astype(F32) + XR1[1].astype(F32)).astype(BF16)
            start(x2_copies())

        @pl.when(has_gu)
        def _():
            gu_part(alt, 2, 3)

        @pl.when(has_a)
        def _():
            wait(act_copies(alt))
            start(fwd_copies(alt))

        @pl.when(has_d)
        def _():
            wait(x2_copies())
            h_wait()
            r = rows(own_half + at.x * xb, xb, xb)
            down = DP[r, :].astype(F32) + XR2[0].astype(F32) + XR2[1].astype(F32)
            YB[r, :] = (H[...].astype(F32) + down).astype(BF16)
            start(xa_copies())
            dy_copy(0).start()

        @pl.when(k == n_chunks)
        def _():
            wait(fwd_copies(alt))
            down(alt)
            last_copy().start()

        @pl.when(has_gu)
        def _():
            gu_part(alt, 3, 4)

        @pl.when(has_d)
        def _():
            wait(xa_copies())
            start(xf_copies())
            dy_copy(1).start()
            dy_copy(2).start()

        @pl.when(has_gu)
        def _():
            gu_part(alt, 4, 5)

        @pl.when(has_d)
        def _():
            wait(xf_copies())
            dy_copy(3).start()
            for i in range(4):
                dy_copy(i).wait_send()
                dy_wait_recv(i)
            y_copy(k - 2).start()
            y_copy(k - 2).wait()

        @pl.when(k < n_chunks + 1)
        def _():
            at.give_credit(credit)


def mlp_phase(x_in, gains, m_early, h_early, o_part, w_gate, w_up, w_down, chunk):
    tokens, width = x_in.shape
    ff = w_gate.shape[1]
    n_chunks = tokens // chunk
    qb, hb = chunk // 4, chunk // 2
    xb = hb // 4
    hbm = pl.BlockSpec(memory_space=pl.ANY)
    sem = pltpu.SemaphoreType.DMA
    S2, P2 = sem((2,)), sem((2, 2))
    vm = lambda *s: pltpu.VMEM(s, BF16)
    return pl.pallas_call(
        functools.partial(mlp_kernel, n_chunks),
        out_shape=tuple(jax.ShapeDtypeStruct((n, width), BF16) for n in (tokens, tokens - EARLY * chunk, tokens // 8 - EARLY * xb)),
        in_specs=[hbm, pl.BlockSpec(memory_space=pltpu.VMEM)] + [hbm] * 6,
        out_specs=(hbm, hbm, hbm),
        scratch_shapes=[
            vm(width, ff), vm(width, ff), vm(ff, width), vm(chunk, width), vm(2, chunk, 2 * ff),
            vm(2, qb // 2, 2 * ff), vm(2, 2, qb, 2 * ff), vm(2, chunk, ff), vm(chunk, width), vm(hb, width),
            vm(2, xb // 2, width), vm(2, xb, width), vm(chunk, width), vm(xb, width),
            vm(hb, width), vm(hb, width), vm(2, xb // 2, width), vm(2, xb, width), vm(xb, width), vm(xb, width), vm(xb, width),
            pltpu.VMEM((n_chunks, 4, 8, 128), F32),
            sem((11,)), sem, sem, sem, sem((4,)), sem, sem, sem((4, 2)), sem((4, 2)), sem((3,)), sem((n_chunks, 3)), sem((4,)), sem((4,)), pltpu.SemaphoreType.REGULAR((5,)),
            S2, S2, P2, P2, S2, S2, P2, P2,
            sem, sem, S2, S2, S2, S2, S2, S2, S2, S2, sem((4,)), sem((4,)),
        ],
        compiler_params=pltpu.CompilerParams(collective_id=1, has_side_effects=True, vmem_limit_bytes=67043328),
        name="mlp_phase",
    )(x_in, gains, m_early, h_early, o_part, w_gate, w_up, w_down)[0]


def attn_kernel(n_chunks, x_hbm, gains, cos_t, sin_t, wq_hbm, wk_hbm, wv_hbm, wo_hbm, m_hbm, h_hbm, wp_hbm,
                WQKV, WO, X, N, QP, R1, R2, QS, KV, O, WP, DR, XR1, XR2, XH, HB, MO, SQ, RC, ST1, ST2,
                w_sem, x_sem, xh_sem, hb_sem, mo_sem, wp_sem, credit,
                t1s, t1r, s1s, s1r, s2s, s2r, kvs, kvr, kfs, kfr, ocs, ocr, ofs, ofr, dds, ddr, x1s, x1r, x2s, x2r, t2s, t2r, xas, xar, xfs, xfr, dms, dmr):
    at = Place()
    tc, width = N.shape
    full_width = width * 4
    qkv_w = WQKV.shape[1]
    head = 128
    heads = QS.shape[1] // (tc // 4)
    q_w = heads * head
    qb = tc // 4
    hq = qb // 2
    hb = tc // 2
    xb = hb // 4
    hx = xb // 2
    own_half = at.core * hb
    my_rows = own_half + at.x * xb
    peers = at.ys + (at.dev_yo,)
    blk = min(128, tc)
    n_blk = tc // blk
    step = 16

    w_copies = [
        pltpu.make_async_copy(w, WQKV.at[:, pl.ds(i * head, head)], w_sem.at[i])
        for i, w in enumerate([wq_hbm.at[h] for h in range(heads)] + [wk_hbm, wv_hbm])
    ] + [pltpu.make_async_copy(wo_hbm, WO, w_sem.at[heads + 2])]

    def x_copy(c):
        return pltpu.make_async_copy(x_hbm.at[rows(c * tc, tc, tc)], X.at[c % 2], x_sem.at[c % 2])

    x_copy(0).start()
    for c in w_copies:
        c.start()
    at.entry(extra=(at.dev_yo,))

    def slot(c):
        return c % 4

    def pair(c):
        return c % 2

    def stats_copies(st, ssem, rsem, c):
        own = st.at[c, at.y]
        return [rcopy(own, own, ssem.at[pair(c), i], rsem.at[c, i], dev) for i, dev in enumerate(peers)]

    def s1_copies(c):
        s, o = slot(c), at.yo * qb
        return two([QP.at[s, rows(r, hq, hq)] for r in (o, o + hq)], slots(R1.at[s]), s1s.at[pair(c)], s1r.at[s], at.ys)

    def s2_copies(c):
        s = slot(c)
        return two([QP.at[s, rows(b * qb, qb, qb)] for b in (at.yp, at.ym)], slots(R2.at[s]), s2s.at[pair(c)], s2r.at[s], at.ys)

    def kv_copies(c):
        own = [KV.at[rows(c * tc + at.y * qb, qb, qb)]] * 2
        return two(own, own, kvs.at[pair(c)], kvr.at[c], at.ys)

    def kf_copies(c):
        half = [KV.at[rows(c * tc + r, hq, hq)] for r in (at.ym * qb, at.yp * qb + hq)]
        return two(half, half, kfs.at[pair(c)], kfr.at[c], at.ys)

    def o_copies(c):
        own = [O.at[slot(c), rows(at.y * qb, qb, qb)]] * 2
        return two(own, own, ocs.at[pair(c)], ocr.at[slot(c)], at.ys)

    def of_copies(c):
        half = [O.at[slot(c), rows(r, hq, hq)] for r in (at.ym * qb, at.yp * qb + hq)]
        return two(half, half, ofs.at[pair(c)], ofr.at[slot(c)], at.ys)

    def dd_copies(c):
        s = slot(c)
        return [rcopy(WP.at[s, rows((1 - at.core) * hb, hb, hb)], DR.at[s], dds.at[pair(c)], ddr.at[s], at.dev_core)]

    def x1_copies(c):
        s, o = slot(c), own_half + at.xo * xb
        return two([WP.at[s, rows(r, hx, hx)] for r in (o, o + hx)], slots(XR1.at[s]), x1s.at[pair(c)], x1r.at[s], at.xs)

    def x2_copies(c):
        s = slot(c)
        return two([WP.at[s, rows(own_half + b * xb, xb, xb)] for b in (at.xp, at.xm)], slots(XR2.at[s]), x2s.at[pair(c)], x2r.at[s], at.xs)

    def m_rows(c, start, size):
        return m_hbm.at[rows(c * tc + start, size, size)]

    def xa_copies(c):
        return two([MO.at[slot(c)]] * 2, [m_rows(c, my_rows, xb)] * 2, xas.at[pair(c)], xar.at[c], at.xs)

    def xf_copies(c):
        half = [m_rows(c, own_half + r, hx) for r in (at.xm * xb, at.xp * xb + hx)]
        return two(half, half, xfs.at[pair(c)], xfr.at[c], at.xs)

    def dm_copy(c, i):
        if i == 0:
            return rcopy(MO.at[slot(c)], m_rows(c, my_rows, xb), dms.at[pair(c), 0], dmr.at[c, 0], at.dev_core)
        b = m_rows(c, own_half + (at.xm, at.xp, at.xo)[i - 1] * xb, xb)
        return rcopy(b, b, dms.at[pair(c), i], dmr.at[c, i], at.dev_core)

    def dm_wait_recv(c, i):
        b = m_rows(c, (1 - at.core) * hb + (at.x, at.xm, at.xp, at.xo)[i] * xb, xb)
        rcopy(b, b, dms.at[pair(c), i], dmr.at[c, i], at.dev_core).wait_recv()

    def xh_copy(c):
        return pltpu.make_async_copy(x_hbm.at[rows(c * tc + my_rows, xb, xb)], XH.at[pair(c)], xh_sem.at[pair(c)])

    def hb_copy(c):
        return pltpu.make_async_copy(HB.at[slot(c)], h_hbm.at[rows(c * xb, xb, xb)], hb_sem.at[pair(c)])

    def mo_copy(c):
        return pltpu.make_async_copy(MO.at[slot(c)], m_rows(c, my_rows, xb), mo_sem.at[pair(c)])

    def wp_copy(c):
        return pltpu.make_async_copy(WP.at[slot(c)], wp_hbm.at[rows((c - EARLY) * tc, tc, tc)], wp_sem.at[pair(c)])

    def stage(k, s, body):
        c = k - s

        @pl.when(jnp.logical_and(c >= 0, c < (EARLY if s >= 8 else n_chunks)))
        def _():
            body(c)

    def st_sumsq(c):
        x_copy(c).wait()

        @pl.loop(0, tc // step)
        def _(i):
            r = rows(i * step, step, step)
            SQ[r, :] = jnp.broadcast_to(square_sum(X[c % 2, r, :]), (step, 128))

        parts = [as_row(SQ[b * blk:(b + 1) * blk, :]) for b in range(n_blk)]
        parts = parts + [jnp.zeros_like(parts[0])] * (8 - n_blk)
        ST1[c, at.y] = jnp.concatenate(parts, axis=0)
        start(stats_copies(ST1, t1s, t1r, c))

    def st_qkv(c):
        wait(stats_copies(ST1, t1s, t1r, c))

        @pl.when(c == 0)
        def _():
            wait(w_copies[:-1])

        inv = inv_rms(ST1, c, full_width)
        for b in range(n_blk):
            RC[b * blk:(b + 1) * blk, :] = jnp.broadcast_to(as_col(inv[b:b + 1, :], blk), (blk, 128))

        @pl.loop(0, tc // step)
        def _(i):
            r = rows(i * step, step, step)
            N[r, :] = (X[c % 2, r, :].astype(F32) * RC[r, 0:1] * gains[0:1, :]).astype(BF16)

        n_t = qkv_w // 384

        @pl.loop(0, n_t)
        def _(n):
            cols = rows(n * 384, 384, 128)
            QP[slot(c), :, cols] = jnp.dot(N[...], WQKV[:, cols], preferred_element_type=F32).astype(BF16)

        start(s1_copies(c))

    def st_add1(c):
        wait(s1_copies(c))
        s = slot(c)

        @pl.loop(0, hq // step)
        def _(i):
            ri = rows(i * step, step, step)
            ra = rows(at.yp * qb + i * step, step, step)
            rb = rows(at.ym * qb + hq + i * step, step, step)
            QP[s, ra, :] = (QP[s, ra, :].astype(F32) + R1[s, 0, ri, :].astype(F32)).astype(BF16)
            QP[s, rb, :] = (QP[s, rb, :].astype(F32) + R1[s, 1, ri, :].astype(F32)).astype(BF16)

        start(s2_copies(c))

    def st_rope(c):
        wait(s2_copies(c))
        s = slot(c)
        own = rows(at.y * qb, qb, qb)
        cos_v = cos_t[rows(c * qb, qb, qb), :]
        sin_v = sin_t[rows(c * qb, qb, qb), :]

        def piece(i):
            cols = slice(i * head, (i + 1) * head)
            v = QP[s, own, cols].astype(F32) + R2[s, 0, :, cols].astype(F32) + R2[s, 1, :, cols].astype(F32)
            return v.astype(BF16)

        def turned(i):
            v = piece(i).astype(F32)
            return (v * cos_v + pltpu.roll(v, head // 2, 1) * sin_v).astype(BF16)

        kv_rows = rows(c * tc + at.y * qb, qb, qb)
        KV[kv_rows, 0:head] = turned(heads)
        KV[kv_rows, head:2 * head] = piece(heads + 1)
        start(kv_copies(c))
        for i in range(heads):
            QS[pair(c), i * qb:(i + 1) * qb, :] = turned(i)

    def st_kvfwd(c):
        wait(kv_copies(c))
        start(kf_copies(c))

    def st_attend(c):
        wait(kf_copies(c))
        q = QS[pair(c)]
        scale = head ** -0.5 * 1.4426950408889634

        def scores(j):
            keys = KV[rows(j * tc, tc, tc), 0:head]
            return lax.dot_general(q, keys, (((1,), (1,)), ((), ())), preferred_element_type=F32) * scale

        def values(j, p):
            return jnp.dot(p.astype(BF16), KV[rows(j * tc, tc, tc), head:2 * head], preferred_element_type=F32)

        qpos = at.y * qb + lax.broadcasted_iota(jnp.int32, (qb, tc), 0)
        keep = lax.broadcasted_iota(jnp.int32, (qb, tc), 1) <= qpos
        sc = scores(c).reshape(heads, qb, tc)
        sc = jnp.where(keep[None], sc, -jnp.inf).reshape(heads * qb, tc)
        top = jnp.max(sc, axis=-1, keepdims=True)
        p = jnp.exp2(sc - top)

        def more(j, carry):
            top, total, acc = carry
            sc = scores(j)
            new = jnp.maximum(top, jnp.max(sc, axis=-1, keepdims=True))
            fade = jnp.exp2(top - new)
            p = jnp.exp2(sc - new)
            return new, total * fade + jnp.sum(p, axis=-1, keepdims=True), acc * fade + values(j, p)

        top, total, acc = lax.fori_loop(0, c, more, (top, jnp.sum(p, axis=-1, keepdims=True), values(c, p)))
        out = (acc / total).astype(BF16)
        for i in range(heads):
            O[slot(c), rows(at.y * qb, qb, qb), i * head:(i + 1) * head] = out[i * qb:(i + 1) * qb, :]

    def st_osend(c):
        start(o_copies(c))

    def st_ofwd(c):
        wait(o_copies(c))
        start(of_copies(c))

    def st_oproj(c):
        wait(of_copies(c))

        @pl.when(c == 0)
        def _():
            w_copies[-1].wait()

        dn_w = 256 if width % 256 == 0 else 128

        @pl.loop(0, width // dn_w)
        def _(n):
            cols = rows(n * dn_w, dn_w, 128)
            WP[slot(c), :, cols] = jnp.dot(O[slot(c)], WO[:, cols], preferred_element_type=F32).astype(BF16)

        @pl.when(c < EARLY)
        def _():
            start(dd_copies(c))

        @pl.when(c >= EARLY)
        def _():
            wp_copy(c).start()

    def st_x1(c):
        @pl.when(c < EARLY)
        def _():
            st_x1_early(c)

        @pl.when(c >= EARLY)
        def _():
            wp_copy(c).wait()

    def st_x1_early(c):
        wait(dd_copies(c))
        s = slot(c)

        @pl.loop(0, hb // step)
        def _(i):
            ri = rows(i * step, step, step)
            ra = rows(own_half + i * step, step, step)
            WP[s, ra, :] = (WP[s, ra, :].astype(F32) + DR[s, ri, :].astype(F32)).astype(BF16)

        start(x1_copies(c))

    def st_x2(c):
        xh_copy(c).start()
        wait(x1_copies(c))
        s = slot(c)
        ra = rows(own_half + at.xp * xb, hx, hx)
        rb = rows(own_half + at.xm * xb + hx, hx, hx)
        WP[s, ra, :] = (WP[s, ra, :].astype(F32) + XR1[s, 0].astype(F32)).astype(BF16)
        WP[s, rb, :] = (WP[s, rb, :].astype(F32) + XR1[s, 1].astype(F32)).astype(BF16)
        start(x2_copies(c))

    def st_h(c):
        wait(x2_copies(c))
        xh_copy(c).wait()
        s = slot(c)
        total = WP[s, rows(my_rows, xb, xb), :].astype(F32) + XR2[s, 0].astype(F32) + XR2[s, 1].astype(F32)
        h = (XH[pair(c)].astype(F32) + total).astype(BF16)
        HB[s] = h
        row = as_row(jnp.broadcast_to(square_sum(h), (xb, 128)))
        ST2[c, at.y] = jnp.broadcast_to(row, (8, 128))
        start(stats_copies(ST2, t2s, t2r, c))
        hb_copy(c).start()

    def st_m(c):
        wait(stats_copies(ST2, t2s, t2r, c))
        hb_copy(c).wait()
        s = slot(c)
        inv = as_col(inv_rms(ST2, c, full_width)[0:1, :], xb)
        MO[s] = (HB[s].astype(F32) * inv * gains[1:2, :]).astype(BF16)
        start(xa_copies(c))
        dm_copy(c, 0).start()
        mo_copy(c).start()

    def st_xf(c):
        wait(xa_copies(c))
        dm_copy(c, 0).wait_send()
        mo_copy(c).wait()
        start(xf_copies(c))
        dm_copy(c, 1).start()
        dm_copy(c, 2).start()

    def st_dm(c):
        wait(xf_copies(c))
        dm_copy(c, 1).wait_send()
        dm_copy(c, 2).wait_send()
        dm_copy(c, 3).start()

    def st_end(c):
        dm_copy(c, 3).wait_send()
        for i in range(4):
            dm_wait_recv(c, i)

    steps = ((0, st_sumsq), (1, st_qkv), (2, st_add1), (3, st_rope), (4, st_attend), (3, st_kvfwd), (4, st_osend), (5, st_ofwd), (6, st_oproj),
             (7, st_x1), (8, st_x2), (9, st_h), (10, st_m), (11, st_xf), (12, st_dm), (13, st_end))
    n_iter = max(n_chunks + 7, EARLY + 13)

    @pl.loop(0, n_iter)
    def _(k):
        @pl.when(k >= 2)
        def _():
            at.take_credit(credit)

        for s, body in steps:
            stage(k, s, body)
            if body is st_qkv:
                @pl.when(k + 1 < n_chunks)
                def _():
                    x_copy(k + 1).start()

        @pl.when(k < n_iter - 2)
        def _():
            at.give_credit(credit)


def attn_phase(x_in, gains, cos_t, sin_t, w_q, w_k, w_v, w_o, chunk):
    tokens, width = x_in.shape
    heads = w_q.shape[0]
    q_w = heads * 128
    n_chunks = tokens // chunk
    qb, hb = chunk // 4, chunk // 2
    xb = hb // 4
    hbm = pl.BlockSpec(memory_space=pl.ANY)
    vmem = pl.BlockSpec(memory_space=pltpu.VMEM)
    sem = pltpu.SemaphoreType.DMA
    S2, P2 = sem((2,)), sem((2, 2))
    vm = lambda *s: pltpu.VMEM(s, BF16)
    vf = lambda *s: pltpu.VMEM(s, F32)
    qkv_w = q_w + 256
    return pl.pallas_call(
        functools.partial(attn_kernel, n_chunks),
        out_shape=tuple(jax.ShapeDtypeStruct((n, width), BF16) for n in (EARLY * chunk, EARLY * xb, tokens - EARLY * chunk)),
        in_specs=[hbm, vmem, vmem, vmem, hbm, hbm, hbm, hbm],
        out_specs=(hbm, hbm, hbm),
        scratch_shapes=[
            vm(width, qkv_w), vm(q_w, width), vm(2, chunk, width), vm(chunk, width), vm(4, chunk, qkv_w),
            vm(4, 2, qb // 2, qkv_w), vm(4, 2, qb, qkv_w), vm(2, heads * qb, 128), vm(tokens, 256), vm(4, chunk, q_w),
            vm(4, chunk, width), vm(4, hb, width), vm(4, 2, xb // 2, width), vm(4, 2, xb, width), vm(2, xb, width), vm(4, xb, width), vm(4, xb, width),
            vf(chunk, 128), vf(chunk, 128), vf(n_chunks, 4, 8, 128), vf(n_chunks, 4, 8, 128),
            sem((heads + 3,)), S2, S2, S2, S2, S2, pltpu.SemaphoreType.REGULAR((5,)),
            sem((2, 3)), sem((n_chunks, 3)), P2, sem((4, 2)), P2, sem((4, 2)), P2, sem((n_chunks, 2)), P2, sem((n_chunks, 2)),
            P2, sem((4, 2)), P2, sem((4, 2)), S2, sem((4,)), P2, sem((4, 2)), P2, sem((4, 2)),
            sem((2, 3)), sem((n_chunks, 3)), P2, sem((n_chunks, 2)), P2, sem((n_chunks, 2)), sem((2, 4)), sem((n_chunks, 4)),
        ],
        compiler_params=pltpu.CompilerParams(collective_id=2, has_side_effects=True, vmem_limit_bytes=67043328),
        name="attn_phase",
    )(x_in, gains, cos_t, sin_t, w_q, w_k, w_v, w_o)


def copy_kernel(src, dst, buf, in_sem, out_sem):
    n, part = buf.shape[:2]
    ins = [pltpu.make_async_copy(src.at[pl.ds(i * part, part)], buf.at[i], in_sem.at[i]) for i in range(n)]
    outs = [pltpu.make_async_copy(buf.at[i], dst.at[pl.ds(i * part, part)], out_sem.at[i]) for i in range(n)]
    start(ins)
    for i in range(n):
        ins[i].wait()
        outs[i].start()
    for c in outs:
        c.wait()


def copy_out(y):
    tokens, width = y.shape
    n = 16
    hbm = pl.BlockSpec(memory_space=pl.ANY)
    return pl.pallas_call(
        copy_kernel,
        out_shape=jax.ShapeDtypeStruct(y.shape, y.dtype),
        in_specs=[hbm],
        out_specs=hbm,
        scratch_shapes=[pltpu.VMEM((n, tokens // n, width), y.dtype), pltpu.SemaphoreType.DMA((n,)), pltpu.SemaphoreType.DMA((n,))],
        compiler_params=pltpu.CompilerParams(vmem_limit_bytes=67043328),
        name="copy_out",
    )(y)


def solution(mesh, chunk=CHUNK):
    my_size = mesh.shape["my"]

    def local_layer(x_in, gain_attn, w_q, w_k, w_v, w_o, gain_mlp, w_gate, w_up, w_down):
        tokens, width = x_in.shape
        head = w_q.shape[-1]
        qb = chunk // my_size
        row = jnp.arange(tokens // my_size)
        positions = (row // qb) * chunk + lax.axis_index("my") * qb + row % qb
        half = head // 2
        inv_freq = ROPE_BASE ** (-jnp.arange(half, dtype=F32) / half)
        angles = positions.astype(F32)[:, None] * inv_freq[None, :]
        cos_h, sin_h = jnp.cos(angles), jnp.sin(angles)
        cos_t = jnp.concatenate([cos_h, cos_h], axis=-1)
        sin_t = jnp.concatenate([-sin_h, sin_h], axis=-1)
        gains = jnp.stack([gain_attn, gain_mlp]).astype(F32)
        m_early, h_early, o_part = attn_phase(
            x_in, gains, cos_t, sin_t, w_q.transpose(1, 0, 2), w_k.reshape(width, -1), w_v.reshape(width, -1), w_o.reshape(-1, width), chunk)
        return copy_out(mlp_phase(x_in, gains, m_early, h_early, o_part, w_gate, w_up, w_down, chunk))

    in_specs = (P("dp", "my"), P("my"), P("my", "mx", None), P("my", "mx", None), P("my", "mx", None), P("mx", None, "my"), P("my"), P("my", "mx"), P("my", "mx"), P("mx", "my"))
    return jax.shard_map(local_layer, mesh=mesh, in_specs=in_specs, out_specs=P("dp", "my"), check_vma=False)
```

```python
import functools

import jax
import jax.numpy as jnp
from jax import lax
from jax.experimental import pallas as pl
from jax.experimental.pallas import tpu as pltpu
from jax.sharding import PartitionSpec as P

ROPE_BASE = 10000.0
NORM_EPS = 1e-6
CHUNK = 512
EARLY = 2
MESH = pl.DeviceIdType.MESH
F32 = jnp.float32
BF16 = jnp.bfloat16


class Place:
    def __init__(self):
        self.y = lax.axis_index("my")
        mx = lax.axis_index("mx")
        self.x = mx // 2
        self.core = mx % 2
        self.yp = (self.y + 1) % 4
        self.ym = (self.y + 3) % 4
        self.yo = (self.y + 2) % 4
        self.xp = (self.x + 1) % 4
        self.xm = (self.x + 3) % 4
        self.xo = (self.x + 2) % 4
        self.dev_yp = {"my": self.yp}
        self.dev_ym = {"my": self.ym}
        self.dev_xp = {"mx": self.xp * 2 + self.core}
        self.dev_xm = {"mx": self.xm * 2 + self.core}
        self.dev_core = {"mx": self.x * 2 + (1 - self.core)}
        self.dev_yo = {"my": self.yo}
        self.ys = (self.dev_yp, self.dev_ym)
        self.xs = (self.dev_xp, self.dev_xm)
        self.partners = (self.dev_yp, self.dev_ym, self.dev_xp, self.dev_xm, self.dev_core)

    def entry(self, extra=()):
        barrier = pltpu.get_barrier_semaphore()
        for dev in self.partners + extra:
            pl.semaphore_signal(barrier, inc=1, device_id=dev, device_id_type=MESH)
        pl.semaphore_wait(barrier, len(self.partners) + len(extra))

    def give_credit(self, credit):
        for slot, dev in ((1, self.dev_yp), (0, self.dev_ym), (3, self.dev_xp), (2, self.dev_xm), (4, self.dev_core)):
            pl.semaphore_signal(credit.at[slot], inc=1, device_id=dev, device_id_type=MESH)

    def take_credit(self, credit):
        for slot in range(5):
            pl.semaphore_wait(credit.at[slot], 1)


def rcopy(src, dst, send_sem, recv_sem, dev):
    return pltpu.make_async_remote_copy(src_ref=src, dst_ref=dst, send_sem=send_sem, recv_sem=recv_sem, device_id=dev, device_id_type=MESH)


def as_row(col_b):
    eye = lax.broadcasted_iota(jnp.int32, col_b.shape, 0) == lax.broadcasted_iota(jnp.int32, col_b.shape, 1)
    return jnp.sum(jnp.where(eye, col_b, 0.0), axis=0, keepdims=True)


def as_col(row, r):
    shape = (r, row.shape[1])
    eye = lax.broadcasted_iota(jnp.int32, shape, 0) == lax.broadcasted_iota(jnp.int32, shape, 1)
    return jnp.sum(jnp.where(eye, jnp.broadcast_to(row, shape), 0.0), axis=1, keepdims=True)


def square_sum(v):
    vf = v.astype(F32)
    return jnp.sum(vf * vf, axis=-1, keepdims=True)


def inv_rms(st, c, full_width):
    tot = (st[c, 0] + st[c, 1]) + (st[c, 2] + st[c, 3])
    return lax.rsqrt(tot / full_width + NORM_EPS)


def two(srcs, dsts, send, recv, devs):
    return [rcopy(src, dst, send.at[i], recv.at[i], dev) for i, (src, dst, dev) in enumerate(zip(srcs, dsts, devs))]


def slots(ref):
    return [ref.at[i] for i in range(2)]


def start(copies):
    for c in copies:
        c.start()


def wait(copies):
    for c in copies:
        c.wait()


def rows(start, size, align):
    return pl.ds(pl.multiple_of(start, align), size)


def mlp_kernel(n_chunks, x_hbm, gains, me_hbm, he_hbm, wp_hbm, wg_hbm, wu_hbm, wd_hbm, y_hbm, ml_hbm, hl_hbm,
               WG, WU, WD, M, PP, R1, R2, ACT, DP, DR, XR1, XR2, YB, H, OP, OR, OX1, OX2, XH, HB, MO, ST,
               w_sem, m_sem, h_sem, y_sem, o_sem, ods, odr, oxs, oxr, ots, otr, oms, omr, credit, s1s, s1r, s2s, s2r, acs, acr, fws, fwr, dds, ddr, x1s, x1r, x2s, x2r, xas, xar, xfs, xfr, dys, dyr):
    at = Place()
    tc, width = M.shape
    ff = WG.shape[1]
    qb = tc // 4
    hq = qb // 2
    hb = tc // 2
    xb = hb // 4
    hx = xb // 2
    gu_tiles = 5
    gu_w = ff // gu_tiles
    dn_w = 256 if width % 256 == 0 else 128

    def m_wait():
        pltpu.make_async_copy(me_hbm.at[pl.ds(0, tc)], M, m_sem).wait()

    def m_start(c):
        @pl.when(c < EARLY)
        def _():
            pltpu.make_async_copy(me_hbm.at[rows(c * tc, tc, tc)], M, m_sem).start()

        @pl.when(c >= EARLY)
        def _():
            pltpu.make_async_copy(ml_hbm.at[rows((c - EARLY) * tc, tc, tc)], M, m_sem).start()

    def gu_copies(n):
        cols = rows(n * gu_w, gu_w, 128)
        return [pltpu.make_async_copy(wg_hbm.at[:, cols], WG.at[:, cols], w_sem.at[n]),
                pltpu.make_async_copy(wu_hbm.at[:, cols], WU.at[:, cols], w_sem.at[gu_tiles + n])]

    wd_copy = pltpu.make_async_copy(wd_hbm, WD, w_sem.at[2 * gu_tiles])
    pltpu.make_async_copy(me_hbm.at[pl.ds(0, tc)], M, m_sem).start()
    for n in range(gu_tiles):
        start(gu_copies(n))
    wd_copy.start()
    at.entry(extra=(at.dev_yo,))

    def gu_part(par, lo, hi):
        @pl.loop(lo, hi)
        def _(n):
            g_cols = rows(n * gu_w, gu_w, 128)
            PP[par, :, g_cols] = jnp.dot(M[...], WG[:, g_cols], preferred_element_type=F32).astype(BF16)
            PP[par, :, rows(ff + n * gu_w, gu_w, 128)] = jnp.dot(M[...], WU[:, g_cols], preferred_element_type=F32).astype(BF16)

    def s1_copies(par):
        o = at.yo * qb
        return two([PP.at[par, rows(r, hq, hq)] for r in (o, o + hq)], slots(R1), s1s, s1r, at.ys)

    def s2_copies(par):
        return two([PP.at[par, rows(b * qb, qb, qb)] for b in (at.yp, at.ym)], slots(R2.at[par]), s2s.at[par], s2r.at[par], at.ys)

    def act_copies(par):
        own = [ACT.at[par, rows(at.y * qb, qb, qb)]] * 2
        return two(own, own, acs, acr, at.ys)

    def fwd_copies(par):
        half = [ACT.at[par, rows(r, hq, hq)] for r in (at.ym * qb, at.yp * qb + hq)]
        return two(half, half, fws.at[par], fwr.at[par], at.ys)

    def dd_copy():
        return rcopy(DP.at[rows((1 - at.core) * hb, hb, hb)], DR, dds, ddr, at.dev_core)

    def last_copy():
        return rcopy(DP.at[rows((1 - at.core) * hb, hb, hb)], OR, ods, odr, at.dev_core)

    def down(par):
        @pl.loop(0, width // dn_w)
        def _(n):
            cols = rows(n * dn_w, dn_w, 128)
            DP[:, cols] = jnp.dot(ACT[par], WD[:, cols], preferred_element_type=F32).astype(BF16)

    own_half = at.core * hb

    def core_add(part):
        @pl.loop(0, hb // 16)
        def _(i):
            ri = rows(i * 16, 16, 16)
            ra = rows(own_half + i * 16, 16, 16)
            DP[ra, :] = (DP[ra, :].astype(F32) + part[ri, :].astype(F32)).astype(BF16)

        start(x1_copies())

    def x1_copies():
        o = own_half + at.xo * xb
        return two([DP.at[rows(r, hx, hx)] for r in (o, o + hx)], slots(XR1), x1s, x1r, at.xs)

    def x2_copies():
        return two([DP.at[rows(own_half + b * xb, xb, xb)] for b in (at.xp, at.xm)], slots(XR2), x2s, x2r, at.xs)

    def yblk(b):
        return YB.at[rows(own_half + b * xb, xb, xb)]

    def xa_copies():
        own = [yblk(at.x)] * 2
        return two(own, own, xas, xar, at.xs)

    def xf_copies():
        half = [YB.at[rows(own_half + r, hx, hx)] for r in (at.xm * xb, at.xp * xb + hx)]
        return two(half, half, xfs, xfr, at.xs)

    def dy_copy(i):
        b = (at.x, at.xm, at.xp, at.xo)[i]
        return rcopy(yblk(b), yblk(b), dys.at[i], dyr.at[i], at.dev_core)

    def dy_wait_recv(i):
        b = (at.x, at.xm, at.xp, at.xo)[i]
        other = YB.at[rows((1 - at.core) * hb + b * xb, xb, xb)]
        rcopy(other, other, dys.at[i], dyr.at[i], at.dev_core).wait_recv()

    def h_wait():
        pltpu.make_async_copy(he_hbm.at[pl.ds(0, xb)], H, h_sem).wait()

    def h_start(c):
        @pl.when(c < EARLY)
        def _():
            pltpu.make_async_copy(he_hbm.at[rows(c * xb, xb, xb)], H, h_sem).start()

        @pl.when(c >= EARLY)
        def _():
            pltpu.make_async_copy(hl_hbm.at[rows((c - EARLY) * xb, xb, xb)], H, h_sem).start()

    def y_copy(c, core):
        return pltpu.make_async_copy(YB.at[rows(core * hb, hb, hb)], y_hbm.at[rows(c * tc + core * hb, hb, hb)], y_sem.at[core])

    my_rows = own_half + at.x * xb
    peers = at.ys + (at.dev_yo,)

    def od_copy(c):
        return rcopy(wp_hbm.at[rows((c - EARLY) * tc + (1 - at.core) * hb, hb, hb)], OR, ods, odr, at.dev_core)

    def op_copy(c):
        return pltpu.make_async_copy(wp_hbm.at[rows((c - EARLY) * tc + own_half, hb, hb)], OP, o_sem.at[0])

    def xh_copy(c):
        return pltpu.make_async_copy(x_hbm.at[rows(c * tc + my_rows, xb, xb)], XH, o_sem.at[1])

    def hl_copy(c):
        return pltpu.make_async_copy(HB, hl_hbm.at[rows((c - EARLY) * xb, xb, xb)], o_sem.at[2])

    def ml_rows(c, first, size):
        return ml_hbm.at[rows((c - EARLY) * tc + first, size, size)]

    def mo_copy(c):
        return pltpu.make_async_copy(MO, ml_rows(c, my_rows, xb), o_sem.at[3])

    def o1_copies():
        return two([OP.at[rows(at.xo * xb + r, hx, hx)] for r in (0, hx)], slots(OX1), oxs.at[0], oxr.at[0], at.xs)

    def o2_copies():
        return two([OP.at[rows(b * xb, xb, xb)] for b in (at.xp, at.xm)], slots(OX2), oxs.at[1], oxr.at[1], at.xs)

    def ot_copies(c):
        own = ST.at[c, at.y]
        return [rcopy(own, own, ots.at[i], otr.at[c, i], dev) for i, dev in enumerate(peers)]

    def oa_copies(c):
        return two([MO] * 2, [ml_rows(c, my_rows, xb)] * 2, oxs.at[2], oxr.at[2], at.xs)

    def of_copies(c):
        half = [ml_rows(c, own_half + r, hx) for r in (at.xm * xb, at.xp * xb + hx)]
        return two(half, half, oxs.at[3], oxr.at[3], at.xs)

    def om_copy(c, i):
        b = ml_rows(c, own_half + (at.x, at.xm, at.xp, at.xo)[i] * xb, xb)
        return rcopy(MO if i == 0 else b, b, oms.at[i], omr.at[i], at.dev_core)

    def om_wait_recv(c, i):
        b = ml_rows(c, (1 - at.core) * hb + (at.x, at.xm, at.xp, at.xo)[i] * xb, xb)
        rcopy(b, b, oms.at[i], omr.at[i], at.dev_core).wait_recv()

    def o_begin(c):
        od_copy(c).start()
        op_copy(c).start()
        xh_copy(c).start()

    def o_core(c):
        od_copy(c).wait()
        op_copy(c).wait()

        @pl.loop(0, hb // 16)
        def _(i):
            r = rows(i * 16, 16, 16)
            OP[r, :] = (OP[r, :].astype(F32) + OR[r, :].astype(F32)).astype(BF16)

        start(o1_copies())

    def o_ring(c):
        wait(o1_copies())
        ra = rows(at.xp * xb, hx, hx)
        rb = rows(at.xm * xb + hx, hx, hx)
        OP[ra, :] = (OP[ra, :].astype(F32) + OX1[0].astype(F32)).astype(BF16)
        OP[rb, :] = (OP[rb, :].astype(F32) + OX1[1].astype(F32)).astype(BF16)
        start(o2_copies())

    def o_sum(c):
        wait(o2_copies())
        xh_copy(c).wait()
        total = OP[rows(at.x * xb, xb, xb), :].astype(F32) + OX2[0].astype(F32) + OX2[1].astype(F32)
        h = (XH[...].astype(F32) + total).astype(BF16)
        HB[...] = h
        ST[c, at.y] = jnp.broadcast_to(as_row(jnp.broadcast_to(square_sum(h), (xb, 128))), (8, 128))
        start(ot_copies(c))
        hl_copy(c).start()

    def o_norm(c):
        wait(ot_copies(c))
        hl_copy(c).wait()
        inv = as_col(inv_rms(ST, c, width * 4)[0:1, :], xb)
        MO[...] = (HB[...].astype(F32) * inv * gains[1:2, :]).astype(BF16)
        start(oa_copies(c))
        om_copy(c, 0).start()
        mo_copy(c).start()

    def o_pass(c):
        wait(oa_copies(c))
        mo_copy(c).wait()
        start(of_copies(c))
        om_copy(c, 1).start()
        om_copy(c, 2).start()

    def o_last(c):
        wait(of_copies(c))
        om_copy(c, 3).start()

    def o_end(c):
        for i in range(4):
            om_copy(c, i).wait_send()
            om_wait_recv(c, i)

    m_wait()
    for i, b in enumerate((at.yo, at.yp, at.ym, at.y)):
        br = rows(b * qb, qb, qb)

        @pl.loop(0, gu_tiles)
        def _(n):
            if i == 0:
                wait(gu_copies(n))
            g_cols = rows(n * gu_w, gu_w, 128)
            PP[0, br, g_cols] = jnp.dot(M[br, :], WG[:, g_cols], preferred_element_type=F32).astype(BF16)
            PP[0, br, rows(ff + n * gu_w, gu_w, 128)] = jnp.dot(M[br, :], WU[:, g_cols], preferred_element_type=F32).astype(BF16)

        if i == 0:
            start(s1_copies(0))
    wd_copy.wait()

    @pl.loop(0, n_chunks + 2)
    def _(k):
        par = k % 2
        alt = (k + 1) % 2
        has_s = k < n_chunks
        has_gu = k + 1 < n_chunks
        has_a = jnp.logical_and(k >= 1, k - 1 < n_chunks)
        has_d = k >= 2

        @pl.when(k >= 1)
        def _():
            at.take_credit(credit)

        @pl.when(jnp.logical_and(has_s, k >= 1))
        def _():
            start(s1_copies(par))

        @pl.when(has_d)
        def _():
            h_start(k - 2)

        def o_step(body):
            @pl.when(k + EARLY < n_chunks)
            def _():
                body(k + EARLY)

        def m_step(body):
            @pl.when(jnp.logical_and(k + 1 >= EARLY, has_gu))
            def _():
                body(k + 1)

        o_step(o_begin)
        m_step(o_norm)

        @pl.when(has_a)
        def _():
            wait(s2_copies(alt))
            base = at.y * qb
            step = 16

            @pl.loop(0, qb // step)
            def _(i):
                r = rows(base + i * step, step, step)
                r2 = rows(i * step, step, step)
                g = PP[alt, r, 0:ff].astype(F32) + R2[alt, 0, r2, 0:ff].astype(F32) + R2[alt, 1, r2, 0:ff].astype(F32)
                u = PP[alt, r, ff:2 * ff].astype(F32) + R2[alt, 0, r2, ff:2 * ff].astype(F32) + R2[alt, 1, r2, ff:2 * ff].astype(F32)
                ACT[alt, r, :] = (g * jax.nn.sigmoid(g) * u).astype(BF16)

            start(act_copies(alt))

        m_step(o_pass)

        is_last = k == n_chunks + 1
        has_dd = jnp.logical_and(has_d, k < n_chunks + 1)

        @pl.when(has_dd)
        def _():
            wait(fwd_copies(par))
            down(par)
            dd_copy().start()

        o_step(o_core)
        m_step(o_last)

        @pl.when(has_s)
        def _():
            wait(s1_copies(par))
            step = 16

            @pl.loop(0, hq // step)
            def _(i):
                ri = rows(i * step, step, step)
                ra = rows(at.yp * qb + i * step, step, step)
                rb = rows(at.ym * qb + hq + i * step, step, step)
                PP[par, ra, :] = (PP[par, ra, :].astype(F32) + R1[0, ri, :].astype(F32)).astype(BF16)
                PP[par, rb, :] = (PP[par, rb, :].astype(F32) + R1[1, ri, :].astype(F32)).astype(BF16)

            start(s2_copies(par))

        o_step(o_ring)
        m_step(o_end)

        @pl.when(has_gu)
        def _():
            m_start(k + 1)

        @pl.when(has_dd)
        def _():
            dd_copy().wait()
            core_add(DR)

        @pl.when(is_last)
        def _():
            last_copy().wait()
            core_add(OR)

        @pl.when(has_gu)
        def _():
            m_wait()
            gu_part(alt, 0, 2)

        o_step(o_sum)

        @pl.when(has_d)
        def _():
            wait(x1_copies())
            ra = rows(own_half + at.xp * xb, hx, hx)
            rb = rows(own_half + at.xm * xb + hx, hx, hx)
            DP[ra, :] = (DP[ra, :].astype(F32) + XR1[0].astype(F32)).astype(BF16)
            DP[rb, :] = (DP[rb, :].astype(F32) + XR1[1].astype(F32)).astype(BF16)
            start(x2_copies())

        @pl.when(has_gu)
        def _():
            gu_part(alt, 2, 3)

        @pl.when(has_a)
        def _():
            wait(act_copies(alt))
            start(fwd_copies(alt))

        @pl.when(has_d)
        def _():
            wait(x2_copies())
            h_wait()
            r = rows(own_half + at.x * xb, xb, xb)
            down = DP[r, :].astype(F32) + XR2[0].astype(F32) + XR2[1].astype(F32)
            YB[r, :] = (H[...].astype(F32) + down).astype(BF16)
            start(xa_copies())
            dy_copy(0).start()

        @pl.when(k == n_chunks)
        def _():
            wait(fwd_copies(alt))
            down(alt)
            last_copy().start()

        @pl.when(has_gu)
        def _():
            gu_part(alt, 3, 4)

        @pl.when(has_d)
        def _():
            wait(xa_copies())
            start(xf_copies())
            dy_copy(1).start()
            dy_copy(2).start()

        @pl.when(has_gu)
        def _():
            gu_part(alt, 4, 5)

        @pl.when(has_d)
        def _():
            wait(xf_copies())
            dy_copy(3).start()
            y_copy(k - 2, at.core).start()
            for i in range(4):
                dy_copy(i).wait_send()
                dy_wait_recv(i)
            y_copy(k - 2, 1 - at.core).start()
            for i in range(2):
                y_copy(k - 2, i).wait()

        @pl.when(k < n_chunks + 1)
        def _():
            at.give_credit(credit)


def mlp_phase(x_in, gains, m_early, h_early, o_part, w_gate, w_up, w_down, chunk):
    tokens, width = x_in.shape
    ff = w_gate.shape[1]
    n_chunks = tokens // chunk
    qb, hb = chunk // 4, chunk // 2
    xb = hb // 4
    hbm = pl.BlockSpec(memory_space=pl.ANY)
    sem = pltpu.SemaphoreType.DMA
    S2, P2 = sem((2,)), sem((2, 2))
    vm = lambda *s: pltpu.VMEM(s, BF16)
    return pl.pallas_call(
        functools.partial(mlp_kernel, n_chunks),
        out_shape=tuple(jax.ShapeDtypeStruct((n, width), BF16) for n in (tokens, tokens - EARLY * chunk, tokens // 8 - EARLY * xb)),
        in_specs=[hbm, pl.BlockSpec(memory_space=pltpu.VMEM)] + [hbm] * 6,
        out_specs=(hbm, hbm, hbm),
        scratch_shapes=[
            vm(width, ff), vm(width, ff), vm(ff, width), vm(chunk, width), vm(2, chunk, 2 * ff),
            vm(2, qb // 2, 2 * ff), vm(2, 2, qb, 2 * ff), vm(2, chunk, ff), vm(chunk, width), vm(hb, width),
            vm(2, xb // 2, width), vm(2, xb, width), vm(chunk, width), vm(xb, width),
            vm(hb, width), vm(hb, width), vm(2, xb // 2, width), vm(2, xb, width), vm(xb, width), vm(xb, width), vm(xb, width),
            pltpu.VMEM((n_chunks, 4, 8, 128), F32),
            sem((11,)), sem, sem, S2, sem((4,)), sem, sem, sem((4, 2)), sem((4, 2)), sem((3,)), sem((n_chunks, 3)), sem((4,)), sem((4,)), pltpu.SemaphoreType.REGULAR((5,)),
            S2, S2, P2, P2, S2, S2, P2, P2,
            sem, sem, S2, S2, S2, S2, S2, S2, S2, S2, sem((4,)), sem((4,)),
        ],
        compiler_params=pltpu.CompilerParams(collective_id=1, has_side_effects=True, vmem_limit_bytes=67043328),
        name="mlp_phase",
    )(x_in, gains, m_early, h_early, o_part, w_gate, w_up, w_down)[0]


def attn_kernel(n_chunks, x_hbm, gains, cos_t, sin_t, wq_hbm, wk_hbm, wv_hbm, wo_hbm, m_hbm, h_hbm, wp_hbm,
                WQKV, WO, X, N, QP, R1, R2, QS, KV, O, WP, DR, XR1, XR2, XH, HB, MO, SQ, RC, ST1, ST2,
                w_sem, x_sem, xh_sem, hb_sem, mo_sem, wp_sem, credit,
                t1s, t1r, s1s, s1r, s2s, s2r, kvs, kvr, kfs, kfr, ocs, ocr, ofs, ofr, dds, ddr, x1s, x1r, x2s, x2r, t2s, t2r, xas, xar, xfs, xfr, dms, dmr):
    at = Place()
    tc, width = N.shape
    full_width = width * 4
    qkv_w = WQKV.shape[1]
    head = 128
    heads = QS.shape[1] // (tc // 4)
    q_w = heads * head
    qb = tc // 4
    hq = qb // 2
    hb = tc // 2
    xb = hb // 4
    hx = xb // 2
    own_half = at.core * hb
    my_rows = own_half + at.x * xb
    peers = at.ys + (at.dev_yo,)
    blk = min(128, tc)
    n_blk = tc // blk
    step = 16

    w_copies = [
        pltpu.make_async_copy(w, WQKV.at[:, pl.ds(i * head, head)], w_sem.at[i])
        for i, w in enumerate([wq_hbm.at[h] for h in range(heads)] + [wk_hbm, wv_hbm])
    ] + [pltpu.make_async_copy(wo_hbm, WO, w_sem.at[heads + 2])]

    def x_copy(c):
        return pltpu.make_async_copy(x_hbm.at[rows(c * tc, tc, tc)], X.at[c % 2], x_sem.at[c % 2])

    x_copy(0).start()
    for c in w_copies:
        c.start()
    at.entry(extra=(at.dev_yo,))

    def slot(c):
        return c % 4

    def pair(c):
        return c % 2

    def stats_copies(st, ssem, rsem, c):
        own = st.at[c, at.y]
        return [rcopy(own, own, ssem.at[pair(c), i], rsem.at[c, i], dev) for i, dev in enumerate(peers)]

    def s1_copies(c):
        s, o = slot(c), at.yo * qb
        return two([QP.at[s, rows(r, hq, hq)] for r in (o, o + hq)], slots(R1.at[s]), s1s.at[pair(c)], s1r.at[s], at.ys)

    def s2_copies(c):
        s = slot(c)
        return two([QP.at[s, rows(b * qb, qb, qb)] for b in (at.yp, at.ym)], slots(R2.at[s]), s2s.at[pair(c)], s2r.at[s], at.ys)

    def kv_copies(c):
        own = [KV.at[rows(c * tc + at.y * qb, qb, qb)]] * 2
        return two(own, own, kvs.at[pair(c)], kvr.at[c], at.ys)

    def kf_copies(c):
        half = [KV.at[rows(c * tc + r, hq, hq)] for r in (at.ym * qb, at.yp * qb + hq)]
        return two(half, half, kfs.at[pair(c)], kfr.at[c], at.ys)

    def o_copies(c):
        own = [O.at[slot(c), rows(at.y * qb, qb, qb)]] * 2
        return two(own, own, ocs.at[pair(c)], ocr.at[slot(c)], at.ys)

    def of_copies(c):
        half = [O.at[slot(c), rows(r, hq, hq)] for r in (at.ym * qb, at.yp * qb + hq)]
        return two(half, half, ofs.at[pair(c)], ofr.at[slot(c)], at.ys)

    def dd_copies(c):
        s = slot(c)
        return [rcopy(WP.at[s, rows((1 - at.core) * hb, hb, hb)], DR.at[s], dds.at[pair(c)], ddr.at[s], at.dev_core)]

    def x1_copies(c):
        s, o = slot(c), own_half + at.xo * xb
        return two([WP.at[s, rows(r, hx, hx)] for r in (o, o + hx)], slots(XR1.at[s]), x1s.at[pair(c)], x1r.at[s], at.xs)

    def x2_copies(c):
        s = slot(c)
        return two([WP.at[s, rows(own_half + b * xb, xb, xb)] for b in (at.xp, at.xm)], slots(XR2.at[s]), x2s.at[pair(c)], x2r.at[s], at.xs)

    def m_rows(c, start, size):
        return m_hbm.at[rows(c * tc + start, size, size)]

    def xa_copies(c):
        return two([MO.at[slot(c)]] * 2, [m_rows(c, my_rows, xb)] * 2, xas.at[pair(c)], xar.at[c], at.xs)

    def xf_copies(c):
        half = [m_rows(c, own_half + r, hx) for r in (at.xm * xb, at.xp * xb + hx)]
        return two(half, half, xfs.at[pair(c)], xfr.at[c], at.xs)

    def dm_copy(c, i):
        if i == 0:
            return rcopy(MO.at[slot(c)], m_rows(c, my_rows, xb), dms.at[pair(c), 0], dmr.at[c, 0], at.dev_core)
        b = m_rows(c, own_half + (at.xm, at.xp, at.xo)[i - 1] * xb, xb)
        return rcopy(b, b, dms.at[pair(c), i], dmr.at[c, i], at.dev_core)

    def dm_wait_recv(c, i):
        b = m_rows(c, (1 - at.core) * hb + (at.x, at.xm, at.xp, at.xo)[i] * xb, xb)
        rcopy(b, b, dms.at[pair(c), i], dmr.at[c, i], at.dev_core).wait_recv()

    def xh_copy(c):
        return pltpu.make_async_copy(x_hbm.at[rows(c * tc + my_rows, xb, xb)], XH.at[pair(c)], xh_sem.at[pair(c)])

    def hb_copy(c):
        return pltpu.make_async_copy(HB.at[slot(c)], h_hbm.at[rows(c * xb, xb, xb)], hb_sem.at[pair(c)])

    def mo_copy(c):
        return pltpu.make_async_copy(MO.at[slot(c)], m_rows(c, my_rows, xb), mo_sem.at[pair(c)])

    def wp_copy(c):
        return pltpu.make_async_copy(WP.at[slot(c)], wp_hbm.at[rows((c - EARLY) * tc, tc, tc)], wp_sem.at[pair(c)])

    def stage(k, s, body):
        c = k - s

        @pl.when(jnp.logical_and(c >= 0, c < (EARLY if body in early_chunks else n_chunks)))
        def _():
            body(c)

    def st_sumsq(c):
        x_copy(c).wait()

        @pl.loop(0, tc // step)
        def _(i):
            r = rows(i * step, step, step)
            SQ[r, :] = jnp.broadcast_to(square_sum(X[c % 2, r, :]), (step, 128))

        parts = [as_row(SQ[b * blk:(b + 1) * blk, :]) for b in range(n_blk)]
        parts = parts + [jnp.zeros_like(parts[0])] * (8 - n_blk)
        ST1[c, at.y] = jnp.concatenate(parts, axis=0)
        start(stats_copies(ST1, t1s, t1r, c))

    def st_qkv(c):
        wait(stats_copies(ST1, t1s, t1r, c))

        @pl.when(c == 0)
        def _():
            wait(w_copies[:-1])

        inv = inv_rms(ST1, c, full_width)
        for b in range(n_blk):
            RC[b * blk:(b + 1) * blk, :] = jnp.broadcast_to(as_col(inv[b:b + 1, :], blk), (blk, 128))

        @pl.loop(0, tc // step)
        def _(i):
            r = rows(i * step, step, step)
            N[r, :] = (X[c % 2, r, :].astype(F32) * RC[r, 0:1] * gains[0:1, :]).astype(BF16)

        n_t = qkv_w // 384

        @pl.loop(0, n_t)
        def _(n):
            cols = rows(n * 384, 384, 128)
            QP[slot(c), :, cols] = jnp.dot(N[...], WQKV[:, cols], preferred_element_type=F32).astype(BF16)

        start(s1_copies(c))

    def st_add1(c):
        wait(s1_copies(c))
        s = slot(c)

        @pl.loop(0, hq // step)
        def _(i):
            ri = rows(i * step, step, step)
            ra = rows(at.yp * qb + i * step, step, step)
            rb = rows(at.ym * qb + hq + i * step, step, step)
            QP[s, ra, :] = (QP[s, ra, :].astype(F32) + R1[s, 0, ri, :].astype(F32)).astype(BF16)
            QP[s, rb, :] = (QP[s, rb, :].astype(F32) + R1[s, 1, ri, :].astype(F32)).astype(BF16)

        start(s2_copies(c))

    def st_rope(c):
        wait(s2_copies(c))
        s = slot(c)
        own = rows(at.y * qb, qb, qb)
        cos_v = cos_t[rows(c * qb, qb, qb), :]
        sin_v = sin_t[rows(c * qb, qb, qb), :]

        def piece(i):
            cols = slice(i * head, (i + 1) * head)
            v = QP[s, own, cols].astype(F32) + R2[s, 0, :, cols].astype(F32) + R2[s, 1, :, cols].astype(F32)
            return v.astype(BF16)

        def turned(i):
            v = piece(i).astype(F32)
            return (v * cos_v + pltpu.roll(v, head // 2, 1) * sin_v).astype(BF16)

        kv_rows = rows(c * tc + at.y * qb, qb, qb)
        KV[kv_rows, 0:head] = turned(heads)
        KV[kv_rows, head:2 * head] = piece(heads + 1)
        start(kv_copies(c))
        for i in range(heads):
            QS[slot(c), i * qb:(i + 1) * qb, :] = turned(i)

    def st_kvfwd(c):
        wait(kv_copies(c))
        start(kf_copies(c))

    def st_attend(c):
        wait(kf_copies(c))
        q = QS[slot(c)]
        scale = head ** -0.5 * 1.4426950408889634

        def scores(j):
            keys = KV[rows(j * tc, tc, tc), 0:head]
            return lax.dot_general(q, keys, (((1,), (1,)), ((), ())), preferred_element_type=F32) * scale

        def values(j, p):
            return jnp.dot(p.astype(BF16), KV[rows(j * tc, tc, tc), head:2 * head], preferred_element_type=F32)

        qpos = at.y * qb + lax.broadcasted_iota(jnp.int32, (qb, tc), 0)
        keep = lax.broadcasted_iota(jnp.int32, (qb, tc), 1) <= qpos
        sc = scores(c).reshape(heads, qb, tc)
        sc = jnp.where(keep[None], sc, -jnp.inf).reshape(heads * qb, tc)
        top = jnp.max(sc, axis=-1, keepdims=True)
        p = jnp.exp2(sc - top)

        def more(j, carry):
            top, total, acc = carry
            sc = scores(j)
            new = jnp.maximum(top, jnp.max(sc, axis=-1, keepdims=True))
            fade = jnp.exp2(top - new)
            p = jnp.exp2(sc - new)
            return new, total * fade + jnp.sum(p, axis=-1, keepdims=True), acc * fade + values(j, p)

        top, total, acc = lax.fori_loop(0, c, more, (top, jnp.sum(p, axis=-1, keepdims=True), values(c, p)))
        out = (acc / total).astype(BF16)
        for i in range(heads):
            O[slot(c), rows(at.y * qb, qb, qb), i * head:(i + 1) * head] = out[i * qb:(i + 1) * qb, :]
        start(o_copies(c))

    def st_ofwd(c):
        wait(o_copies(c))
        start(of_copies(c))

    def st_oproj(c):
        wait(of_copies(c))

        @pl.when(c == 0)
        def _():
            w_copies[-1].wait()

        dn_w = 256 if width % 256 == 0 else 128

        @pl.loop(0, width // dn_w)
        def _(n):
            cols = rows(n * dn_w, dn_w, 128)
            WP[slot(c), :, cols] = jnp.dot(O[slot(c)], WO[:, cols], preferred_element_type=F32).astype(BF16)

        @pl.when(c < EARLY)
        def _():
            start(dd_copies(c))

        @pl.when(c >= EARLY)
        def _():
            wp_copy(c).start()

    def st_x1(c):
        @pl.when(c < EARLY)
        def _():
            st_x1_early(c)

        @pl.when(c >= EARLY)
        def _():
            wp_copy(c).wait()

    def st_x1_early(c):
        wait(dd_copies(c))
        s = slot(c)

        @pl.loop(0, hb // step)
        def _(i):
            ri = rows(i * step, step, step)
            ra = rows(own_half + i * step, step, step)
            WP[s, ra, :] = (WP[s, ra, :].astype(F32) + DR[s, ri, :].astype(F32)).astype(BF16)

        start(x1_copies(c))

    def st_x2(c):
        xh_copy(c).start()
        wait(x1_copies(c))
        s = slot(c)
        ra = rows(own_half + at.xp * xb, hx, hx)
        rb = rows(own_half + at.xm * xb + hx, hx, hx)
        WP[s, ra, :] = (WP[s, ra, :].astype(F32) + XR1[s, 0].astype(F32)).astype(BF16)
        WP[s, rb, :] = (WP[s, rb, :].astype(F32) + XR1[s, 1].astype(F32)).astype(BF16)
        start(x2_copies(c))

    def st_h(c):
        wait(x2_copies(c))
        xh_copy(c).wait()
        s = slot(c)
        total = WP[s, rows(my_rows, xb, xb), :].astype(F32) + XR2[s, 0].astype(F32) + XR2[s, 1].astype(F32)
        h = (XH[pair(c)].astype(F32) + total).astype(BF16)
        HB[s] = h
        row = as_row(jnp.broadcast_to(square_sum(h), (xb, 128)))
        ST2[c, at.y] = jnp.broadcast_to(row, (8, 128))
        start(stats_copies(ST2, t2s, t2r, c))
        hb_copy(c).start()

    def st_m(c):
        wait(stats_copies(ST2, t2s, t2r, c))
        hb_copy(c).wait()
        s = slot(c)
        inv = as_col(inv_rms(ST2, c, full_width)[0:1, :], xb)
        MO[s] = (HB[s].astype(F32) * inv * gains[1:2, :]).astype(BF16)
        start(xa_copies(c))
        dm_copy(c, 0).start()
        mo_copy(c).start()

    def st_xf(c):
        wait(xa_copies(c))
        dm_copy(c, 0).wait_send()
        mo_copy(c).wait()
        start(xf_copies(c))
        dm_copy(c, 1).start()
        dm_copy(c, 2).start()

    def st_dm(c):
        wait(xf_copies(c))
        dm_copy(c, 1).wait_send()
        dm_copy(c, 2).wait_send()
        dm_copy(c, 3).start()

    def st_end(c):
        dm_copy(c, 3).wait_send()
        for i in range(4):
            dm_wait_recv(c, i)

    all_chunks = (st_sumsq, st_qkv, st_add1, st_rope, st_kvfwd, st_attend, st_ofwd, st_oproj, st_x1)
    early_chunks = (st_x2, st_h, st_m, st_xf, st_dm, st_end)
    steps = all_chunks + early_chunks
    n_iter = max(n_chunks + len(all_chunks), EARLY + len(steps)) - 1

    @pl.loop(0, n_iter)
    def _(k):
        @pl.when(k >= 2)
        def _():
            at.take_credit(credit)

        for s, body in enumerate(steps):
            stage(k, s, body)
            if body is st_qkv:
                @pl.when(k + 1 < n_chunks)
                def _():
                    x_copy(k + 1).start()

        @pl.when(k < n_iter - 2)
        def _():
            at.give_credit(credit)


def attn_phase(x_in, gains, cos_t, sin_t, w_q, w_k, w_v, w_o, chunk):
    tokens, width = x_in.shape
    heads = w_q.shape[0]
    q_w = heads * 128
    n_chunks = tokens // chunk
    qb, hb = chunk // 4, chunk // 2
    xb = hb // 4
    hbm = pl.BlockSpec(memory_space=pl.ANY)
    vmem = pl.BlockSpec(memory_space=pltpu.VMEM)
    sem = pltpu.SemaphoreType.DMA
    S2, P2 = sem((2,)), sem((2, 2))
    vm = lambda *s: pltpu.VMEM(s, BF16)
    vf = lambda *s: pltpu.VMEM(s, F32)
    qkv_w = q_w + 256
    return pl.pallas_call(
        functools.partial(attn_kernel, n_chunks),
        out_shape=tuple(jax.ShapeDtypeStruct((n, width), BF16) for n in (EARLY * chunk, EARLY * xb, tokens - EARLY * chunk)),
        in_specs=[hbm, vmem, vmem, vmem, hbm, hbm, hbm, hbm],
        out_specs=(hbm, hbm, hbm),
        scratch_shapes=[
            vm(width, qkv_w), vm(q_w, width), vm(2, chunk, width), vm(chunk, width), vm(4, chunk, qkv_w),
            vm(4, 2, qb // 2, qkv_w), vm(4, 2, qb, qkv_w), vm(4, heads * qb, 128), vm(tokens, 256), vm(4, chunk, q_w),
            vm(4, chunk, width), vm(4, hb, width), vm(4, 2, xb // 2, width), vm(4, 2, xb, width), vm(2, xb, width), vm(4, xb, width), vm(4, xb, width),
            vf(chunk, 128), vf(chunk, 128), vf(n_chunks, 4, 8, 128), vf(n_chunks, 4, 8, 128),
            sem((heads + 3,)), S2, S2, S2, S2, S2, pltpu.SemaphoreType.REGULAR((5,)),
            sem((2, 3)), sem((n_chunks, 3)), P2, sem((4, 2)), P2, sem((4, 2)), P2, sem((n_chunks, 2)), P2, sem((n_chunks, 2)),
            P2, sem((4, 2)), P2, sem((4, 2)), S2, sem((4,)), P2, sem((4, 2)), P2, sem((4, 2)),
            sem((2, 3)), sem((n_chunks, 3)), P2, sem((n_chunks, 2)), P2, sem((n_chunks, 2)), sem((2, 4)), sem((n_chunks, 4)),
        ],
        compiler_params=pltpu.CompilerParams(collective_id=2, has_side_effects=True, vmem_limit_bytes=67043328),
        name="attn_phase",
    )(x_in, gains, cos_t, sin_t, w_q, w_k, w_v, w_o)


def copy_kernel(src, dst, buf, in_sem, out_sem):
    n, part = buf.shape[:2]
    ins = [pltpu.make_async_copy(src.at[pl.ds(i * part, part)], buf.at[i], in_sem.at[i]) for i in range(n)]
    outs = [pltpu.make_async_copy(buf.at[i], dst.at[pl.ds(i * part, part)], out_sem.at[i]) for i in range(n)]
    start(ins)
    for i in range(n):
        ins[i].wait()
        outs[i].start()
    for c in outs:
        c.wait()


def copy_out(y):
    tokens, width = y.shape
    n = 16
    hbm = pl.BlockSpec(memory_space=pl.ANY)
    return pl.pallas_call(
        copy_kernel,
        out_shape=jax.ShapeDtypeStruct(y.shape, y.dtype),
        in_specs=[hbm],
        out_specs=hbm,
        scratch_shapes=[pltpu.VMEM((n, tokens // n, width), y.dtype), pltpu.SemaphoreType.DMA((n,)), pltpu.SemaphoreType.DMA((n,))],
        compiler_params=pltpu.CompilerParams(vmem_limit_bytes=67043328),
        name="copy_out",
    )(y)


def solution(mesh, chunk=CHUNK):
    my_size = mesh.shape["my"]

    def local_layer(x_in, gain_attn, w_q, w_k, w_v, w_o, gain_mlp, w_gate, w_up, w_down):
        tokens, width = x_in.shape
        head = w_q.shape[-1]
        qb = chunk // my_size
        row = jnp.arange(tokens // my_size)
        positions = (row // qb) * chunk + lax.axis_index("my") * qb + row % qb
        half = head // 2
        inv_freq = ROPE_BASE ** (-jnp.arange(half, dtype=F32) / half)
        angles = positions.astype(F32)[:, None] * inv_freq[None, :]
        cos_h, sin_h = jnp.cos(angles), jnp.sin(angles)
        cos_t = jnp.concatenate([cos_h, cos_h], axis=-1)
        sin_t = jnp.concatenate([-sin_h, sin_h], axis=-1)
        gains = jnp.stack([gain_attn, gain_mlp]).astype(F32)
        m_early, h_early, o_part = attn_phase(
            x_in, gains, cos_t, sin_t, w_q.transpose(1, 0, 2), w_k.reshape(width, -1), w_v.reshape(width, -1), w_o.reshape(-1, width), chunk)
        return copy_out(mlp_phase(x_in, gains, m_early, h_early, o_part, w_gate, w_up, w_down, chunk))

    in_specs = (P("dp", "my"), P("my"), P("my", "mx", None), P("my", "mx", None), P("my", "mx", None), P("mx", None, "my"), P("my"), P("my", "mx"), P("my", "mx"), P("mx", "my"))
    return jax.shard_map(local_layer, mesh=mesh, in_specs=in_specs, out_specs=P("dp", "my"), check_vma=False)
```

```python
import functools

import jax
import jax.numpy as jnp
from jax import lax
from jax.experimental import pallas as pl
from jax.experimental.pallas import tpu as pltpu
from jax.sharding import PartitionSpec as P

ROPE_BASE = 10000.0
NORM_EPS = 1e-6
CHUNK = 512
EARLY = 2
MESH = pl.DeviceIdType.MESH
F32 = jnp.float32
BF16 = jnp.bfloat16


class Place:
    def __init__(self):
        self.y = lax.axis_index("my")
        mx = lax.axis_index("mx")
        self.x = mx // 2
        self.core = mx % 2
        self.yp = (self.y + 1) % 4
        self.ym = (self.y + 3) % 4
        self.yo = (self.y + 2) % 4
        self.xp = (self.x + 1) % 4
        self.xm = (self.x + 3) % 4
        self.xo = (self.x + 2) % 4
        self.dev_yp = {"my": self.yp}
        self.dev_ym = {"my": self.ym}
        self.dev_xp = {"mx": self.xp * 2 + self.core}
        self.dev_xm = {"mx": self.xm * 2 + self.core}
        self.dev_core = {"mx": self.x * 2 + (1 - self.core)}
        self.dev_yo = {"my": self.yo}
        self.ys = (self.dev_yp, self.dev_ym)
        self.xs = (self.dev_xp, self.dev_xm)
        self.partners = (self.dev_yp, self.dev_ym, self.dev_xp, self.dev_xm, self.dev_core)

    def entry(self, extra=()):
        barrier = pltpu.get_barrier_semaphore()
        for dev in self.partners + extra:
            pl.semaphore_signal(barrier, inc=1, device_id=dev, device_id_type=MESH)
        pl.semaphore_wait(barrier, len(self.partners) + len(extra))

    def give_credit(self, credit):
        for slot, dev in ((1, self.dev_yp), (0, self.dev_ym), (3, self.dev_xp), (2, self.dev_xm), (4, self.dev_core)):
            pl.semaphore_signal(credit.at[slot], inc=1, device_id=dev, device_id_type=MESH)

    def take_credit(self, credit):
        for slot in range(5):
            pl.semaphore_wait(credit.at[slot], 1)


def rcopy(src, dst, send_sem, recv_sem, dev):
    return pltpu.make_async_remote_copy(src_ref=src, dst_ref=dst, send_sem=send_sem, recv_sem=recv_sem, device_id=dev, device_id_type=MESH)


def as_row(col_b):
    eye = lax.broadcasted_iota(jnp.int32, col_b.shape, 0) == lax.broadcasted_iota(jnp.int32, col_b.shape, 1)
    return jnp.sum(jnp.where(eye, col_b, 0.0), axis=0, keepdims=True)


def as_col(row, r):
    shape = (r, row.shape[1])
    eye = lax.broadcasted_iota(jnp.int32, shape, 0) == lax.broadcasted_iota(jnp.int32, shape, 1)
    return jnp.sum(jnp.where(eye, jnp.broadcast_to(row, shape), 0.0), axis=1, keepdims=True)


def square_sum(v):
    vf = v.astype(F32)
    return jnp.sum(vf * vf, axis=-1, keepdims=True)


def inv_rms(st, c, full_width):
    tot = (st[c, 0] + st[c, 1]) + (st[c, 2] + st[c, 3])
    return lax.rsqrt(tot / full_width + NORM_EPS)


def two(srcs, dsts, send, recv, devs):
    return [rcopy(src, dst, send.at[i], recv.at[i], dev) for i, (src, dst, dev) in enumerate(zip(srcs, dsts, devs))]


def slots(ref):
    return [ref.at[i] for i in range(2)]


def start(copies):
    for c in copies:
        c.start()


def wait(copies):
    for c in copies:
        c.wait()


def rows(start, size, align):
    return pl.ds(pl.multiple_of(start, align), size)


def mlp_kernel(n_chunks, x_hbm, gains, me_hbm, he_hbm, wp_hbm, wg_hbm, wu_hbm, wd_hbm, y_hbm, ml_hbm, hl_hbm,
               WG, WU, WD, M, PP, R1, R2, ACT, DP, DR, XR1, XR2, YB, H, OP, OR, OX1, OX2, XH, HB, MO, ST,
               w_sem, m_sem, h_sem, y_sem, o_sem, ods, odr, oxs, oxr, ots, otr, oms, omr, credit, s1s, s1r, s2s, s2r, acs, acr, fws, fwr, dds, ddr, x1s, x1r, x2s, x2r, xas, xar, xfs, xfr, dys, dyr):
    at = Place()
    tc, width = M.shape
    ff = WG.shape[1]
    qb = tc // 4
    hq = qb // 2
    hb = tc // 2
    xb = hb // 4
    hx = xb // 2
    gu_tiles = 5
    gu_w = ff // gu_tiles
    dn_w = 256 if width % 256 == 0 else 128

    def m_wait():
        pltpu.make_async_copy(me_hbm.at[pl.ds(0, tc)], M, m_sem).wait()

    def m_start(c):
        @pl.when(c < EARLY)
        def _():
            pltpu.make_async_copy(me_hbm.at[rows(c * tc, tc, tc)], M, m_sem).start()

        @pl.when(c >= EARLY)
        def _():
            pltpu.make_async_copy(ml_hbm.at[rows((c - EARLY) * tc, tc, tc)], M, m_sem).start()

    def gu_copies(n):
        cols = rows(n * gu_w, gu_w, 128)
        return [pltpu.make_async_copy(wg_hbm.at[:, cols], WG.at[:, cols], w_sem.at[n]),
                pltpu.make_async_copy(wu_hbm.at[:, cols], WU.at[:, cols], w_sem.at[gu_tiles + n])]

    wd_copy = pltpu.make_async_copy(wd_hbm, WD, w_sem.at[2 * gu_tiles])
    pltpu.make_async_copy(me_hbm.at[pl.ds(0, tc)], M, m_sem).start()
    ahead = 2
    for n in range(ahead):
        start(gu_copies(n))
    at.entry(extra=(at.dev_yo,))

    def gu_part(par, lo, hi):
        @pl.loop(lo, hi)
        def _(n):
            g_cols = rows(n * gu_w, gu_w, 128)
            PP[par, :, g_cols] = jnp.dot(M[...], WG[:, g_cols], preferred_element_type=F32).astype(BF16)
            PP[par, :, rows(ff + n * gu_w, gu_w, 128)] = jnp.dot(M[...], WU[:, g_cols], preferred_element_type=F32).astype(BF16)

    def s1_copies(par):
        o = at.yo * qb
        return two([PP.at[par, rows(r, hq, hq)] for r in (o, o + hq)], slots(R1), s1s, s1r, at.ys)

    def s2_copies(par):
        return two([PP.at[par, rows(b * qb, qb, qb)] for b in (at.yp, at.ym)], slots(R2.at[par]), s2s.at[par], s2r.at[par], at.ys)

    def act_copies(par):
        own = [ACT.at[par, rows(at.y * qb, qb, qb)]] * 2
        return two(own, own, acs, acr, at.ys)

    def fwd_copies(par):
        half = [ACT.at[par, rows(r, hq, hq)] for r in (at.ym * qb, at.yp * qb + hq)]
        return two(half, half, fws.at[par], fwr.at[par], at.ys)

    def dd_copy():
        return rcopy(DP.at[rows((1 - at.core) * hb, hb, hb)], DR, dds, ddr, at.dev_core)

    def last_copy():
        return rcopy(DP.at[rows((1 - at.core) * hb, hb, hb)], OR, ods, odr, at.dev_core)

    def down(par):
        @pl.loop(0, width // dn_w)
        def _(n):
            cols = rows(n * dn_w, dn_w, 128)
            DP[:, cols] = jnp.dot(ACT[par], WD[:, cols], preferred_element_type=F32).astype(BF16)

    own_half = at.core * hb

    def core_add(part):
        @pl.loop(0, hb // 16)
        def _(i):
            ri = rows(i * 16, 16, 16)
            ra = rows(own_half + i * 16, 16, 16)
            DP[ra, :] = (DP[ra, :].astype(F32) + part[ri, :].astype(F32)).astype(BF16)

        start(x1_copies())

    def x1_copies():
        o = own_half + at.xo * xb
        return two([DP.at[rows(r, hx, hx)] for r in (o, o + hx)], slots(XR1), x1s, x1r, at.xs)

    def x2_copies():
        return two([DP.at[rows(own_half + b * xb, xb, xb)] for b in (at.xp, at.xm)], slots(XR2), x2s, x2r, at.xs)

    def yblk(b):
        return YB.at[rows(own_half + b * xb, xb, xb)]

    def xa_copies():
        own = [yblk(at.x)] * 2
        return two(own, own, xas, xar, at.xs)

    def xf_copies():
        half = [YB.at[rows(own_half + r, hx, hx)] for r in (at.xm * xb, at.xp * xb + hx)]
        return two(half, half, xfs, xfr, at.xs)

    def dy_copy(i):
        b = (at.x, at.xm, at.xp, at.xo)[i]
        return rcopy(yblk(b), yblk(b), dys.at[i], dyr.at[i], at.dev_core)

    def dy_wait_recv(i):
        b = (at.x, at.xm, at.xp, at.xo)[i]
        other = YB.at[rows((1 - at.core) * hb + b * xb, xb, xb)]
        rcopy(other, other, dys.at[i], dyr.at[i], at.dev_core).wait_recv()

    def h_wait():
        pltpu.make_async_copy(he_hbm.at[pl.ds(0, xb)], H, h_sem).wait()

    def h_start(c):
        @pl.when(c < EARLY)
        def _():
            pltpu.make_async_copy(he_hbm.at[rows(c * xb, xb, xb)], H, h_sem).start()

        @pl.when(c >= EARLY)
        def _():
            pltpu.make_async_copy(hl_hbm.at[rows((c - EARLY) * xb, xb, xb)], H, h_sem).start()

    def y_copy(c, core):
        return pltpu.make_async_copy(YB.at[rows(core * hb, hb, hb)], y_hbm.at[rows(c * tc + core * hb, hb, hb)], y_sem.at[core])

    my_rows = own_half + at.x * xb
    peers = at.ys + (at.dev_yo,)

    def od_copy(c):
        return rcopy(wp_hbm.at[rows((c - EARLY) * tc + (1 - at.core) * hb, hb, hb)], OR, ods, odr, at.dev_core)

    def op_copy(c):
        return pltpu.make_async_copy(wp_hbm.at[rows((c - EARLY) * tc + own_half, hb, hb)], OP, o_sem.at[0])

    def xh_copy(c):
        return pltpu.make_async_copy(x_hbm.at[rows(c * tc + my_rows, xb, xb)], XH, o_sem.at[1])

    def hl_copy(c):
        return pltpu.make_async_copy(HB, hl_hbm.at[rows((c - EARLY) * xb, xb, xb)], o_sem.at[2])

    def ml_rows(c, first, size):
        return ml_hbm.at[rows((c - EARLY) * tc + first, size, size)]

    def mo_copy(c):
        return pltpu.make_async_copy(MO, ml_rows(c, my_rows, xb), o_sem.at[3])

    def o1_copies():
        return two([OP.at[rows(at.xo * xb + r, hx, hx)] for r in (0, hx)], slots(OX1), oxs.at[0], oxr.at[0], at.xs)

    def o2_copies():
        return two([OP.at[rows(b * xb, xb, xb)] for b in (at.xp, at.xm)], slots(OX2), oxs.at[1], oxr.at[1], at.xs)

    def ot_copies(c):
        own = ST.at[c, at.y]
        return [rcopy(own, own, ots.at[i], otr.at[c, i], dev) for i, dev in enumerate(peers)]

    def oa_copies(c):
        return two([MO] * 2, [ml_rows(c, my_rows, xb)] * 2, oxs.at[2], oxr.at[2], at.xs)

    def of_copies(c):
        half = [ml_rows(c, own_half + r, hx) for r in (at.xm * xb, at.xp * xb + hx)]
        return two(half, half, oxs.at[3], oxr.at[3], at.xs)

    def om_copy(c, i):
        b = ml_rows(c, own_half + (at.x, at.xm, at.xp, at.xo)[i] * xb, xb)
        return rcopy(MO if i == 0 else b, b, oms.at[i], omr.at[i], at.dev_core)

    def om_wait_recv(c, i):
        b = ml_rows(c, (1 - at.core) * hb + (at.x, at.xm, at.xp, at.xo)[i] * xb, xb)
        rcopy(b, b, oms.at[i], omr.at[i], at.dev_core).wait_recv()

    def o_begin(c):
        od_copy(c).start()
        op_copy(c).start()
        xh_copy(c).start()

    def o_core(c):
        od_copy(c).wait()
        op_copy(c).wait()

        @pl.loop(0, hb // 16)
        def _(i):
            r = rows(i * 16, 16, 16)
            OP[r, :] = (OP[r, :].astype(F32) + OR[r, :].astype(F32)).astype(BF16)

        start(o1_copies())

    def o_ring(c):
        wait(o1_copies())
        ra = rows(at.xp * xb, hx, hx)
        rb = rows(at.xm * xb + hx, hx, hx)
        OP[ra, :] = (OP[ra, :].astype(F32) + OX1[0].astype(F32)).astype(BF16)
        OP[rb, :] = (OP[rb, :].astype(F32) + OX1[1].astype(F32)).astype(BF16)
        start(o2_copies())

    def o_sum(c):
        wait(o2_copies())
        xh_copy(c).wait()
        total = OP[rows(at.x * xb, xb, xb), :].astype(F32) + OX2[0].astype(F32) + OX2[1].astype(F32)
        h = (XH[...].astype(F32) + total).astype(BF16)
        HB[...] = h
        ST[c, at.y] = jnp.broadcast_to(as_row(jnp.broadcast_to(square_sum(h), (xb, 128))), (8, 128))
        start(ot_copies(c))
        hl_copy(c).start()

    def o_norm(c):
        wait(ot_copies(c))
        hl_copy(c).wait()
        inv = as_col(inv_rms(ST, c, width * 4)[0:1, :], xb)
        MO[...] = (HB[...].astype(F32) * inv * gains[1:2, :]).astype(BF16)
        start(oa_copies(c))
        om_copy(c, 0).start()
        mo_copy(c).start()

    def o_pass(c):
        wait(oa_copies(c))
        mo_copy(c).wait()
        start(of_copies(c))
        om_copy(c, 1).start()
        om_copy(c, 2).start()

    def o_last(c):
        wait(of_copies(c))
        om_copy(c, 3).start()

    def o_end(c):
        for i in range(4):
            om_copy(c, i).wait_send()
            om_wait_recv(c, i)

    m_wait()
    for i, b in enumerate((at.yo, at.yp, at.ym, at.y)):
        br = rows(b * qb, qb, qb)

        @pl.loop(0, gu_tiles)
        def _(n):
            if i == 0:
                @pl.when(n + ahead < gu_tiles)
                def _():
                    start(gu_copies(n + ahead))

                wait(gu_copies(n))
            g_cols = rows(n * gu_w, gu_w, 128)
            PP[0, br, g_cols] = jnp.dot(M[br, :], WG[:, g_cols], preferred_element_type=F32).astype(BF16)
            PP[0, br, rows(ff + n * gu_w, gu_w, 128)] = jnp.dot(M[br, :], WU[:, g_cols], preferred_element_type=F32).astype(BF16)

        if i == 0:
            start(s1_copies(0))
            wd_copy.start()
    wd_copy.wait()

    @pl.loop(0, n_chunks + 2)
    def _(k):
        par = k % 2
        alt = (k + 1) % 2
        has_s = k < n_chunks
        has_gu = k + 1 < n_chunks
        has_a = jnp.logical_and(k >= 1, k - 1 < n_chunks)
        has_d = k >= 2

        @pl.when(k >= 1)
        def _():
            at.take_credit(credit)

        @pl.when(jnp.logical_and(has_s, k >= 1))
        def _():
            start(s1_copies(par))

        @pl.when(has_d)
        def _():
            h_start(k - 2)

        def o_step(body):
            @pl.when(k + EARLY < n_chunks)
            def _():
                body(k + EARLY)

        def m_step(body):
            @pl.when(jnp.logical_and(k + 1 >= EARLY, has_gu))
            def _():
                body(k + 1)

        o_step(o_begin)
        m_step(o_norm)

        @pl.when(has_a)
        def _():
            wait(s2_copies(alt))
            base = at.y * qb
            step = 16

            @pl.loop(0, qb // step)
            def _(i):
                r = rows(base + i * step, step, step)
                r2 = rows(i * step, step, step)
                g = PP[alt, r, 0:ff].astype(F32) + R2[alt, 0, r2, 0:ff].astype(F32) + R2[alt, 1, r2, 0:ff].astype(F32)
                u = PP[alt, r, ff:2 * ff].astype(F32) + R2[alt, 0, r2, ff:2 * ff].astype(F32) + R2[alt, 1, r2, ff:2 * ff].astype(F32)
                ACT[alt, r, :] = (g * jax.nn.sigmoid(g) * u).astype(BF16)

            start(act_copies(alt))

        m_step(o_pass)

        is_last = k == n_chunks + 1
        has_dd = jnp.logical_and(has_d, k < n_chunks + 1)

        @pl.when(has_dd)
        def _():
            wait(fwd_copies(par))
            down(par)
            dd_copy().start()

        o_step(o_core)
        m_step(o_last)

        @pl.when(has_s)
        def _():
            wait(s1_copies(par))
            step = 16

            @pl.loop(0, hq // step)
            def _(i):
                ri = rows(i * step, step, step)
                ra = rows(at.yp * qb + i * step, step, step)
                rb = rows(at.ym * qb + hq + i * step, step, step)
                PP[par, ra, :] = (PP[par, ra, :].astype(F32) + R1[0, ri, :].astype(F32)).astype(BF16)
                PP[par, rb, :] = (PP[par, rb, :].astype(F32) + R1[1, ri, :].astype(F32)).astype(BF16)

            start(s2_copies(par))

        o_step(o_ring)
        m_step(o_end)

        @pl.when(has_gu)
        def _():
            m_start(k + 1)

        @pl.when(has_dd)
        def _():
            dd_copy().wait()
            core_add(DR)

        @pl.when(is_last)
        def _():
            last_copy().wait()
            core_add(OR)

        @pl.when(has_gu)
        def _():
            m_wait()
            gu_part(alt, 0, 2)

        o_step(o_sum)

        @pl.when(has_d)
        def _():
            wait(x1_copies())
            ra = rows(own_half + at.xp * xb, hx, hx)
            rb = rows(own_half + at.xm * xb + hx, hx, hx)
            DP[ra, :] = (DP[ra, :].astype(F32) + XR1[0].astype(F32)).astype(BF16)
            DP[rb, :] = (DP[rb, :].astype(F32) + XR1[1].astype(F32)).astype(BF16)
            start(x2_copies())

        @pl.when(has_gu)
        def _():
            gu_part(alt, 2, 3)

        @pl.when(has_a)
        def _():
            wait(act_copies(alt))
            start(fwd_copies(alt))

        @pl.when(has_d)
        def _():
            wait(x2_copies())
            h_wait()
            r = rows(own_half + at.x * xb, xb, xb)
            down = DP[r, :].astype(F32) + XR2[0].astype(F32) + XR2[1].astype(F32)
            YB[r, :] = (H[...].astype(F32) + down).astype(BF16)
            start(xa_copies())
            dy_copy(0).start()

        @pl.when(k == n_chunks)
        def _():
            wait(fwd_copies(alt))
            down(alt)
            last_copy().start()

        @pl.when(has_gu)
        def _():
            gu_part(alt, 3, 4)

        @pl.when(has_d)
        def _():
            wait(xa_copies())
            start(xf_copies())
            dy_copy(1).start()
            dy_copy(2).start()

        @pl.when(has_gu)
        def _():
            gu_part(alt, 4, 5)

        @pl.when(has_d)
        def _():
            wait(xf_copies())
            dy_copy(3).start()
            y_copy(k - 2, at.core).start()
            for i in range(4):
                dy_copy(i).wait_send()
                dy_wait_recv(i)
            y_copy(k - 2, 1 - at.core).start()
            for i in range(2):
                y_copy(k - 2, i).wait()

        @pl.when(k < n_chunks + 1)
        def _():
            at.give_credit(credit)


def mlp_phase(x_in, gains, m_early, h_early, o_part, w_gate, w_up, w_down, chunk):
    tokens, width = x_in.shape
    ff = w_gate.shape[1]
    n_chunks = tokens // chunk
    qb, hb = chunk // 4, chunk // 2
    xb = hb // 4
    hbm = pl.BlockSpec(memory_space=pl.ANY)
    sem = pltpu.SemaphoreType.DMA
    S2, P2 = sem((2,)), sem((2, 2))
    vm = lambda *s: pltpu.VMEM(s, BF16)
    return pl.pallas_call(
        functools.partial(mlp_kernel, n_chunks),
        out_shape=tuple(jax.ShapeDtypeStruct((n, width), BF16) for n in (tokens, tokens - EARLY * chunk, tokens // 8 - EARLY * xb)),
        in_specs=[hbm, pl.BlockSpec(memory_space=pltpu.VMEM)] + [hbm] * 6,
        out_specs=(hbm, hbm, hbm),
        scratch_shapes=[
            vm(width, ff), vm(width, ff), vm(ff, width), vm(chunk, width), vm(2, chunk, 2 * ff),
            vm(2, qb // 2, 2 * ff), vm(2, 2, qb, 2 * ff), vm(2, chunk, ff), vm(chunk, width), vm(hb, width),
            vm(2, xb // 2, width), vm(2, xb, width), vm(chunk, width), vm(xb, width),
            vm(hb, width), vm(hb, width), vm(2, xb // 2, width), vm(2, xb, width), vm(xb, width), vm(xb, width), vm(xb, width),
            pltpu.VMEM((n_chunks, 4, 8, 128), F32),
            sem((11,)), sem, sem, S2, sem((4,)), sem, sem, sem((4, 2)), sem((4, 2)), sem((3,)), sem((n_chunks, 3)), sem((4,)), sem((4,)), pltpu.SemaphoreType.REGULAR((5,)),
            S2, S2, P2, P2, S2, S2, P2, P2,
            sem, sem, S2, S2, S2, S2, S2, S2, S2, S2, sem((4,)), sem((4,)),
        ],
        compiler_params=pltpu.CompilerParams(collective_id=1, has_side_effects=True, vmem_limit_bytes=67043328),
        name="mlp_phase",
    )(x_in, gains, m_early, h_early, o_part, w_gate, w_up, w_down)[0]


def attn_kernel(n_chunks, x_hbm, gains, cos_t, sin_t, wq_hbm, wk_hbm, wv_hbm, wo_hbm, m_hbm, h_hbm, wp_hbm,
                WQKV, WO, X, N, QP, R1, R2, QS, KV, O, WP, DR, XR1, XR2, XH, HB, MO, SQ, RC, ST1, ST2,
                w_sem, x_sem, xh_sem, hb_sem, mo_sem, wp_sem, credit,
                t1s, t1r, s1s, s1r, s2s, s2r, kvs, kvr, kfs, kfr, ocs, ocr, ofs, ofr, dds, ddr, x1s, x1r, x2s, x2r, t2s, t2r, xas, xar, xfs, xfr, dms, dmr):
    at = Place()
    tc, width = N.shape
    full_width = width * 4
    qkv_w = WQKV.shape[1]
    head = 128
    heads = QS.shape[1] // (tc // 4)
    q_w = heads * head
    qb = tc // 4
    hq = qb // 2
    hb = tc // 2
    xb = hb // 4
    hx = xb // 2
    own_half = at.core * hb
    my_rows = own_half + at.x * xb
    peers = at.ys + (at.dev_yo,)
    blk = min(128, tc)
    n_blk = tc // blk
    step = 16

    w_copies = [
        pltpu.make_async_copy(w, WQKV.at[:, pl.ds(i * head, head)], w_sem.at[i])
        for i, w in enumerate([wq_hbm.at[h] for h in range(heads)] + [wk_hbm, wv_hbm])
    ] + [pltpu.make_async_copy(wo_hbm, WO, w_sem.at[heads + 2])]

    def x_copy(c):
        return pltpu.make_async_copy(x_hbm.at[rows(c * tc, tc, tc)], X.at[c % 2], x_sem.at[c % 2])

    x_copy(0).start()
    for c in w_copies:
        c.start()
    at.entry(extra=(at.dev_yo,))

    def slot(c):
        return c % 4

    def pair(c):
        return c % 2

    def stats_copies(st, ssem, rsem, c):
        own = st.at[c, at.y]
        return [rcopy(own, own, ssem.at[pair(c), i], rsem.at[c, i], dev) for i, dev in enumerate(peers)]

    def s1_copies(c):
        s, o = slot(c), at.yo * qb
        return two([QP.at[s, rows(r, hq, hq)] for r in (o, o + hq)], slots(R1.at[s]), s1s.at[pair(c)], s1r.at[s], at.ys)

    def s2_copies(c):
        s = slot(c)
        return two([QP.at[s, rows(b * qb, qb, qb)] for b in (at.yp, at.ym)], slots(R2.at[s]), s2s.at[pair(c)], s2r.at[s], at.ys)

    def kv_copies(c):
        own = [KV.at[rows(c * tc + at.y * qb, qb, qb)]] * 2
        return two(own, own, kvs.at[pair(c)], kvr.at[c], at.ys)

    def kf_copies(c):
        half = [KV.at[rows(c * tc + r, hq, hq)] for r in (at.ym * qb, at.yp * qb + hq)]
        return two(half, half, kfs.at[pair(c)], kfr.at[c], at.ys)

    def o_copies(c):
        own = [O.at[slot(c), rows(at.y * qb, qb, qb)]] * 2
        return two(own, own, ocs.at[pair(c)], ocr.at[slot(c)], at.ys)

    def of_copies(c):
        half = [O.at[slot(c), rows(r, hq, hq)] for r in (at.ym * qb, at.yp * qb + hq)]
        return two(half, half, ofs.at[pair(c)], ofr.at[slot(c)], at.ys)

    def dd_copies(c):
        s = slot(c)
        return [rcopy(WP.at[s, rows((1 - at.core) * hb, hb, hb)], DR.at[s], dds.at[pair(c)], ddr.at[s], at.dev_core)]

    def x1_copies(c):
        s, o = slot(c), own_half + at.xo * xb
        return two([WP.at[s, rows(r, hx, hx)] for r in (o, o + hx)], slots(XR1.at[s]), x1s.at[pair(c)], x1r.at[s], at.xs)

    def x2_copies(c):
        s = slot(c)
        return two([WP.at[s, rows(own_half + b * xb, xb, xb)] for b in (at.xp, at.xm)], slots(XR2.at[s]), x2s.at[pair(c)], x2r.at[s], at.xs)

    def m_rows(c, start, size):
        return m_hbm.at[rows(c * tc + start, size, size)]

    def xa_copies(c):
        return two([MO.at[slot(c)]] * 2, [m_rows(c, my_rows, xb)] * 2, xas.at[pair(c)], xar.at[c], at.xs)

    def xf_copies(c):
        half = [m_rows(c, own_half + r, hx) for r in (at.xm * xb, at.xp * xb + hx)]
        return two(half, half, xfs.at[pair(c)], xfr.at[c], at.xs)

    def dm_copy(c, i):
        if i == 0:
            return rcopy(MO.at[slot(c)], m_rows(c, my_rows, xb), dms.at[pair(c), 0], dmr.at[c, 0], at.dev_core)
        b = m_rows(c, own_half + (at.xm, at.xp, at.xo)[i - 1] * xb, xb)
        return rcopy(b, b, dms.at[pair(c), i], dmr.at[c, i], at.dev_core)

    def dm_wait_recv(c, i):
        b = m_rows(c, (1 - at.core) * hb + (at.x, at.xm, at.xp, at.xo)[i] * xb, xb)
        rcopy(b, b, dms.at[pair(c), i], dmr.at[c, i], at.dev_core).wait_recv()

    def xh_copy(c):
        return pltpu.make_async_copy(x_hbm.at[rows(c * tc + my_rows, xb, xb)], XH.at[pair(c)], xh_sem.at[pair(c)])

    def hb_copy(c):
        return pltpu.make_async_copy(HB.at[slot(c)], h_hbm.at[rows(c * xb, xb, xb)], hb_sem.at[pair(c)])

    def mo_copy(c):
        return pltpu.make_async_copy(MO.at[slot(c)], m_rows(c, my_rows, xb), mo_sem.at[pair(c)])

    def wp_copy(c):
        return pltpu.make_async_copy(WP.at[slot(c)], wp_hbm.at[rows((c - EARLY) * tc, tc, tc)], wp_sem.at[pair(c)])

    def stage(k, s, body):
        c = k - s

        @pl.when(jnp.logical_and(c >= 0, c < (EARLY if body in early_chunks else n_chunks)))
        def _():
            body(c)

    def st_sumsq(c):
        x_copy(c).wait()

        @pl.loop(0, tc // step)
        def _(i):
            r = rows(i * step, step, step)
            SQ[r, :] = jnp.broadcast_to(square_sum(X[c % 2, r, :]), (step, 128))

        parts = [as_row(SQ[b * blk:(b + 1) * blk, :]) for b in range(n_blk)]
        parts = parts + [jnp.zeros_like(parts[0])] * (8 - n_blk)
        ST1[c, at.y] = jnp.concatenate(parts, axis=0)
        start(stats_copies(ST1, t1s, t1r, c))

    def st_qkv(c):
        wait(stats_copies(ST1, t1s, t1r, c))

        @pl.when(c == 0)
        def _():
            wait(w_copies[:-1])

        inv = inv_rms(ST1, c, full_width)
        for b in range(n_blk):
            RC[b * blk:(b + 1) * blk, :] = jnp.broadcast_to(as_col(inv[b:b + 1, :], blk), (blk, 128))

        @pl.loop(0, tc // step)
        def _(i):
            r = rows(i * step, step, step)
            N[r, :] = (X[c % 2, r, :].astype(F32) * RC[r, 0:1] * gains[0:1, :]).astype(BF16)

        n_t = qkv_w // 384

        @pl.loop(0, n_t)
        def _(n):
            cols = rows(n * 384, 384, 128)
            QP[slot(c), :, cols] = jnp.dot(N[...], WQKV[:, cols], preferred_element_type=F32).astype(BF16)

        start(s1_copies(c))

    def st_add1(c):
        wait(s1_copies(c))
        s = slot(c)

        @pl.loop(0, hq // step)
        def _(i):
            ri = rows(i * step, step, step)
            ra = rows(at.yp * qb + i * step, step, step)
            rb = rows(at.ym * qb + hq + i * step, step, step)
            QP[s, ra, :] = (QP[s, ra, :].astype(F32) + R1[s, 0, ri, :].astype(F32)).astype(BF16)
            QP[s, rb, :] = (QP[s, rb, :].astype(F32) + R1[s, 1, ri, :].astype(F32)).astype(BF16)

        start(s2_copies(c))

    def st_rope(c):
        wait(s2_copies(c))
        s = slot(c)
        own = rows(at.y * qb, qb, qb)
        cos_v = cos_t[rows(c * qb, qb, qb), :]
        sin_v = sin_t[rows(c * qb, qb, qb), :]

        def piece(i):
            cols = slice(i * head, (i + 1) * head)
            v = QP[s, own, cols].astype(F32) + R2[s, 0, :, cols].astype(F32) + R2[s, 1, :, cols].astype(F32)
            return v.astype(BF16)

        def turned(i):
            v = piece(i).astype(F32)
            return (v * cos_v + pltpu.roll(v, head // 2, 1) * sin_v).astype(BF16)

        kv_rows = rows(c * tc + at.y * qb, qb, qb)
        KV[kv_rows, 0:head] = turned(heads)
        KV[kv_rows, head:2 * head] = piece(heads + 1)
        start(kv_copies(c))
        for i in range(heads):
            QS[slot(c), i * qb:(i + 1) * qb, :] = turned(i)

    def st_kvfwd(c):
        wait(kv_copies(c))
        start(kf_copies(c))

    def st_attend(c):
        wait(kf_copies(c))
        q = QS[slot(c)]
        scale = head ** -0.5 * 1.4426950408889634

        def scores(j):
            keys = KV[rows(j * tc, tc, tc), 0:head]
            return lax.dot_general(q, keys, (((1,), (1,)), ((), ())), preferred_element_type=F32) * scale

        def values(j, p):
            return jnp.dot(p.astype(BF16), KV[rows(j * tc, tc, tc), head:2 * head], preferred_element_type=F32)

        qpos = at.y * qb + lax.broadcasted_iota(jnp.int32, (qb, tc), 0)
        keep = lax.broadcasted_iota(jnp.int32, (qb, tc), 1) <= qpos
        sc = scores(c).reshape(heads, qb, tc)
        sc = jnp.where(keep[None], sc, -jnp.inf).reshape(heads * qb, tc)
        top = jnp.max(sc, axis=-1, keepdims=True)
        p = jnp.exp2(sc - top)

        def more(j, carry):
            top, total, acc = carry
            sc = scores(j)
            new = jnp.maximum(top, jnp.max(sc, axis=-1, keepdims=True))
            fade = jnp.exp2(top - new)
            p = jnp.exp2(sc - new)
            return new, total * fade + jnp.sum(p, axis=-1, keepdims=True), acc * fade + values(j, p)

        top, total, acc = lax.fori_loop(0, c, more, (top, jnp.sum(p, axis=-1, keepdims=True), values(c, p)))
        out = (acc / total).astype(BF16)
        for i in range(heads):
            O[slot(c), rows(at.y * qb, qb, qb), i * head:(i + 1) * head] = out[i * qb:(i + 1) * qb, :]
        start(o_copies(c))

    def st_ofwd(c):
        wait(o_copies(c))
        start(of_copies(c))

    def st_oproj(c):
        wait(of_copies(c))

        @pl.when(c == 0)
        def _():
            w_copies[-1].wait()

        dn_w = 256 if width % 256 == 0 else 128

        @pl.loop(0, width // dn_w)
        def _(n):
            cols = rows(n * dn_w, dn_w, 128)
            WP[slot(c), :, cols] = jnp.dot(O[slot(c)], WO[:, cols], preferred_element_type=F32).astype(BF16)

        @pl.when(c < EARLY)
        def _():
            start(dd_copies(c))

        @pl.when(c >= EARLY)
        def _():
            wp_copy(c).start()

    def st_x1(c):
        @pl.when(c < EARLY)
        def _():
            st_x1_early(c)

        @pl.when(c >= EARLY)
        def _():
            wp_copy(c).wait()

    def st_x1_early(c):
        wait(dd_copies(c))
        s = slot(c)

        @pl.loop(0, hb // step)
        def _(i):
            ri = rows(i * step, step, step)
            ra = rows(own_half + i * step, step, step)
            WP[s, ra, :] = (WP[s, ra, :].astype(F32) + DR[s, ri, :].astype(F32)).astype(BF16)

        start(x1_copies(c))

    def st_x2(c):
        xh_copy(c).start()
        wait(x1_copies(c))
        s = slot(c)
        ra = rows(own_half + at.xp * xb, hx, hx)
        rb = rows(own_half + at.xm * xb + hx, hx, hx)
        WP[s, ra, :] = (WP[s, ra, :].astype(F32) + XR1[s, 0].astype(F32)).astype(BF16)
        WP[s, rb, :] = (WP[s, rb, :].astype(F32) + XR1[s, 1].astype(F32)).astype(BF16)
        start(x2_copies(c))

    def st_h(c):
        wait(x2_copies(c))
        xh_copy(c).wait()
        s = slot(c)
        total = WP[s, rows(my_rows, xb, xb), :].astype(F32) + XR2[s, 0].astype(F32) + XR2[s, 1].astype(F32)
        h = (XH[pair(c)].astype(F32) + total).astype(BF16)
        HB[s] = h
        row = as_row(jnp.broadcast_to(square_sum(h), (xb, 128)))
        ST2[c, at.y] = jnp.broadcast_to(row, (8, 128))
        start(stats_copies(ST2, t2s, t2r, c))
        hb_copy(c).start()

    def st_m(c):
        wait(stats_copies(ST2, t2s, t2r, c))
        hb_copy(c).wait()
        s = slot(c)
        inv = as_col(inv_rms(ST2, c, full_width)[0:1, :], xb)
        MO[s] = (HB[s].astype(F32) * inv * gains[1:2, :]).astype(BF16)
        start(xa_copies(c))
        dm_copy(c, 0).start()
        mo_copy(c).start()

    def st_xf(c):
        wait(xa_copies(c))
        dm_copy(c, 0).wait_send()
        mo_copy(c).wait()
        start(xf_copies(c))
        dm_copy(c, 1).start()
        dm_copy(c, 2).start()

    def st_dm(c):
        wait(xf_copies(c))
        dm_copy(c, 1).wait_send()
        dm_copy(c, 2).wait_send()
        dm_copy(c, 3).start()

    def st_end(c):
        dm_copy(c, 3).wait_send()
        for i in range(4):
            dm_wait_recv(c, i)

    all_chunks = (st_sumsq, st_qkv, st_add1, st_rope, st_kvfwd, st_attend, st_ofwd, st_oproj, st_x1)
    early_chunks = (st_x2, st_h, st_m, st_xf, st_dm, st_end)
    steps = all_chunks + early_chunks
    n_iter = max(n_chunks + len(all_chunks), EARLY + len(steps)) - 1

    @pl.loop(0, n_iter)
    def _(k):
        @pl.when(k >= 2)
        def _():
            at.take_credit(credit)

        for s, body in enumerate(steps):
            stage(k, s, body)
            if body is st_qkv:
                @pl.when(k + 1 < n_chunks)
                def _():
                    x_copy(k + 1).start()

        @pl.when(k < n_iter - 2)
        def _():
            at.give_credit(credit)


def attn_phase(x_in, gains, cos_t, sin_t, w_q, w_k, w_v, w_o, chunk):
    tokens, width = x_in.shape
    heads = w_q.shape[0]
    q_w = heads * 128
    n_chunks = tokens // chunk
    qb, hb = chunk // 4, chunk // 2
    xb = hb // 4
    hbm = pl.BlockSpec(memory_space=pl.ANY)
    vmem = pl.BlockSpec(memory_space=pltpu.VMEM)
    sem = pltpu.SemaphoreType.DMA
    S2, P2 = sem((2,)), sem((2, 2))
    vm = lambda *s: pltpu.VMEM(s, BF16)
    vf = lambda *s: pltpu.VMEM(s, F32)
    qkv_w = q_w + 256
    return pl.pallas_call(
        functools.partial(attn_kernel, n_chunks),
        out_shape=tuple(jax.ShapeDtypeStruct((n, width), BF16) for n in (EARLY * chunk, EARLY * xb, tokens - EARLY * chunk)),
        in_specs=[hbm, vmem, vmem, vmem, hbm, hbm, hbm, hbm],
        out_specs=(hbm, hbm, hbm),
        scratch_shapes=[
            vm(width, qkv_w), vm(q_w, width), vm(2, chunk, width), vm(chunk, width), vm(4, chunk, qkv_w),
            vm(4, 2, qb // 2, qkv_w), vm(4, 2, qb, qkv_w), vm(4, heads * qb, 128), vm(tokens, 256), vm(4, chunk, q_w),
            vm(4, chunk, width), vm(4, hb, width), vm(4, 2, xb // 2, width), vm(4, 2, xb, width), vm(2, xb, width), vm(4, xb, width), vm(4, xb, width),
            vf(chunk, 128), vf(chunk, 128), vf(n_chunks, 4, 8, 128), vf(n_chunks, 4, 8, 128),
            sem((heads + 3,)), S2, S2, S2, S2, S2, pltpu.SemaphoreType.REGULAR((5,)),
            sem((2, 3)), sem((n_chunks, 3)), P2, sem((4, 2)), P2, sem((4, 2)), P2, sem((n_chunks, 2)), P2, sem((n_chunks, 2)),
            P2, sem((4, 2)), P2, sem((4, 2)), S2, sem((4,)), P2, sem((4, 2)), P2, sem((4, 2)),
            sem((2, 3)), sem((n_chunks, 3)), P2, sem((n_chunks, 2)), P2, sem((n_chunks, 2)), sem((2, 4)), sem((n_chunks, 4)),
        ],
        compiler_params=pltpu.CompilerParams(collective_id=2, has_side_effects=True, vmem_limit_bytes=67043328),
        name="attn_phase",
    )(x_in, gains, cos_t, sin_t, w_q, w_k, w_v, w_o)


def copy_kernel(src, dst, buf, in_sem, out_sem):
    n, part = buf.shape[:2]
    ins = [pltpu.make_async_copy(src.at[pl.ds(i * part, part)], buf.at[i], in_sem.at[i]) for i in range(n)]
    outs = [pltpu.make_async_copy(buf.at[i], dst.at[pl.ds(i * part, part)], out_sem.at[i]) for i in range(n)]
    start(ins)
    for i in range(n):
        ins[i].wait()
        outs[i].start()
    for c in outs:
        c.wait()


def copy_out(y):
    tokens, width = y.shape
    n = 16
    hbm = pl.BlockSpec(memory_space=pl.ANY)
    return pl.pallas_call(
        copy_kernel,
        out_shape=jax.ShapeDtypeStruct(y.shape, y.dtype),
        in_specs=[hbm],
        out_specs=hbm,
        scratch_shapes=[pltpu.VMEM((n, tokens // n, width), y.dtype), pltpu.SemaphoreType.DMA((n,)), pltpu.SemaphoreType.DMA((n,))],
        compiler_params=pltpu.CompilerParams(vmem_limit_bytes=67043328),
        name="copy_out",
    )(y)


def solution(mesh, chunk=CHUNK):
    my_size = mesh.shape["my"]

    def local_layer(x_in, gain_attn, w_q, w_k, w_v, w_o, gain_mlp, w_gate, w_up, w_down):
        tokens, width = x_in.shape
        head = w_q.shape[-1]
        qb = chunk // my_size
        row = jnp.arange(tokens // my_size)
        positions = (row // qb) * chunk + lax.axis_index("my") * qb + row % qb
        half = head // 2
        inv_freq = ROPE_BASE ** (-jnp.arange(half, dtype=F32) / half)
        inv_freq = jnp.concatenate([inv_freq, inv_freq])
        angles = positions.astype(F32)[:, None] * inv_freq[None, :]
        cos_t = jnp.cos(angles)
        sin_t = jnp.sin(angles) * jnp.where(jnp.arange(head) < half, -1.0, 1.0)
        gains = jnp.stack([gain_attn, gain_mlp]).astype(F32)
        m_early, h_early, o_part = attn_phase(
            x_in, gains, cos_t, sin_t, w_q.transpose(1, 0, 2), w_k.reshape(width, -1), w_v.reshape(width, -1), w_o.reshape(-1, width), chunk)
        return copy_out(mlp_phase(x_in, gains, m_early, h_early, o_part, w_gate, w_up, w_down, chunk))

    in_specs = (P("dp", "my"), P("my"), P("my", "mx", None), P("my", "mx", None), P("my", "mx", None), P("mx", None, "my"), P("my"), P("my", "mx"), P("my", "mx"), P("mx", "my"))
    return jax.shard_map(local_layer, mesh=mesh, in_specs=in_specs, out_specs=P("dp", "my"), check_vma=False)
```
